8 devices in a mesh: dp: 1 (over z), pz: 2 (over y), py: 4 (over x, core).
Axes of the slice: x: 2, y: 2, z: 1, core: 2. Of those that a mesh axis runs over, the one named last changes fastest.
Arguments:
- rho_re: float32 [32, 64, 64, 64], P('dp', None, 'py', 'pz')
- rho_im: float32 [32, 64, 64, 64], P('dp', None, 'py', 'pz')
- g_re: float32 [64, 64, 64], P('py', 'pz')
- g_im: float32 [64, 64, 64], P('py', 'pz')
Outputs:
- output 1: float32 [32, 64, 64, 64], P('dp', None, 'py', 'pz')
- output 2: float32 [32, 64, 64, 64], P('dp', None, 'py', 'pz')
- output 3: float32 [32, 64, 64, 64], P('dp', 'py', 'pz')
- output 4: float32 [32, 64, 64, 64], P('dp', 'py', 'pz')
All inputs are finite; a program needn't handle non-finite values.
Results may differ from the reference program's by a relative error of at most 0.001.
Values sent between devices are 32-bit elements.
A program may use at most 1 GiB of HBM per device.

```python
import jax
import jax.numpy as jnp
from jax import lax

GRID = 64
FIELDS = 32


def green_kernel():
    positions = jnp.arange(GRID)
    wavenum = jnp.where(positions < (GRID + 1) // 2, positions, positions - GRID).astype(jnp.float32)
    wave_sq = wavenum * wavenum * (16.0 / (GRID * GRID))
    return 1.0 / (1.0 + wave_sq[:, None, None] + 2.0 * wave_sq[None, :, None] + 3.0 * wave_sq[None, None, :])


def setup_inputs(seed: int = 0, part: int = 0) -> dict:
    part_key = jax.random.fold_in(jax.random.key(seed), part)
    key_re, key_im = jax.random.split(part_key)
    field_shape = (FIELDS, GRID, GRID, GRID)
    rho_re = jax.random.normal(key_re, field_shape, jnp.float32)
    rho_im = jax.random.normal(key_im, field_shape, jnp.float32)
    green_re_key, green_im_key = jax.random.split(jax.random.key(seed + 1))
    kernel = green_kernel()
    g_re = kernel * (1.0 + 0.5 * jax.random.normal(green_re_key, kernel.shape, jnp.float32))
    g_im = kernel * (0.5 * jax.random.normal(green_im_key, kernel.shape, jnp.float32))
    return {"rho_re": rho_re, "rho_im": rho_im, "g_re": g_re, "g_im": g_im}


def reference(rho_re, rho_im, g_re, g_im):
    green_fn = lax.complex(g_re, g_im)

    def one_field(field_pair):
        volume = lax.complex(field_pair[0], field_pair[1])
        spectrum = jnp.fft.fftn(volume, axes=(0, 1, 2), norm="ortho") * green_fn
        restored = jnp.fft.ifftn(spectrum, axes=(0, 1, 2), norm="ortho")
        return jnp.real(restored), jnp.imag(restored), jnp.real(spectrum), jnp.imag(spectrum)

    phi_re, phi_im, hat_re, hat_im = lax.map(one_field, (rho_re, rho_im))
    return (phi_re, phi_im, hat_re, hat_im)
```

```python
import functools

import jax
import jax.numpy as jnp
import ml_dtypes
import numpy as np
from jax import lax
from jax.experimental import pallas as pl
from jax.experimental.pallas import tpu as pltpu
from jax.sharding import PartitionSpec as P

MESH = pl.DeviceIdType.MESH
F32, BF16 = jnp.float32, jnp.bfloat16
N = 64
FIELDS = 32
FG = 4
NG = FIELDS // FG
NU = NG * 4
NPY, NPZ = 4, 2
LAG3, LAG4 = 2, 4
LAG5 = LAG4 + 5
RING = 8
RA = 3


def dft(sign):
    jk = np.outer(np.arange(N), np.arange(N)) % N
    c, s = np.cos(2 * np.pi * jk / N) / 8, sign * np.sin(2 * np.pi * jk / N) / 8
    return np.stack([np.stack([c, -s], 1), np.stack([s, c], 1)])


def split_np(w):
    w = np.asarray(w, np.float32)
    parts = []
    for _ in range(3):
        part = w.astype(ml_dtypes.bfloat16)
        parts.append(part)
        w = w - part.astype(np.float32)
    return np.stack(parts)


def tables():
    fwd, inv = dft(-1), dft(1)
    i16, i32 = np.arange(16), np.arange(32)
    w1, w2, w3, w3i, w4, w5 = [], [], [], [], [], []
    for a in range(NPY):
        to = [16 * ((a + r) % 4) + i16 for r in range(4)]
        frm = [16 * ((a - r) % 4) + i16 for r in range(4)]
        out = np.stack([fwd[:, k] for k in to]).reshape(4, 2, 4, 4, 2, N)
        w1.append(out.transpose(4, 5, 0, 2, 3, 1).reshape(128, 128))
        inn = np.stack([inv[:, :, :, k] for k in frm]).reshape(4, 2, N, 2, 4, 4)
        w5.append(inn.transpose(4, 0, 5, 3, 1, 2).reshape(128, 128))
        for b in range(NPZ):
            half = [32 * (b ^ q) + i32 for q in range(2)]
            m = np.stack([fwd[:, k] for k in half])
            m = np.stack([m[..., y] for y in frm])
            w2.append(m.transpose(1, 2, 3, 0, 4, 5).reshape(128, 128))
            m = np.stack([inv[:, y] for y in to])
            m = np.stack([m[..., k] for k in half])
            w4.append(m.transpose(1, 2, 3, 0, 4, 5).reshape(128, 128))
    for b in range(NPZ):
        half = [32 * (b ^ q) + i32 for q in range(2)]
        m = np.stack([fwd[..., z] for z in half])
        w3.append(m.transpose(0, 3, 4, 1, 2).reshape(128, 128))
        m = np.stack([inv[:, z] for z in half])
        w3i.append(m.transpose(3, 4, 0, 1, 2).reshape(128, 128))
    return [np.stack([split_np(w) for w in ws]) for ws in (w1, w2, w3, w3i, w4, w5)]


def split3(x):
    hi = x.astype(BF16)
    rest = x - hi.astype(F32)
    mid = rest.astype(BF16)
    return hi, mid, (rest - mid.astype(F32)).astype(BF16)


def dot(a, b):
    return jnp.dot(a, b, preferred_element_type=F32)


def left(w, x):
    hi, mid, lo = split3(x)
    wide = dot(w[0][...], jnp.concatenate([hi, mid], 0))
    return wide[:128] + (wide[128:] + dot(w[1][...], jnp.concatenate([hi, lo], 0)))


def right(x, w):
    hi, mid, lo = split3(x)
    wide = dot(jnp.concatenate([hi, mid], 1), w[0][...])
    return wide[:, :128] + (wide[:, 128:] + dot(jnp.concatenate([hi, lo], 1), w[1][...]))


def swap_lanes(tiles):
    lane = lax.broadcasted_iota(jnp.int32, tiles[0].shape, 1)
    odd, high = (lane // 32) % 2 == 1, lane >= 64
    t = list(tiles)
    for lo in (0, 2):
        a, b = t[lo], t[lo + 1]
        t[lo] = jnp.where(odd, pltpu.roll(b, 32, 1), a)
        t[lo + 1] = jnp.where(odd, b, pltpu.roll(a, 96, 1))
    for lo in (0, 1):
        a, b = t[lo], t[lo + 2]
        t[lo] = jnp.where(high, pltpu.roll(b, 64, 1), a)
        t[lo + 2] = jnp.where(high, b, pltpu.roll(a, 64, 1))
    return t


def kernel(rho_re, rho_im, g_re, g_im, t1, t2, t3, t3i, t4, t5, phi_re, phi_im, hat_re, hat_im,
           rin, wraw, wbig, wsmall, ga, gb, a_send, a_recv, b_send, b_recv, c_send, c_recv, d_send, d_recv,
           hat_st, phi_st,
           in_sem, w_sem, hat_sem, phi_sem, as_sem, ar_sem, bs_sem, br_sem, cs_sem, cr_sem, ds_sem, dr_sem):
    me, mz = lax.axis_index("py"), lax.axis_index("pz")
    zero = lax.axis_index("dp")

    def py_peer(r):
        return (zero, mz, lax.rem(me + r, NPY))

    pz_peer = (zero, 1 - mz, me)

    def load_in(g):
        slot = lax.rem(g, 2)
        return [pltpu.make_async_copy(src.at[pl.ds(g * FG, FG)], rin.at[slot, i], in_sem.at[slot, i])
                for i, src in enumerate((rho_re, rho_im))]

    both = me * NPZ + mz
    tabs = [pltpu.make_async_copy(t.at[i], wraw.at[k], w_sem.at[k])
            for k, (t, i) in enumerate(((t1, me), (t2, both), (t3, mz), (t3i, mz), (t4, both), (t5, me)))]
    for cp in load_in(0):
        cp.start()
    for cp in tabs:
        cp.start()
    for cp in load_in(1):
        cp.start()
    barrier = pltpu.get_barrier_semaphore()
    for peer in [py_peer(r) for r in (1, 2, 3)] + [pz_peer]:
        pl.semaphore_signal(barrier, inc=1, device_id=peer, device_id_type=MESH)
    for k, cp in enumerate(tabs):
        cp.wait()
        w1, w2, w3 = (wraw[k, i] for i in range(3))
        if k in (1, 4):
            wbig[k] = jnp.concatenate([jnp.concatenate([w1, w1], 1), jnp.concatenate([w2, w2], 1)], 0)
            wsmall[k] = jnp.concatenate([w3, w1], 1).reshape(wsmall.shape[1:])
        else:
            wbig[k] = jnp.concatenate([jnp.concatenate([w1, w2], 1)] * 2, 0)
            wsmall[k] = jnp.concatenate([w3, w1], 1)
    gr, gi = g_re[...].reshape(512, N), g_im[...].reshape(512, N)
    ga[...] = jnp.concatenate([gr, gr], 1)
    gb[...] = jnp.concatenate([-gi, gi], 1)
    pl.semaphore_wait(barrier, 4)

    def lmat(k):
        return wbig.at[k], wsmall.at[k]

    def rmat(k):
        def small():
            w = wsmall[k]
            return jnp.concatenate([w[:, :128], w[:, 128:]], 0)
        return wbig[k], small()

    def stage1(g, y0, ny):
        slot, ring = lax.rem(g, 2), lax.rem(g, RA)
        w = rmat(0)
        for i in range(ny):
            y = y0 + i
            x = jnp.concatenate([rin[slot, 0, :, y].reshape(128, N), rin[slot, 1, :, y].reshape(128, N)], 1)
            out = right(x, w).T
            rows = pl.ds(pl.multiple_of(y * 8, 8), 8)
            for c in range(4):
                for r in range(4):
                    tile = out[(r * 4 + c) * 8:(r * 4 + c + 1) * 8]
                    if r == 0:
                        a_recv[g * 4 + c, 0, rows, :] = tile
                    else:
                        a_send[ring, c, r - 1, rows, :] = tile

    def a_copy(u, r):
        g, c = u // 4, lax.rem(u, 4)
        ring = lax.rem(g, RA)
        return pltpu.make_async_remote_copy(
            src_ref=a_send.at[ring, c, r - 1], dst_ref=a_recv.at[u, r], send_sem=as_sem.at[ring, c, r - 1],
            recv_sem=ar_sem.at[u, r - 1], device_id=py_peer(r), device_id_type=MESH)

    def b_copy(u):
        ring = lax.rem(u, RING)
        return pltpu.make_async_remote_copy(
            src_ref=b_send.at[ring], dst_ref=b_recv.at[u, 1], send_sem=bs_sem.at[ring], recv_sem=br_sem.at[u],
            device_id=pz_peer, device_id_type=MESH)

    def c_copy(u):
        ring = lax.rem(u, RING)
        return pltpu.make_async_remote_copy(
            src_ref=c_send.at[ring], dst_ref=c_recv.at[u, 1], send_sem=cs_sem.at[ring], recv_sem=cr_sem.at[u],
            device_id=pz_peer, device_id_type=MESH)

    def d_copy(u, r):
        ring = lax.rem(u, RING)
        return pltpu.make_async_remote_copy(
            src_ref=d_send.at[ring, r - 1], dst_ref=d_recv.at[u, r], send_sem=ds_sem.at[ring, r - 1],
            recv_sem=dr_sem.at[u, r - 1], device_id=py_peer(r), device_id_type=MESH)

    def send_a(g):
        for c in range(4):
            for r in (2, 1, 3):
                a_copy(g * 4 + c, r).start()

    def stage2(u):
        for r in (1, 2, 3):
            a_copy(u, r).wait_recv()
        ring = lax.rem(u, RING)

        @pl.when(u >= RING)
        def _():
            b_copy(u - RING).wait_send()

        w = lmat(1)
        for kp in range(2):
            cols = [jnp.concatenate([a_recv[u, r, pl.ds(kk * 2 + ri, 16, stride=8), :]
                                     for r in range(4) for ri in range(2)], 0) for kk in (2 * kp, 2 * kp + 1)]
            out = left(w, jnp.concatenate(cols, 1))
            for i in range(2):
                kk = 2 * kp + i
                b_recv[u, 0, kk] = out[:64, i * 128:(i + 1) * 128]
                b_send[ring, kk] = out[64:, i * 128:(i + 1) * 128]
        b_copy(u).start()

    def hat_copy(u, i):
        slot = lax.rem(u, 2)
        g, c = u // 4, lax.rem(u, 4)
        return pltpu.make_async_copy(
            hat_st.at[slot, i], (hat_re, hat_im)[i].at[pl.ds(g * FG, FG), pl.ds(c * 4, 4)], hat_sem.at[slot, i])

    def stage3(u):
        b_copy(u).wait_recv()
        ring, slot = lax.rem(u, RING), lax.rem(u, 2)
        c = lax.rem(u, 4)

        @pl.when(u >= RING)
        def _():
            c_copy(u - RING).wait_send()

        @pl.when(u >= 2)
        def _():
            for i in range(2):
                hat_copy(u - 2, i).wait()

        wf, wi = rmat(2), rmat(3)
        for kp in range(2):
            rows = []
            for kk in (2 * kp, 2 * kp + 1):
                rows += swap_lanes([b_recv[u, q, kk, ri * 32:(ri + 1) * 32, :] for q in range(2) for ri in range(2)])
            spec = right(jnp.concatenate(rows, 0), wf)
            hats = []
            for i in range(2):
                kk = 2 * kp + i
                gr = pl.ds(pl.multiple_of((c * 4 + kk) * 32, 32), 32)
                gan, gbn = ga[gr, :], gb[gr, :]
                for f in range(FG):
                    s = spec[(i * FG + f) * 32:(i * FG + f + 1) * 32]
                    h = s * gan + pltpu.roll(s, 64, 1) * gbn
                    hat_st[slot, 0, f, kk] = h[:, :N]
                    hat_st[slot, 1, f, kk] = h[:, N:]
                    hats.append(h)
            back = right(jnp.concatenate(hats, 0), wi)
            for i in range(2):
                kk = 2 * kp + i
                t = swap_lanes([back[(i * FG + f) * 32:(i * FG + f + 1) * 32] for f in range(FG)])
                for ri in range(2):
                    c_recv[u, 0, kk, ri * 32:(ri + 1) * 32, :] = t[ri]
                    c_send[ring, kk, ri * 32:(ri + 1) * 32, :] = t[2 + ri]
        c_copy(u).start()
        for i in range(2):
            hat_copy(u, i).start()

    def stage4(u):
        c_copy(u).wait_recv()
        ring = lax.rem(u, RING)

        @pl.when(u >= RING)
        def _():
            for r in (1, 2, 3):
                d_copy(u - RING, r).wait_send()

        w = lmat(4)
        for kp in range(2):
            cols = [jnp.concatenate([c_recv[u, q, kk] for q in range(2)], 0) for kk in (2 * kp, 2 * kp + 1)]
            out = left(w, jnp.concatenate(cols, 1))
            for i in range(2):
                kk = 2 * kp + i
                for r in range(4):
                    for ro in range(2):
                        rows = pl.ds(kk * 2 + ro, 16, stride=8)
                        tile = out[(r * 2 + ro) * 16:(r * 2 + ro + 1) * 16, i * 128:(i + 1) * 128]
                        if r == 0:
                            d_recv[u, 0, rows, :] = tile
                        else:
                            d_send[ring, r - 1, rows, :] = tile
        for r in (2, 1, 3):
            d_copy(u, r).start()

    def phi_copy(g, i):
        slot = lax.rem(g, 2)
        return pltpu.make_async_copy(phi_st.at[slot, i], (phi_re, phi_im)[i].at[pl.ds(g * FG, FG)],
                                     phi_sem.at[slot, i])

    def stage5(g, y0, ny):
        slot = lax.rem(g, 2)
        w = rmat(5)
        for i in range(ny):
            y = y0 + i
            rows = pl.ds(pl.multiple_of(y * 8, 8), 8)
            x = jnp.concatenate([d_recv[g * 4 + c, r, rows, :] for c in range(4) for r in range(4)], 0)
            out = right(x.T, w)
            phi_st[slot, 0, :, y] = out[:, :N].reshape(FG, 32, N)
            phi_st[slot, 1, :, y] = out[:, N:].reshape(FG, 32, N)

    for g in range(2):
        for cp in load_in(g):
            cp.wait()

        @pl.loop(0, 4)
        def _(q, g=g):
            stage1(g, q * 4, 4)

        send_a(g)
        for cp in load_in(g + 2):
            cp.start()

    def step(t, carry):
        c = lax.rem(t, 4)
        g1 = t // 4 + 2

        @pl.when(t < NU)
        def _():
            stage2(t)

        u3 = t - LAG3

        @pl.when(jnp.logical_and(u3 >= 0, u3 < NU))
        def _():
            stage3(u3)

        u4 = t - LAG4

        @pl.when(jnp.logical_and(u4 >= 0, u4 < NU))
        def _():
            stage4(u4)

        @pl.when(g1 < NG)
        def _():
            @pl.when(c == 0)
            def _():
                for cp in load_in(g1):
                    cp.wait()

                @pl.when(g1 >= RA)
                def _():
                    for cc in range(4):
                        for r in (1, 2, 3):
                            a_copy((g1 - RA) * 4 + cc, r).wait_send()

            stage1(g1, c * 4, 4)

            @pl.when(c == 3)
            def _():
                send_a(g1)

                @pl.when(g1 + 2 < NG)
                def _():
                    for cp in load_in(g1 + 2):
                        cp.start()

        u5 = t - LAG5
        g5 = u5 // 4
        c5 = lax.rem(u5 + 16, 4)

        @pl.when(u5 >= 0)
        def _():
            @pl.when(c5 == 0)
            def _():
                for cc in range(4):
                    for r in (1, 2, 3):
                        d_copy(g5 * 4 + cc, r).wait_recv()

                @pl.when(g5 >= 2)
                def _():
                    for i in range(2):
                        phi_copy(g5 - 2, i).wait()

            stage5(g5, c5 * 4, 4)

            @pl.when(c5 == 3)
            def _():
                for i in range(2):
                    phi_copy(g5, i).start()

        return carry

    lax.fori_loop(0, NU + LAG5, step, 0)

    for g in range(NG - 2, NG):
        for i in range(2):
            phi_copy(g, i).wait()
    for u in range(NU - 2, NU):
        for i in range(2):
            hat_copy(u, i).wait()
    for g in range(NG - RA, NG):
        for c in range(4):
            for r in (1, 2, 3):
                a_copy(g * 4 + c, r).wait_send()
    for u in range(NU - RING, NU):
        b_copy(u).wait_send()
        c_copy(u).wait_send()
        for r in (1, 2, 3):
            d_copy(u, r).wait_send()


def solution(mesh):
    consts = tables()

    def local_solve(rho_re, rho_im, g_re, g_im):
        dma, vmem, hbm = pltpu.SemaphoreType.DMA, pltpu.VMEM, pl.BlockSpec(memory_space=pl.ANY)
        tabs = [jnp.asarray(c) for c in consts]
        field = jax.ShapeDtypeStruct((FIELDS, 16, 32, N), F32)
        outs = pl.pallas_call(
            kernel,
            out_shape=[field] * 4,
            in_specs=[hbm, hbm] + [pl.BlockSpec(memory_space=pltpu.VMEM)] * 2 + [hbm] * 6,
            out_specs=[hbm] * 4,
            scratch_shapes=[
                vmem((2, 2, FG, 16, 32, N), F32),
                vmem((6, 3, 128, 128), BF16),
                vmem((6, 256, 256), BF16),
                vmem((6, 128, 256), BF16),
                vmem((512, 128), F32), vmem((512, 128), F32),
                vmem((RA, 4, 3, 128, 128), F32),
                vmem((NU, 4, 128, 128), F32),
                vmem((RING, 4, 64, 128), F32),
                vmem((NU, 2, 4, 64, 128), F32),
                vmem((RING, 4, 64, 128), F32),
                vmem((NU, 2, 4, 64, 128), F32),
                vmem((RING, 3, 128, 128), F32),
                vmem((NU, 4, 128, 128), F32),
                vmem((2, 2, FG, 4, 32, N), F32),
                vmem((2, 2, FG, 16, 32, N), F32),
                dma((2, 2)), dma((6,)), dma((2, 2)), dma((2, 2)),
                dma((RA, 4, 3)), dma((NU, 3)), dma((RING,)), dma((NU,)), dma((RING,)), dma((NU,)),
                dma((RING, 3)), dma((NU, 3)),
            ],
            compiler_params=pltpu.CompilerParams(collective_id=0, has_side_effects=True,
                                                 vmem_limit_bytes=60 * 2 ** 20),
            name="spectral",
        )(jnp.transpose(rho_re, (0, 2, 3, 1)), jnp.transpose(rho_im, (0, 2, 3, 1)), g_re, g_im, *tabs)
        phi_re, phi_im, hat_re, hat_im = outs
        return jnp.transpose(phi_re, (0, 3, 1, 2)), jnp.transpose(phi_im, (0, 3, 1, 2)), hat_re, hat_im

    space_layout = P("dp", None, "py", "pz")
    wave_layout = P("dp", "py", "pz", None)
    green_layout = P("py", "pz", None)
    return jax.shard_map(local_solve, mesh=mesh,
                         in_specs=(space_layout, space_layout, green_layout, green_layout),
                         out_specs=(space_layout, space_layout, wave_layout, wave_layout),
                         check_vma=False)
```

```python
import functools

import jax
import jax.numpy as jnp
import ml_dtypes
import numpy as np
from jax import lax
from jax.experimental import pallas as pl
from jax.experimental.pallas import tpu as pltpu
from jax.sharding import PartitionSpec as P

MESH = pl.DeviceIdType.MESH
F32, BF16 = jnp.float32, jnp.bfloat16
N = 64
FIELDS = 32
FG = 4
NG = FIELDS // FG
NU = NG * 4
NPY, NPZ = 4, 2
LAG3, LAG4 = 2, 4
LAG5 = LAG4 + 5
RING = 8
RA = 3
FB, SLOTS = 2, 4


def dft(sign):
    jk = np.outer(np.arange(N), np.arange(N)) % N
    c, s = np.cos(2 * np.pi * jk / N) / 8, sign * np.sin(2 * np.pi * jk / N) / 8
    return np.stack([np.stack([c, -s], 1), np.stack([s, c], 1)])


def split_np(w):
    w = np.asarray(w, np.float32)
    parts = []
    for _ in range(3):
        part = w.astype(ml_dtypes.bfloat16)
        parts.append(part)
        w = w - part.astype(np.float32)
    return np.stack(parts)


def tables():
    fwd, inv = dft(-1), dft(1)
    i16, i32 = np.arange(16), np.arange(32)
    w1, w2, w3, w3i, w4, w5 = [], [], [], [], [], []
    for a in range(NPY):
        to = [16 * ((a + r) % 4) + i16 for r in range(4)]
        frm = [16 * ((a - r) % 4) + i16 for r in range(4)]
        out = np.stack([fwd[:, k] for k in to]).reshape(4, 2, 4, 4, 2, N)
        w1.append(out.transpose(4, 5, 0, 2, 3, 1).reshape(128, 128))
        inn = np.stack([inv[:, :, :, k] for k in frm]).reshape(4, 2, N, 2, 4, 4)
        w5.append(inn.transpose(4, 0, 5, 3, 1, 2).reshape(128, 128))
        for b in range(NPZ):
            half = [32 * (b ^ q) + i32 for q in range(2)]
            m = np.stack([fwd[:, k] for k in half])
            m = np.stack([m[..., y] for y in frm])
            w2.append(m.transpose(1, 2, 3, 0, 4, 5).reshape(128, 128))
            m = np.stack([inv[:, y] for y in to])
            m = np.stack([m[..., k] for k in half])
            w4.append(m.transpose(1, 2, 3, 0, 4, 5).reshape(128, 128))
    for b in range(NPZ):
        half = [32 * (b ^ q) + i32 for q in range(2)]
        m = np.stack([fwd[..., z] for z in half])
        w3.append(m.transpose(0, 3, 4, 1, 2).reshape(128, 128))
        m = np.stack([inv[:, z] for z in half])
        w3i.append(m.transpose(3, 4, 0, 1, 2).reshape(128, 128))
    return [np.stack([split_np(w) for w in ws]) for ws in (w1, w2, w3, w3i, w4, w5)]


def split3(x):
    hi = x.astype(BF16)
    rest = x - hi.astype(F32)
    mid = rest.astype(BF16)
    return hi, mid, (rest - mid.astype(F32)).astype(BF16)


def dot(a, b):
    return jnp.dot(a, b, preferred_element_type=F32)


def left(w, x):
    hi, mid, lo = split3(x)
    wide = dot(w[0][...], jnp.concatenate([hi, mid], 0))
    return wide[:128] + (wide[128:] + dot(w[1][...], jnp.concatenate([hi, lo], 0)))


def right(x, w):
    hi, mid, lo = split3(x)
    wide = dot(jnp.concatenate([hi, mid], 1), w[0][...])
    return wide[:, :128] + (wide[:, 128:] + dot(jnp.concatenate([hi, lo], 1), w[1][...]))


def swap_lanes(tiles):
    lane = lax.broadcasted_iota(jnp.int32, tiles[0].shape, 1)
    odd, high = (lane // 32) % 2 == 1, lane >= 64
    t = list(tiles)
    for lo in (0, 2):
        a, b = t[lo], t[lo + 1]
        t[lo] = jnp.where(odd, pltpu.roll(b, 32, 1), a)
        t[lo + 1] = jnp.where(odd, b, pltpu.roll(a, 96, 1))
    for lo in (0, 1):
        a, b = t[lo], t[lo + 2]
        t[lo] = jnp.where(high, pltpu.roll(b, 64, 1), a)
        t[lo + 2] = jnp.where(high, b, pltpu.roll(a, 64, 1))
    return t


def kernel(rho_re, rho_im, g_re, g_im, t1, t2, t3, t3i, t4, t5, d_recv, hat,
           rin, wraw, wbig, wsmall, ga, gb, a_send, a_recv, b_send, b_recv, c_send, c_recv, d_send,
           in_sem, w_sem, as_sem, ar_sem, bs_sem, br_sem, cs_sem, cr_sem, ds_sem, dr_sem):
    me, mz = lax.axis_index("py"), lax.axis_index("pz")
    zero = lax.axis_index("dp")

    def py_peer(r):
        return (zero, mz, lax.rem(me + r, NPY))

    pz_peer = (zero, 1 - mz, me)

    def load_in(g):
        slot = lax.rem(g, 2)
        return [pltpu.make_async_copy(src.at[pl.ds(g * FG, FG)], rin.at[slot, i], in_sem.at[slot, i])
                for i, src in enumerate((rho_re, rho_im))]

    both = me * NPZ + mz
    tabs = [pltpu.make_async_copy(t.at[i], wraw.at[k], w_sem.at[k])
            for k, (t, i) in enumerate(((t1, me), (t2, both), (t3, mz), (t3i, mz), (t4, both), (t5, me)))]
    for cp in load_in(0):
        cp.start()
    for cp in tabs:
        cp.start()
    for cp in load_in(1):
        cp.start()
    barrier = pltpu.get_barrier_semaphore()
    for peer in [py_peer(r) for r in (1, 2, 3)] + [pz_peer]:
        pl.semaphore_signal(barrier, inc=1, device_id=peer, device_id_type=MESH)
    for k, cp in enumerate(tabs):
        cp.wait()
        w1, w2, w3 = (wraw[k, i] for i in range(3))
        if k in (1, 4):
            wbig[k] = jnp.concatenate([jnp.concatenate([w1, w1], 1), jnp.concatenate([w2, w2], 1)], 0)
            wsmall[k] = jnp.concatenate([w3, w1], 1).reshape(wsmall.shape[1:])
        else:
            wbig[k] = jnp.concatenate([jnp.concatenate([w1, w2], 1)] * 2, 0)
            wsmall[k] = jnp.concatenate([w3, w1], 1)
    gr, gi = g_re[...].reshape(512, N), g_im[...].reshape(512, N)
    ga[...] = jnp.concatenate([gr, gr], 1)
    gb[...] = jnp.concatenate([-gi, gi], 1)
    pl.semaphore_wait(barrier, 4)

    def lmat(k):
        return wbig.at[k], wsmall.at[k]

    def rmat(k):
        def small():
            w = wsmall[k]
            return jnp.concatenate([w[:, :128], w[:, 128:]], 0)
        return wbig[k], small()

    def stage1(g, y0, ny):
        slot, ring = lax.rem(g, 2), lax.rem(g, RA)
        w = rmat(0)
        for i in range(ny):
            y = y0 + i
            x = jnp.concatenate([rin[slot, 0, :, y].reshape(128, N), rin[slot, 1, :, y].reshape(128, N)], 1)
            out = right(x, w).T
            rows = pl.ds(pl.multiple_of(y * 8, 8), 8)
            for c in range(4):
                for r in range(4):
                    tile = out[(r * 4 + c) * 8:(r * 4 + c + 1) * 8]
                    if r == 0:
                        a_recv[g * 4 + c, 0, rows, :] = tile
                    else:
                        a_send[ring, c, r - 1, rows, :] = tile

    def a_copy(u, r):
        g, c = u // 4, lax.rem(u, 4)
        ring = lax.rem(g, RA)
        return pltpu.make_async_remote_copy(
            src_ref=a_send.at[ring, c, r - 1], dst_ref=a_recv.at[u, r], send_sem=as_sem.at[ring, c, r - 1],
            recv_sem=ar_sem.at[u, r - 1], device_id=py_peer(r), device_id_type=MESH)

    def b_copy(u):
        ring = lax.rem(u, RING)
        return pltpu.make_async_remote_copy(
            src_ref=b_send.at[ring], dst_ref=b_recv.at[u, 1], send_sem=bs_sem.at[ring], recv_sem=br_sem.at[u],
            device_id=pz_peer, device_id_type=MESH)

    def c_copy(u):
        ring = lax.rem(u, RING)
        return pltpu.make_async_remote_copy(
            src_ref=c_send.at[ring], dst_ref=c_recv.at[u, 1], send_sem=cs_sem.at[ring], recv_sem=cr_sem.at[u],
            device_id=pz_peer, device_id_type=MESH)

    def d_copy(u, r):
        ring = lax.rem(u, RING)
        return pltpu.make_async_remote_copy(
            src_ref=d_send.at[ring, r - 1], dst_ref=d_recv.at[u, r], send_sem=ds_sem.at[ring, r - 1],
            recv_sem=dr_sem.at[u, r - 1], device_id=py_peer(r), device_id_type=MESH)

    def send_a(g):
        for c in range(4):
            for r in (2, 1, 3):
                a_copy(g * 4 + c, r).start()

    def stage2(u):
        for r in (1, 2, 3):
            a_copy(u, r).wait_recv()
        ring = lax.rem(u, RING)

        @pl.when(u >= RING)
        def _():
            b_copy(u - RING).wait_send()

        w = lmat(1)
        for kp in range(2):
            cols = [jnp.concatenate([a_recv[u, r, pl.ds(kk * 2 + ri, 16, stride=8), :]
                                     for r in range(4) for ri in range(2)], 0) for kk in (2 * kp, 2 * kp + 1)]
            out = left(w, jnp.concatenate(cols, 1))
            for i in range(2):
                kk = 2 * kp + i
                b_recv[u, 0, kk] = out[:64, i * 128:(i + 1) * 128]
                b_send[ring, kk] = out[64:, i * 128:(i + 1) * 128]
        b_copy(u).start()

    def stage3(u):
        b_copy(u).wait_recv()
        ring, c, f0 = lax.rem(u, RING), lax.rem(u, 4), u // 4 * FG

        @pl.when(u >= RING)
        def _():
            c_copy(u - RING).wait_send()

        wf, wi = rmat(2), rmat(3)
        for kp in range(2):
            rows = []
            for kk in (2 * kp, 2 * kp + 1):
                rows += swap_lanes([b_recv[u, q, kk, ri * 32:(ri + 1) * 32, :] for q in range(2) for ri in range(2)])
            spec = right(jnp.concatenate(rows, 0), wf)
            hats = []
            for i in range(2):
                kk = 2 * kp + i
                gr = pl.ds(pl.multiple_of((c * 4 + kk) * 32, 32), 32)
                gan, gbn = ga[gr, :], gb[gr, :]
                for f in range(FG):
                    s = spec[(i * FG + f) * 32:(i * FG + f + 1) * 32]
                    h = s * gan + pltpu.roll(s, 64, 1) * gbn
                    hat[f0 + f, c * 4 + kk] = h
                    hats.append(h)
            back = right(jnp.concatenate(hats, 0), wi)
            for i in range(2):
                kk = 2 * kp + i
                t = swap_lanes([back[(i * FG + f) * 32:(i * FG + f + 1) * 32] for f in range(FG)])
                for ri in range(2):
                    c_recv[u, 0, kk, ri * 32:(ri + 1) * 32, :] = t[ri]
                    c_send[ring, kk, ri * 32:(ri + 1) * 32, :] = t[2 + ri]
        c_copy(u).start()

    def stage4(u):
        c_copy(u).wait_recv()
        ring = lax.rem(u, RING)

        @pl.when(u >= RING)
        def _():
            for r in (1, 2, 3):
                d_copy(u - RING, r).wait_send()

        w = lmat(4)
        for kp in range(2):
            cols = [jnp.concatenate([c_recv[u, q, kk] for q in range(2)], 0) for kk in (2 * kp, 2 * kp + 1)]
            out = left(w, jnp.concatenate(cols, 1))
            for i in range(2):
                kk = 2 * kp + i
                for r in range(4):
                    for ro in range(2):
                        rows = pl.ds(kk * 2 + ro, 16, stride=8)
                        tile = out[(r * 2 + ro) * 16:(r * 2 + ro + 1) * 16, i * 128:(i + 1) * 128]
                        if r == 0:
                            d_recv[u, 0, rows, :] = tile
                        else:
                            d_send[ring, r - 1, rows, :] = tile
        for r in (2, 1, 3):
            d_copy(u, r).start()

    def stage5(g, y0, ny):
        w = rmat(5)
        for i in range(ny):
            y = y0 + i
            rows = pl.ds(pl.multiple_of(y * 8, 8), 8)
            x = jnp.concatenate([d_recv[g * 4 + c, r, rows, :] for c in range(4) for r in range(4)], 0)
            out = right(x.T, w)
            for f in range(FG):
                for r in range(4):
                    d_recv[g * 4 + f, r, rows, :] = out[(f * 4 + r) * 8:(f * 4 + r + 1) * 8]

    for g in range(2):
        for cp in load_in(g):
            cp.wait()

        @pl.loop(0, 4)
        def _(q, g=g):
            stage1(g, q * 4, 4)

        send_a(g)
        for cp in load_in(g + 2):
            cp.start()

    def step(t, carry):
        c = lax.rem(t, 4)
        g1 = t // 4 + 2

        @pl.when(t < NU)
        def _():
            stage2(t)

        u3 = t - LAG3

        @pl.when(jnp.logical_and(u3 >= 0, u3 < NU))
        def _():
            stage3(u3)

        u4 = t - LAG4

        @pl.when(jnp.logical_and(u4 >= 0, u4 < NU))
        def _():
            stage4(u4)

        @pl.when(g1 < NG)
        def _():
            @pl.when(c == 0)
            def _():
                for cp in load_in(g1):
                    cp.wait()

                @pl.when(g1 >= RA)
                def _():
                    for cc in range(4):
                        for r in (1, 2, 3):
                            a_copy((g1 - RA) * 4 + cc, r).wait_send()

            stage1(g1, c * 4, 4)

            @pl.when(c == 3)
            def _():
                send_a(g1)

                @pl.when(g1 + 2 < NG)
                def _():
                    for cp in load_in(g1 + 2):
                        cp.start()

        u5 = t - LAG5
        g5 = u5 // 4
        c5 = lax.rem(u5 + 16, 4)

        @pl.when(u5 >= 0)
        def _():
            @pl.when(c5 == 0)
            def _():
                for cc in range(4):
                    for r in (1, 2, 3):
                        d_copy(g5 * 4 + cc, r).wait_recv()

            stage5(g5, c5 * 4, 4)

        return carry

    lax.fori_loop(0, NU + LAG5, step, 0)

    for g in range(NG - RA, NG):
        for c in range(4):
            for r in (1, 2, 3):
                a_copy(g * 4 + c, r).wait_send()
    for u in range(NU - RING, NU):
        b_copy(u).wait_send()
        c_copy(u).wait_send()
        for r in (1, 2, 3):
            d_copy(u, r).wait_send()


def unpack(phi, hat, phi_re, phi_im, hat_re, hat_im, st, sem):
    outs = (phi_re, phi_im, hat_re, hat_im)

    def copy(i, k):
        slot = lax.rem(i, SLOTS)
        return pltpu.make_async_copy(st.at[slot, k], outs[k].at[pl.ds(i * FB, FB)], sem.at[slot, k])

    def step(i, carry):
        slot = lax.rem(i, SLOTS)

        @pl.when(i >= SLOTS)
        def _():
            for k in range(4):
                copy(i - SLOTS, k).wait()

        for f in range(FB):
            h = hat[i * FB + f].reshape(512, 128)
            st[slot, 2, f] = h[:, :N].reshape(16, 32, N)
            st[slot, 3, f] = h[:, N:].reshape(16, 32, N)
        for k in (2, 3):
            copy(i, k).start()
        for f in range(FB):
            for r in range(4):
                p = phi[i * FB + f, r]
                st[slot, 0, f, :, r * 8:(r + 1) * 8] = p[:, :N].reshape(16, 8, N)
                st[slot, 1, f, :, r * 8:(r + 1) * 8] = p[:, N:].reshape(16, 8, N)
        for k in (0, 1):
            copy(i, k).start()
        return carry

    lax.fori_loop(0, FIELDS // FB, step, 0)
    for i in range(FIELDS // FB - SLOTS, FIELDS // FB):
        for k in range(4):
            copy(i, k).wait()


def solution(mesh):
    consts = tables()

    def local_solve(rho_re, rho_im, g_re, g_im):
        dma, vmem, hbm = pltpu.SemaphoreType.DMA, pltpu.VMEM, pl.BlockSpec(memory_space=pl.ANY)
        tabs = [jnp.asarray(c) for c in consts]
        field = jax.ShapeDtypeStruct((FIELDS, 16, 32, N), F32)
        phi, hat = pl.pallas_call(
            kernel,
            out_shape=[pltpu.VMEM((NU, 4, 128, 128), F32), pltpu.VMEM((FIELDS, 16, 32, 128), F32)],
            in_specs=[hbm, hbm] + [pl.BlockSpec(memory_space=pltpu.VMEM)] * 2 + [hbm] * 6,
            out_specs=[pl.BlockSpec(memory_space=pltpu.VMEM)] * 2,
            scratch_shapes=[
                vmem((2, 2, FG, 16, 32, N), F32),
                vmem((6, 3, 128, 128), BF16),
                vmem((6, 256, 256), BF16),
                vmem((6, 128, 256), BF16),
                vmem((512, 128), F32), vmem((512, 128), F32),
                vmem((RA, 4, 3, 128, 128), F32),
                vmem((NU, 4, 128, 128), F32),
                vmem((RING, 4, 64, 128), F32),
                vmem((NU, 2, 4, 64, 128), F32),
                vmem((RING, 4, 64, 128), F32),
                vmem((NU, 2, 4, 64, 128), F32),
                vmem((RING, 3, 128, 128), F32),
                dma((2, 2)), dma((6,)),
                dma((RA, 4, 3)), dma((NU, 3)), dma((RING,)), dma((NU,)), dma((RING,)), dma((NU,)),
                dma((RING, 3)), dma((NU, 3)),
            ],
            compiler_params=pltpu.CompilerParams(collective_id=0, has_side_effects=True,
                                                 vmem_limit_bytes=44 * 2 ** 20),
            name="spectral",
        )(jnp.transpose(rho_re, (0, 2, 3, 1)), jnp.transpose(rho_im, (0, 2, 3, 1)), g_re, g_im, *tabs)
        phi, hat = (pltpu.with_memory_space_constraint(x, pltpu.VMEM) for x in (phi, hat))
        phi_re, phi_im, hat_re, hat_im = pl.pallas_call(
            unpack,
            out_shape=[field] * 4,
            in_specs=[pl.BlockSpec(memory_space=pltpu.VMEM)] * 2,
            out_specs=[hbm] * 4,
            scratch_shapes=[vmem((SLOTS, 4, FB, 16, 32, N), F32), dma((SLOTS, 4))],
            compiler_params=pltpu.CompilerParams(vmem_limit_bytes=20 * 2 ** 20),
            name="unpack",
        )(phi, hat)
        return jnp.transpose(phi_re, (0, 3, 1, 2)), jnp.transpose(phi_im, (0, 3, 1, 2)), hat_re, hat_im

    space_layout = P("dp", None, "py", "pz")
    wave_layout = P("dp", "py", "pz", None)
    green_layout = P("py", "pz", None)
    return jax.shard_map(local_solve, mesh=mesh,
                         in_specs=(space_layout, space_layout, green_layout, green_layout),
                         out_specs=(space_layout, space_layout, wave_layout, wave_layout),
                         check_vma=False)
```

```python
import functools

import jax
import jax.numpy as jnp
import ml_dtypes
import numpy as np
from jax import lax
from jax.experimental import pallas as pl
from jax.experimental.pallas import tpu as pltpu
from jax.sharding import PartitionSpec as P

MESH = pl.DeviceIdType.MESH
F32, BF16 = jnp.float32, jnp.bfloat16
N = 64
FIELDS = 32
FG = 4
NG = FIELDS // FG
NU = NG * 4
NPY, NPZ = 4, 2
LAG3, LAG4 = 2, 4
LAG5 = LAG4 + 5
RING = 8
RA = 3
FB, SLOTS = 2, 8


def dft(sign):
    jk = np.outer(np.arange(N), np.arange(N)) % N
    c, s = np.cos(2 * np.pi * jk / N) / 8, sign * np.sin(2 * np.pi * jk / N) / 8
    return np.stack([np.stack([c, -s], 1), np.stack([s, c], 1)])


def split_np(w):
    w = np.asarray(w, np.float32)
    parts = []
    for _ in range(3):
        part = w.astype(ml_dtypes.bfloat16)
        parts.append(part)
        w = w - part.astype(np.float32)
    return np.stack(parts)


def tables():
    fwd, inv = dft(-1), dft(1)
    i16, i32 = np.arange(16), np.arange(32)
    w1, w2, w3, w3i, w4, w5 = [], [], [], [], [], []
    for a in range(NPY):
        to = [16 * ((a + r) % 4) + i16 for r in range(4)]
        frm = [16 * ((a - r) % 4) + i16 for r in range(4)]
        out = np.stack([fwd[:, k] for k in to]).reshape(4, 2, 4, 4, 2, N)
        w1.append(out.transpose(4, 5, 0, 2, 3, 1).reshape(128, 128))
        inn = np.stack([inv[:, :, :, k] for k in frm]).reshape(4, 2, N, 2, 4, 4)
        w5.append(inn.transpose(4, 0, 5, 3, 1, 2).reshape(128, 128))
        for b in range(NPZ):
            half = [32 * (b ^ q) + i32 for q in range(2)]
            m = np.stack([fwd[:, k] for k in half])
            m = np.stack([m[..., y] for y in frm])
            w2.append(m.transpose(1, 2, 3, 0, 4, 5).reshape(128, 128))
            m = np.stack([inv[:, y] for y in to])
            m = np.stack([m[..., k] for k in half])
            w4.append(m.transpose(1, 2, 3, 0, 4, 5).reshape(128, 128))
    for b in range(NPZ):
        half = [32 * (b ^ q) + i32 for q in range(2)]
        m = np.stack([fwd[..., z] for z in half])
        w3.append(m.transpose(0, 3, 4, 1, 2).reshape(128, 128))
        m = np.stack([inv[:, z] for z in half])
        w3i.append(m.transpose(3, 4, 0, 1, 2).reshape(128, 128))
    return [np.stack([split_np(w) for w in ws]) for ws in (w1, w2, w3, w3i, w4, w5)]


def split3(x):
    hi = x.astype(BF16)
    rest = x - hi.astype(F32)
    mid = rest.astype(BF16)
    return hi, mid, (rest - mid.astype(F32)).astype(BF16)


def dot(a, b):
    return jnp.dot(a, b, preferred_element_type=F32)


def left(w, x):
    hi, mid, lo = split3(x)
    wide = dot(w[0][...], jnp.concatenate([hi, mid], 0))
    return wide[:128] + (wide[128:] + dot(w[1][...], jnp.concatenate([hi, lo], 0)))


def right(x, w):
    hi, mid, lo = split3(x)
    wide = dot(jnp.concatenate([hi, mid], 1), w[0][...])
    return wide[:, :128] + (wide[:, 128:] + dot(jnp.concatenate([hi, lo], 1), w[1][...]))


def left_table(w1, w2, w3):
    pairs = [jnp.concatenate([a, b], 1) for a, b in ((w1, w1), (w2, w2), (w3, w1))]
    return jnp.concatenate(pairs[:2], 0), pairs[2]


def right_table(w1, w2, w3):
    return jnp.concatenate([jnp.concatenate([w1, w2], 1)] * 2, 0), jnp.concatenate([w3, w1], 1)


def from_wide(w):
    return jnp.concatenate([w[:, :128], w[:, 128:]], 0)


def swap_lanes(tiles):
    lane = lax.broadcasted_iota(jnp.int32, tiles[0].shape, 1)
    odd, high = (lane // 32) % 2 == 1, lane >= 64
    t = list(tiles)
    for lo in (0, 2):
        a, b = t[lo], t[lo + 1]
        t[lo] = jnp.where(odd, pltpu.roll(b, 32, 1), a)
        t[lo + 1] = jnp.where(odd, b, pltpu.roll(a, 96, 1))
    for lo in (0, 1):
        a, b = t[lo], t[lo + 2]
        t[lo] = jnp.where(high, pltpu.roll(b, 64, 1), a)
        t[lo + 2] = jnp.where(high, b, pltpu.roll(a, 64, 1))
    return t


def kernel(rho_re, rho_im, g_re, g_im, t1, t2, t3, t3i, t4, t5, d_recv, hat,
           rin, gin, wraw, wbig, wsmall, ga, gb, a_send, a_recv, b_send, b_recv, c_send, c_recv, d_send,
           in_sem, g_sem, w_sem, as_sem, ar_sem, bs_sem, br_sem, cs_sem, cr_sem, ds_sem, dr_sem):
    me, mz = lax.axis_index("py"), lax.axis_index("pz")
    zero = lax.axis_index("dp")

    def py_peer(r):
        return (zero, mz, lax.rem(me + r, NPY))

    pz_peer = (zero, 1 - mz, me)

    def load_in(g):
        slot = lax.rem(g, 2)
        return [pltpu.make_async_copy(src.at[pl.ds(g * FG, FG)], rin.at[slot, i], in_sem.at[slot, i])
                for i, src in enumerate((rho_re, rho_im))]

    barrier = pltpu.get_barrier_semaphore()
    for peer in [py_peer(r) for r in (1, 2, 3)] + [pz_peer]:
        pl.semaphore_signal(barrier, inc=1, device_id=peer, device_id_type=MESH)
    both = me * NPZ + mz
    tabs = [pltpu.make_async_copy(t.at[i], wraw.at[k], w_sem.at[k])
            for k, (t, i) in enumerate(((t1, me), (t2, both), (t3, mz), (t3i, mz), (t4, both), (t5, me)))]
    greens = [pltpu.make_async_copy(src, gin.at[i], g_sem.at[i]) for i, src in enumerate((g_re, g_im))]
    for cp in tabs[:1] + load_in(0) + tabs[1:] + greens + load_in(1):
        cp.start()

    def table(k):
        tabs[k].wait()
        wide, narrow = (left_table if k in (1, 4) else right_table)(*(wraw[k, i] for i in range(3)))
        wbig[k] = wide
        wsmall[k] = narrow

    def lmat(k):
        return wbig.at[k], wsmall.at[k]

    def rmat(k):
        return wbig[k], from_wide(wsmall[k])

    def stage1(g, y0, ny):
        slot, ring = lax.rem(g, 2), lax.rem(g, RA)
        w = rmat(0)
        for i in range(ny):
            y = y0 + i
            x = jnp.concatenate([rin[slot, 0, :, y].reshape(128, N), rin[slot, 1, :, y].reshape(128, N)], 1)
            out = right(x, w).T
            rows = pl.ds(pl.multiple_of(y * 8, 8), 8)
            for c in range(4):
                for r in range(4):
                    tile = out[(r * 4 + c) * 8:(r * 4 + c + 1) * 8]
                    if r == 0:
                        a_recv[g * 4 + c, 0, rows, :] = tile
                    else:
                        a_send[ring, c, r - 1, rows, :] = tile

    def a_copy(u, r):
        g, c = u // 4, lax.rem(u, 4)
        ring = lax.rem(g, RA)
        return pltpu.make_async_remote_copy(
            src_ref=a_send.at[ring, c, r - 1], dst_ref=a_recv.at[u, r], send_sem=as_sem.at[ring],
            recv_sem=ar_sem.at[u], device_id=py_peer(r), device_id_type=MESH)

    def a_sent(g):
        ring = lax.rem(g, RA)
        return pltpu.make_async_copy(a_send.at[ring], a_send.at[ring], as_sem.at[ring])

    def a_arrived(u):
        ref = a_recv.at[u, pl.ds(1, 3)]
        return pltpu.make_async_copy(ref, ref, ar_sem.at[u])

    def d_sent(u):
        ring = lax.rem(u, RING)
        return pltpu.make_async_copy(d_send.at[ring], d_send.at[ring], ds_sem.at[ring])

    def d_arrived(g):
        ref = d_recv.at[pl.ds(g * 4, 4), pl.ds(1, 3)]
        return pltpu.make_async_copy(ref, ref, dr_sem.at[g])

    def b_copy(u):
        ring = lax.rem(u, RING)
        return pltpu.make_async_remote_copy(
            src_ref=b_send.at[ring], dst_ref=b_recv.at[u, 1], send_sem=bs_sem.at[ring], recv_sem=br_sem.at[ring],
            device_id=pz_peer, device_id_type=MESH)

    def c_copy(u):
        ring = lax.rem(u, RING)
        return pltpu.make_async_remote_copy(
            src_ref=c_send.at[ring], dst_ref=c_recv.at[u, 1], send_sem=cs_sem.at[ring], recv_sem=cr_sem.at[ring],
            device_id=pz_peer, device_id_type=MESH)

    def d_copy(u, r):
        ring = lax.rem(u, RING)
        return pltpu.make_async_remote_copy(
            src_ref=d_send.at[ring, r - 1], dst_ref=d_recv.at[u, r], send_sem=ds_sem.at[ring],
            recv_sem=dr_sem.at[u // 4], device_id=py_peer(r), device_id_type=MESH)

    def send_a(g):
        for c in range(4):
            for r in (2, 1, 3):
                a_copy(g * 4 + c, r).start()

    def stage2(u):
        a_arrived(u).wait()
        ring = lax.rem(u, RING)

        @pl.when(u >= RING)
        def _():
            b_copy(u - RING).wait_send()

        w = lmat(1)
        for kp in range(2):
            cols = [jnp.concatenate([a_recv[u, r, pl.ds(kk * 2 + ri, 16, stride=8), :]
                                     for r in range(4) for ri in range(2)], 0) for kk in (2 * kp, 2 * kp + 1)]
            out = left(w, jnp.concatenate(cols, 1))
            for i in range(2):
                kk = 2 * kp + i
                b_recv[u, 0, kk] = out[:64, i * 128:(i + 1) * 128]
                b_send[ring, kk] = out[64:, i * 128:(i + 1) * 128]
        b_copy(u).start()

    def stage3(u):
        b_copy(u).wait_recv()
        ring, c, f0 = lax.rem(u, RING), lax.rem(u, 4), u // 4 * FG

        @pl.when(u >= RING)
        def _():
            c_copy(u - RING).wait_send()

        wf, wi = rmat(2), rmat(3)
        for kp in range(2):
            rows = []
            for kk in (2 * kp, 2 * kp + 1):
                rows += swap_lanes([b_recv[u, q, kk, ri * 32:(ri + 1) * 32, :] for q in range(2) for ri in range(2)])
            spec = right(jnp.concatenate(rows, 0), wf)
            hats = []
            for i in range(2):
                kk = 2 * kp + i
                gr = pl.ds(pl.multiple_of((c * 4 + kk) * 32, 32), 32)
                gan, gbn = ga[gr, :], gb[gr, :]
                for f in range(FG):
                    s = spec[(i * FG + f) * 32:(i * FG + f + 1) * 32]
                    h = s * gan + pltpu.roll(s, 64, 1) * gbn
                    hat[f0 + f, c * 4 + kk] = h
                    hats.append(h)
            back = right(jnp.concatenate(hats, 0), wi)
            for i in range(2):
                kk = 2 * kp + i
                t = swap_lanes([back[(i * FG + f) * 32:(i * FG + f + 1) * 32] for f in range(FG)])
                for ri in range(2):
                    c_recv[u, 0, kk, ri * 32:(ri + 1) * 32, :] = t[ri]
                    c_send[ring, kk, ri * 32:(ri + 1) * 32, :] = t[2 + ri]
        c_copy(u).start()

    def stage4(u):
        c_copy(u).wait_recv()
        ring = lax.rem(u, RING)

        @pl.when(u >= RING)
        def _():
            d_sent(u - RING).wait()

        w = lmat(4)
        for kp in range(2):
            cols = [jnp.concatenate([c_recv[u, q, kk] for q in range(2)], 0) for kk in (2 * kp, 2 * kp + 1)]
            out = left(w, jnp.concatenate(cols, 1))
            for i in range(2):
                kk = 2 * kp + i
                for r in range(4):
                    for ro in range(2):
                        rows = pl.ds(kk * 2 + ro, 16, stride=8)
                        tile = out[(r * 2 + ro) * 16:(r * 2 + ro + 1) * 16, i * 128:(i + 1) * 128]
                        if r == 0:
                            d_recv[u, 0, rows, :] = tile
                        else:
                            d_send[ring, r - 1, rows, :] = tile
        for r in (2, 1, 3):
            d_copy(u, r).start()

    def stage5(g, y0, ny):
        w = rmat(5)
        for i in range(ny):
            y = y0 + i
            rows = pl.ds(pl.multiple_of(y * 8, 8), 8)
            x = jnp.concatenate([d_recv[g * 4 + c, r, rows, :] for c in range(4) for r in range(4)], 0)
            out = right(x.T, w)
            for f in range(FG):
                for r in range(4):
                    d_recv[g * 4 + f, r, rows, :] = out[(f * 4 + r) * 8:(f * 4 + r + 1) * 8]

    table(0)
    for g in range(2):
        for cp in load_in(g):
            cp.wait()

        @pl.loop(0, 4)
        def _(q, g=g):
            stage1(g, q * 4, 4)

        if g == 0:
            pl.semaphore_wait(barrier, 4)
        send_a(g)
        for cp in load_in(g + 2):
            cp.start()
        if g == 0:
            for k in range(1, 6):
                table(k)
            for cp in greens:
                cp.wait()
            gr, gi = gin[0].reshape(512, N), gin[1].reshape(512, N)
            ga[...] = jnp.concatenate([gr, gr], 1)
            gb[...] = jnp.concatenate([-gi, gi], 1)

    def step(t, carry):
        c = lax.rem(t, 4)
        g1 = t // 4 + 2

        @pl.when(t < NU)
        def _():
            stage2(t)

        u3 = t - LAG3

        @pl.when(jnp.logical_and(u3 >= 0, u3 < NU))
        def _():
            stage3(u3)

        u4 = t - LAG4

        @pl.when(jnp.logical_and(u4 >= 0, u4 < NU))
        def _():
            stage4(u4)

        @pl.when(g1 < NG)
        def _():
            @pl.when(c == 0)
            def _():
                for cp in load_in(g1):
                    cp.wait()

                @pl.when(g1 >= RA)
                def _():
                    a_sent(g1 - RA).wait()

            stage1(g1, c * 4, 4)

            @pl.when(c == 3)
            def _():
                send_a(g1)

                @pl.when(g1 + 2 < NG)
                def _():
                    for cp in load_in(g1 + 2):
                        cp.start()

        u5 = t - LAG5
        g5 = u5 // 4
        c5 = lax.rem(u5 + 16, 4)

        @pl.when(u5 >= 0)
        def _():
            @pl.when(c5 == 0)
            def _():
                d_arrived(g5).wait()

            stage5(g5, c5 * 4, 4)

        return carry

    lax.fori_loop(0, NU + LAG4, step, 0)
    stage5(NG - 2, 12, 4)
    d_arrived(NG - 1).wait()

    for g in range(NG - RA, NG):
        a_sent(g).wait()
    for u in range(NU - RING, NU):
        b_copy(u).wait_send()
        c_copy(u).wait_send()
        d_sent(u).wait()


def unpack(phi, hat, t5, phi_re, phi_im, hat_re, hat_im, wraw, st, w_sem, sem):
    tab = pltpu.make_async_copy(t5.at[lax.axis_index("py")], wraw, w_sem)
    tab.start()

    def copy(outs, n, i, k):
        return pltpu.make_async_copy(st.at[lax.rem(n, SLOTS), k], outs[k].at[pl.ds(i * FB, FB)],
                                     sem.at[lax.rem(n, SLOTS), k])

    hats, phis = (hat_re, hat_im), (phi_re, phi_im)
    jobs = FIELDS // FB

    def free(n):
        @pl.when(n >= SLOTS)
        def _():
            for k in range(2):
                copy(hats, n - SLOTS, 0, k).wait()

    def hat_job(i, carry):
        slot = lax.rem(i, SLOTS)
        free(i)
        for f in range(FB):
            h = hat[i * FB + f].reshape(512, 128)
            st[slot, 0, f] = h[:, :N].reshape(16, 32, N)
            st[slot, 1, f] = h[:, N:].reshape(16, 32, N)
        for k in range(2):
            copy(hats, i, i, k).start()
        return carry

    def phi_job(i, carry):
        n = i + jobs
        slot = lax.rem(n, SLOTS)
        free(n)
        for f in range(FB):
            for r in range(4):
                p = phi[i * FB + f, r]
                st[slot, 0, f, :, r * 8:(r + 1) * 8] = p[:, :N].reshape(16, 8, N)
                st[slot, 1, f, :, r * 8:(r + 1) * 8] = p[:, N:].reshape(16, 8, N)
        for k in range(2):
            copy(phis, n, i, k).start()
        return carry

    last = jobs - FG // FB
    lax.fori_loop(0, jobs, hat_job, 0)
    lax.fori_loop(0, last, phi_job, 0)
    tab.wait()
    wide, narrow = right_table(*(wraw[i] for i in range(3)))
    w = wide, from_wide(narrow)
    for j in range(FG // FB):
        free(jobs + last + j)

    @pl.loop(0, 4)
    def _(q):
        for i in range(4):
            y = q * 4 + i
            rows = pl.ds(pl.multiple_of(y * 8, 8), 8)
            x = jnp.concatenate([phi[NU - 4 + c, r, rows, :] for c in range(4) for r in range(4)], 0)
            out = right(x.T, w)
            for f in range(FG):
                slot = (jobs + last + f // FB) % SLOTS
                st[slot, 0, f % FB, y] = out[f * 32:(f + 1) * 32, :N]
                st[slot, 1, f % FB, y] = out[f * 32:(f + 1) * 32, N:]

    for j in range(FG // FB):
        for k in range(2):
            copy(phis, jobs + last + j, last + j, k).start()
    for n in range(2 * jobs - SLOTS, 2 * jobs):
        for k in range(2):
            copy(hats, n, 0, k).wait()


def solution(mesh):
    consts = tables()

    def local_solve(rho_re, rho_im, g_re, g_im):
        dma, vmem, hbm = pltpu.SemaphoreType.DMA, pltpu.VMEM, pl.BlockSpec(memory_space=pl.ANY)
        tabs = [jnp.asarray(c) for c in consts]
        field = jax.ShapeDtypeStruct((FIELDS, 16, 32, N), F32)
        phi, hat = pl.pallas_call(
            kernel,
            out_shape=[pltpu.VMEM((NU, 4, 128, 128), F32), pltpu.VMEM((FIELDS, 16, 32, 128), F32)],
            in_specs=[hbm] * 10,
            out_specs=[pl.BlockSpec(memory_space=pltpu.VMEM)] * 2,
            scratch_shapes=[
                vmem((2, 2, FG, 16, 32, N), F32),
                vmem((2, 16, 32, N), F32),
                vmem((6, 3, 128, 128), BF16),
                vmem((6, 256, 256), BF16),
                vmem((6, 128, 256), BF16),
                vmem((512, 128), F32), vmem((512, 128), F32),
                vmem((RA, 4, 3, 128, 128), F32),
                vmem((NU, 4, 128, 128), F32),
                vmem((RING, 4, 64, 128), F32),
                vmem((NU, 2, 4, 64, 128), F32),
                vmem((RING, 4, 64, 128), F32),
                vmem((NU, 2, 4, 64, 128), F32),
                vmem((RING, 3, 128, 128), F32),
                dma((2, 2)), dma((2,)), dma((6,)), dma((RA,)), dma((NU,)),
                dma((RING,)), dma((RING,)), dma((RING,)), dma((RING,)), dma((RING,)), dma((NG,)),
            ],
            compiler_params=pltpu.CompilerParams(collective_id=0, has_side_effects=True,
                                                 vmem_limit_bytes=44 * 2 ** 20),
            name="spectral",
        )(jnp.transpose(rho_re, (0, 2, 3, 1)), jnp.transpose(rho_im, (0, 2, 3, 1)), g_re, g_im, *tabs)
        phi, hat = (pltpu.with_memory_space_constraint(x, pltpu.VMEM) for x in (phi, hat))
        phi_re, phi_im, hat_re, hat_im = pl.pallas_call(
            unpack,
            out_shape=[field] * 4,
            in_specs=[pl.BlockSpec(memory_space=pltpu.VMEM)] * 2 + [hbm],
            out_specs=[hbm] * 4,
            scratch_shapes=[vmem((3, 128, 128), BF16), vmem((SLOTS, 2, FB, 16, 32, N), F32), dma, dma((SLOTS, 2))],
            compiler_params=pltpu.CompilerParams(vmem_limit_bytes=20 * 2 ** 20),
            name="unpack",
        )(phi, hat, tabs[5])
        return jnp.transpose(phi_re, (0, 3, 1, 2)), jnp.transpose(phi_im, (0, 3, 1, 2)), hat_re, hat_im

    space_layout = P("dp", None, "py", "pz")
    wave_layout = P("dp", "py", "pz", None)
    green_layout = P("py", "pz", None)
    return jax.shard_map(local_solve, mesh=mesh,
                         in_specs=(space_layout, space_layout, green_layout, green_layout),
                         out_specs=(space_layout, space_layout, wave_layout, wave_layout),
                         check_vma=False)
```

```python
import functools

import jax
import jax.numpy as jnp
import ml_dtypes
import numpy as np
from jax import lax
from jax.experimental import pallas as pl
from jax.experimental.pallas import tpu as pltpu
from jax.sharding import PartitionSpec as P

MESH = pl.DeviceIdType.MESH
F32, BF16 = jnp.float32, jnp.bfloat16
N = 64
FIELDS = 32
FG = 4
NG = FIELDS // FG
NU = NG * 4
NPY, NPZ = 4, 2
LAG3, LAG4 = 2, 4
LAG5 = LAG4 + 5
RING = 4
RECV = 8
RA = 3
EARLY = 2
LATE = 3
FB, SLOTS = 2, 8


def dft(sign):
    jk = np.outer(np.arange(N), np.arange(N)) % N
    c, s = np.cos(2 * np.pi * jk / N) / 8, sign * np.sin(2 * np.pi * jk / N) / 8
    return np.stack([np.stack([c, -s], 1), np.stack([s, c], 1)])


def split_np(w):
    w = np.asarray(w, np.float32)
    parts = []
    for _ in range(3):
        part = w.astype(ml_dtypes.bfloat16)
        parts.append(part)
        w = w - part.astype(np.float32)
    return np.stack(parts)


def tables():
    fwd, inv = dft(-1), dft(1)
    i16, i32 = np.arange(16), np.arange(32)
    w1, w2, w3, w3i, w4, w5 = [], [], [], [], [], []
    for a in range(NPY):
        to = [16 * ((a + r) % 4) + i16 for r in range(4)]
        frm = [16 * ((a - r) % 4) + i16 for r in range(4)]
        out = np.stack([fwd[:, k] for k in to]).reshape(4, 2, 4, 4, 2, N)
        w1.append(out.transpose(4, 5, 0, 2, 3, 1).reshape(128, 128))
        inn = np.stack([inv[:, :, :, k] for k in frm]).reshape(4, 2, N, 2, 4, 4)
        w5.append(inn.transpose(4, 0, 5, 3, 1, 2).reshape(128, 128))
        for b in range(NPZ):
            half = [32 * (b ^ q) + i32 for q in range(2)]
            m = np.stack([fwd[:, k] for k in half])
            m = np.stack([m[..., y] for y in frm])
            w2.append(m.transpose(1, 2, 3, 0, 4, 5).reshape(128, 128))
            m = np.stack([inv[:, y] for y in to])
            m = np.stack([m[..., k] for k in half])
            w4.append(m.transpose(1, 2, 3, 0, 4, 5).reshape(128, 128))
    for b in range(NPZ):
        half = [32 * (b ^ q) + i32 for q in range(2)]
        m = np.stack([fwd[..., z] for z in half])
        w3.append(m.transpose(0, 3, 4, 1, 2).reshape(128, 128))
        m = np.stack([inv[:, z] for z in half])
        w3i.append(m.transpose(3, 4, 0, 1, 2).reshape(128, 128))
    return [np.stack([split_np(w) for w in ws]) for ws in (w1, w2, w3, w3i, w4, w5)]


def split3(x):
    hi = x.astype(BF16)
    rest = x - hi.astype(F32)
    mid = rest.astype(BF16)
    return hi, mid, (rest - mid.astype(F32)).astype(BF16)


def dot(a, b):
    return jnp.dot(a, b, preferred_element_type=F32)


def left(w, x):
    hi, mid, lo = split3(x)
    wide = dot(w[0][...], jnp.concatenate([hi, mid], 0))
    return wide[:128] + (wide[128:] + dot(w[1][...], jnp.concatenate([hi, lo], 0)))


def right(x, w):
    hi, mid, lo = split3(x)
    wide = dot(jnp.concatenate([hi, mid], 1), w[0][...])
    return wide[:, :128] + (wide[:, 128:] + dot(jnp.concatenate([hi, lo], 1), w[1][...]))


def left_table(w1, w2, w3):
    pairs = [jnp.concatenate([a, b], 1) for a, b in ((w1, w1), (w2, w2), (w3, w1))]
    return jnp.concatenate(pairs[:2], 0), pairs[2]


def right_table(w1, w2, w3):
    return jnp.concatenate([jnp.concatenate([w1, w2], 1)] * 2, 0), jnp.concatenate([w3, w1], 1)


def from_wide(w):
    return jnp.concatenate([w[:, :128], w[:, 128:]], 0)


def swap_lanes(tiles):
    lane = lax.broadcasted_iota(jnp.int32, tiles[0].shape, 1)
    odd, high = (lane // 32) % 2 == 1, lane >= 64
    t = list(tiles)
    for lo in (0, 2):
        a, b = t[lo], t[lo + 1]
        t[lo] = jnp.where(odd, pltpu.roll(b, 32, 1), a)
        t[lo + 1] = jnp.where(odd, b, pltpu.roll(a, 96, 1))
    for lo in (0, 1):
        a, b = t[lo], t[lo + 2]
        t[lo] = jnp.where(high, pltpu.roll(b, 64, 1), a)
        t[lo + 2] = jnp.where(high, b, pltpu.roll(a, 64, 1))
    return t


def kernel(rho_re, rho_im, g_re, g_im, t1, t2, t3, t3i, t4, t5, d_recv, hat,
           rin, gin, wraw, wbig, wsmall, ga, gb, a_send, a_recv, b_send, b_recv, c_send, c_recv, d_send,
           in_sem, first_sem, g_sem, w_sem, as_sem, ar_sem, half_sem, bs_sem, br_sem, cs_sem, cr_sem, part_sem,
           ds_sem, dr_sem):
    me, mz = lax.axis_index("py"), lax.axis_index("pz")
    zero = lax.axis_index("dp")

    def py_peer(r):
        return (zero, mz, lax.rem(me + r, NPY))

    pz_peer = (zero, 1 - mz, me)

    def load_in(g):
        slot = lax.rem(g, 2)
        return [pltpu.make_async_copy(src.at[pl.ds(g * FG, FG)], rin.at[slot, i], in_sem.at[slot, i])
                for i, src in enumerate((rho_re, rho_im))]

    def load_first(q):
        ys = pl.ds(q * 4, 4)
        return [pltpu.make_async_copy(src.at[pl.ds(0, FG), ys], rin.at[0, i, :, ys], first_sem.at[q])
                for i, src in enumerate((rho_re, rho_im))]

    def first_loaded(q):
        ref = rin.at[0, :, :, pl.ds(q * 4, 4)]
        return pltpu.make_async_copy(ref, ref, first_sem.at[q])

    barrier = pltpu.get_barrier_semaphore()
    for peer in [py_peer(r) for r in (1, 2, 3)] + [pz_peer]:
        pl.semaphore_signal(barrier, inc=1, device_id=peer, device_id_type=MESH)
    both = me * NPZ + mz
    tabs = [pltpu.make_async_copy(t.at[i], wraw.at[k], w_sem.at[min(k, 1)])
            for k, (t, i) in enumerate(((t1, me), (t2, both), (t3, mz), (t3i, mz), (t4, both), (t5, me)))]
    greens = [pltpu.make_async_copy(src, gin.at[i], g_sem) for i, src in enumerate((g_re, g_im))]
    firsts = [cp for q in range(4) for cp in load_first(q)]
    for cp in tabs[:1] + firsts + tabs[1:] + greens + load_in(1):
        cp.start()

    def table(k):
        wide, narrow = (left_table if k in (1, 4) else right_table)(*(wraw[k, i] for i in range(3)))
        wbig[k] = wide
        wsmall[k] = narrow

    def lmat(k):
        return wbig.at[k], wsmall.at[k]

    def rmat(k):
        return wbig[k], from_wide(wsmall[k])

    def stage1(g, y0, ny):
        slot, ring = lax.rem(g, 2), lax.rem(g, RA)
        w = rmat(0)
        for i in range(ny):
            y = y0 + i
            x = jnp.concatenate([rin[slot, 0, :, y].reshape(128, N), rin[slot, 1, :, y].reshape(128, N)], 1)
            out = right(x, w).T
            rows = pl.ds(pl.multiple_of(y * 8, 8), 8)
            for c in range(4):
                for r in range(4):
                    tile = out[(r * 4 + c) * 8:(r * 4 + c + 1) * 8]
                    if r == 0:
                        a_recv[g * 4 + c, 0, rows, :] = tile
                    else:
                        a_send[ring, c, r - 1, rows, :] = tile

    def a_copy(u, r):
        g, c = u // 4, lax.rem(u, 4)
        ring = lax.rem(g, RA)
        return pltpu.make_async_remote_copy(
            src_ref=a_send.at[ring, c, r - 1], dst_ref=a_recv.at[u, r], send_sem=as_sem.at[ring],
            recv_sem=ar_sem.at[u], device_id=py_peer(r), device_id_type=MESH)

    def a_half(u, r, h, y0, ny):
        part = (pl.ds(y0, ny), pl.ds(4 * h, 4))
        src, dst = (ref.reshape(16, 8, 128).at[part] for ref in (a_send.at[0, u, r - 1], a_recv.at[u, r]))
        return pltpu.make_async_remote_copy(
            src_ref=src, dst_ref=dst, send_sem=as_sem.at[0], recv_sem=half_sem.at[u, h],
            device_id=py_peer(r), device_id_type=MESH)

    def half_arrived(u, h):
        ref = a_recv.at[u, pl.ds(1, 3), pl.ds(64 * h, 64)]
        return pltpu.make_async_copy(ref, ref, half_sem.at[u, h])

    def c_part(u, kk):
        ring = lax.rem(u, RING)
        return pltpu.make_async_remote_copy(
            src_ref=c_send.at[ring, kk], dst_ref=c_recv.at[u, 1, kk], send_sem=cs_sem.at[ring],
            recv_sem=part_sem.at[u - (NU - LATE), kk], device_id=pz_peer, device_id_type=MESH)

    def d_part(u, r, kk):
        part = (slice(None), pl.ds(2 * kk, 2))
        src, dst = (ref.reshape(16, 8, 128).at[part] for ref in (d_send.at[u % RING, r - 1], d_recv.at[u, r]))
        return pltpu.make_async_remote_copy(
            src_ref=src, dst_ref=dst, send_sem=ds_sem.at[u % RING], recv_sem=dr_sem.at[NG - 1],
            device_id=py_peer(r), device_id_type=MESH)

    def a_sent(g):
        ring = lax.rem(g, RA)
        return pltpu.make_async_copy(a_send.at[ring], a_send.at[ring], as_sem.at[ring])

    def a_arrived(u):
        ref = a_recv.at[u, pl.ds(1, 3)]
        return pltpu.make_async_copy(ref, ref, ar_sem.at[u])

    def d_sent(u):
        ring = lax.rem(u, RING)
        return pltpu.make_async_copy(d_send.at[ring], d_send.at[ring], ds_sem.at[ring])

    def d_arrived(g):
        ref = d_recv.at[pl.ds(g * 4, 4), pl.ds(1, 3)]
        return pltpu.make_async_copy(ref, ref, dr_sem.at[g])

    def b_copy(u):
        ring = lax.rem(u, RING)
        return pltpu.make_async_remote_copy(
            src_ref=b_send.at[ring], dst_ref=b_recv.at[u, 1], send_sem=bs_sem.at[ring], recv_sem=br_sem.at[lax.rem(u, RECV)],
            device_id=pz_peer, device_id_type=MESH)

    def b_half(u, h):
        kk = pl.ds(2 * h, 2)
        return pltpu.make_async_remote_copy(
            src_ref=b_send.at[u, kk], dst_ref=b_recv.at[u, 1, kk], send_sem=bs_sem.at[u], recv_sem=br_sem.at[u],
            device_id=pz_peer, device_id_type=MESH)

    def c_copy(u):
        ring = lax.rem(u, RING)
        return pltpu.make_async_remote_copy(
            src_ref=c_send.at[ring], dst_ref=c_recv.at[u, 1], send_sem=cs_sem.at[ring], recv_sem=cr_sem.at[lax.rem(u, RECV)],
            device_id=pz_peer, device_id_type=MESH)

    def d_copy(u, r):
        ring = lax.rem(u, RING)
        return pltpu.make_async_remote_copy(
            src_ref=d_send.at[ring, r - 1], dst_ref=d_recv.at[u, r], send_sem=ds_sem.at[ring],
            recv_sem=dr_sem.at[u // 4], device_id=py_peer(r), device_id_type=MESH)

    def send_a(g):
        for c in range(4):
            for r in (2, 1, 3):
                a_copy(g * 4 + c, r).start()

    def y_lines(u, kp):
        ring = lax.rem(u, RING)
        cols = [jnp.concatenate([a_recv[u, r, pl.ds(kk * 2 + ri, 16, stride=8), :]
                                 for r in range(4) for ri in range(2)], 0) for kk in (2 * kp, 2 * kp + 1)]
        out = left(lmat(1), jnp.concatenate(cols, 1))
        for i in range(2):
            kk = 2 * kp + i
            b_recv[u, 0, kk] = out[:64, i * 128:(i + 1) * 128]
            b_send[ring, kk] = out[64:, i * 128:(i + 1) * 128]

    def stage2(u):
        a_arrived(u).wait()

        @pl.when(u >= RING)
        def _():
            b_copy(u - RING).wait_send()

        for kp in range(2):
            y_lines(u, kp)
        b_copy(u).start()

    def stage3(u):
        b_copy(u).wait_recv()
        ring, c, f0 = lax.rem(u, RING), lax.rem(u, 4), u // 4 * FG

        @pl.when(u >= RING)
        def _():
            c_copy(u - RING).wait_send()

        wf, wi = rmat(2), rmat(3)
        for kp in range(2):
            rows = []
            for kk in (2 * kp, 2 * kp + 1):
                rows += swap_lanes([b_recv[u, q, kk, ri * 32:(ri + 1) * 32, :] for q in range(2) for ri in range(2)])
            spec = right(jnp.concatenate(rows, 0), wf)
            hats = []
            for i in range(2):
                kk = 2 * kp + i
                gr = pl.ds(pl.multiple_of((c * 4 + kk) * 32, 32), 32)
                gan, gbn = ga[gr, :], gb[gr, :]
                for f in range(FG):
                    s = spec[(i * FG + f) * 32:(i * FG + f + 1) * 32]
                    h = s * gan + pltpu.roll(s, 64, 1) * gbn
                    hat[f0 + f, c * 4 + kk] = h
                    hats.append(h)
            back = right(jnp.concatenate(hats, 0), wi)
            for i in range(2):
                kk = 2 * kp + i
                t = swap_lanes([back[(i * FG + f) * 32:(i * FG + f + 1) * 32] for f in range(FG)])
                for ri in range(2):
                    c_recv[u, 0, kk, ri * 32:(ri + 1) * 32, :] = t[ri]
                    c_send[ring, kk, ri * 32:(ri + 1) * 32, :] = t[2 + ri]

        @pl.when(u < NU - LATE)
        def _():
            c_copy(u).start()

        @pl.when(u >= NU - LATE)
        def _():
            for kk in range(4):
                c_part(u, kk).start()

    def y_lines_back(u, kks):
        ring = lax.rem(u, RING)
        cols = [jnp.concatenate([c_recv[u, q, kk] for q in range(2)], 0) for kk in kks]
        out = left(lmat(4), jnp.concatenate(cols, 1))
        for i, kk in enumerate(kks):
            for r in range(4):
                for ro in range(2):
                    rows = pl.ds(kk * 2 + ro, 16, stride=8)
                    tile = out[(r * 2 + ro) * 16:(r * 2 + ro + 1) * 16, i * 128:(i + 1) * 128]
                    if r == 0:
                        d_recv[u, 0, rows, :] = tile
                    else:
                        d_send[ring, r - 1, rows, :] = tile

    def stage4(u):
        c_copy(u).wait_recv()

        @pl.when(u >= RING)
        def _():
            d_sent(u - RING).wait()

        for kp in range(2):
            y_lines_back(u, (2 * kp, 2 * kp + 1))
        for r in (2, 1, 3):
            d_copy(u, r).start()

    def stage5(g, y0, ny):
        w = rmat(5)
        for i in range(ny):
            y = y0 + i
            rows = pl.ds(pl.multiple_of(y * 8, 8), 8)
            x = jnp.concatenate([d_recv[g * 4 + c, r, rows, :] for c in range(4) for r in range(4)], 0)
            out = right(x.T, w)
            for f in range(FG):
                for r in range(4):
                    d_recv[g * 4 + f, r, rows, :] = out[(f * 4 + r) * 8:(f * 4 + r + 1) * 8]

    tabs[0].wait()
    table(0)
    for q in range(4):
        first_loaded(q).wait()
        stage1(0, q * 4, 4)
        if q == 0:
            pl.semaphore_wait(barrier, 4)
        for r in (2, 1, 3):
            a_half(0, r, 0, q * 4, 4).start()
    for u, h in [(0, 1)] + [(u, h) for u in range(1, EARLY) for h in range(2)]:
        for r in (2, 1, 3):
            a_half(u, r, h, 0, 16).start()
    for u in range(EARLY, 4):
        for r in (2, 1, 3):
            a_copy(u, r).start()
    for cp in load_in(2):
        cp.start()
    pltpu.make_async_copy(wraw.at[pl.ds(1, 5)], wraw.at[pl.ds(1, 5)], w_sem.at[1]).wait()
    for k in range(1, 6):
        table(k)
    pltpu.make_async_copy(gin, gin, g_sem).wait()
    gr, gi = gin[0].reshape(512, N), gin[1].reshape(512, N)
    ga[...] = jnp.concatenate([gr, gr], 1)
    gb[...] = jnp.concatenate([-gi, gi], 1)
    for cp in load_in(1):
        cp.wait()

    @pl.loop(0, 4)
    def _(q):
        stage1(1, q * 4, 4)

    send_a(1)
    for cp in load_in(3):
        cp.start()
    for u in range(EARLY):
        for h in range(2):
            half_arrived(u, h).wait()
            y_lines(u, h)
            b_half(u, h).start()
    stage3(0)

    def inputs_of(g):
        for cp in load_in(g):
            cp.wait()

    inputs_of(2)
    for q in range(EARLY):
        stage1(2, q * 4, 4)

    def step(t, carry):
        c = lax.rem(t, 4)
        g1 = t // 4 + 2

        @pl.when(t < NU)
        def _():
            stage2(t)

        u3 = t - LAG3

        @pl.when(u3 >= 1)
        def _():
            stage3(u3)

        u4 = t - LAG4

        @pl.when(u4 >= 0)
        def _():
            stage4(u4)

        @pl.when(g1 < NG)
        def _():
            @pl.when(c == 0)
            def _():
                inputs_of(g1)

                @pl.when(g1 >= RA)
                def _():
                    a_sent(g1 - RA).wait()

            stage1(g1, c * 4, 4)

            @pl.when(c == 3)
            def _():
                send_a(g1)

                @pl.when(g1 + 2 < NG)
                def _():
                    for cp in load_in(g1 + 2):
                        cp.start()

        u5 = t - LAG5

        @pl.when(u5 >= 0)
        def _():
            @pl.when(lax.rem(u5, 4) == 0)
            def _():
                d_arrived(u5 // 4).wait()

            stage5(u5 // 4, lax.rem(u5, 4) * 4, 4)

        return carry

    steps = NU - LATE + LAG4
    lax.fori_loop(EARLY, steps, step, 0)
    rest = [u5 for u5 in range(steps - LAG5, NU - 4)]
    u3 = [u for u in range(steps - LAG3, NU)]
    for u in range(NU - LATE, NU):
        if u3:
            stage3(u3.pop(0))
        d_sent(u - RING).wait()
        for kk in range(4):
            c_part(u, kk).wait_recv()
            y_lines_back(u, (kk,))
            for r in (2, 1, 3):
                d_part(u, r, kk).start()
        for u5 in rest[:2]:
            if u5 % 4 == 0:
                d_arrived(u5 // 4).wait()
            stage5(u5 // 4, u5 % 4 * 4, 4)
        rest = rest[2:]
    d_arrived(NG - 1).wait()

    for g in range(NG - RA, NG):
        a_sent(g).wait()
    for u in range(NU - RING, NU):
        b_copy(u).wait_send()
        c_copy(u).wait_send()
        d_sent(u).wait()


def unpack(phi, hat, t5, phi_re, phi_im, hat_re, hat_im, wraw, st, st_last, w_sem, sem, last_sem):
    tab = pltpu.make_async_copy(t5.at[lax.axis_index("py")], wraw, w_sem)
    tab.start()

    def copy(outs, n, i, k):
        return pltpu.make_async_copy(st.at[lax.rem(n, SLOTS), k], outs[k].at[pl.ds(i * FB, FB)],
                                     sem.at[lax.rem(n, SLOTS), k])

    hats, phis = (hat_re, hat_im), (phi_re, phi_im)
    jobs = FIELDS // FB

    def free(n):
        @pl.when(n >= SLOTS)
        def _():
            for k in range(2):
                copy(hats, n - SLOTS, 0, k).wait()

    def hat_job(i, carry):
        slot = lax.rem(i, SLOTS)
        free(i)
        for f in range(FB):
            h = hat[i * FB + f].reshape(512, 128)
            st[slot, 0, f] = h[:, :N].reshape(16, 32, N)
            st[slot, 1, f] = h[:, N:].reshape(16, 32, N)
        for k in range(2):
            copy(hats, i, i, k).start()
        return carry

    def phi_job(i, carry):
        n = i + jobs
        slot = lax.rem(n, SLOTS)
        free(n)
        for f in range(FB):
            for r in range(4):
                p = phi[i * FB + f, r]
                st[slot, 0, f, :, r * 8:(r + 1) * 8] = p[:, :N].reshape(16, 8, N)
                st[slot, 1, f, :, r * 8:(r + 1) * 8] = p[:, N:].reshape(16, 8, N)
        for k in range(2):
            copy(phis, n, i, k).start()
        return carry

    def last_copy(k):
        return pltpu.make_async_copy(st_last.at[k], phis[k].at[pl.ds(FIELDS - FG, FG)], last_sem.at[k])

    lax.fori_loop(0, jobs, hat_job, 0)
    tab.wait()
    wide, narrow = right_table(*(wraw[i] for i in range(3)))
    w = wide, from_wide(narrow)

    @pl.loop(0, 4)
    def _(q):
        for i in range(4):
            y = q * 4 + i
            rows = pl.ds(pl.multiple_of(y * 8, 8), 8)
            x = jnp.concatenate([phi[NU - 4 + c, r, rows, :] for c in range(4) for r in range(4)], 0)
            out = right(x.T, w)
            st_last[0, :, y] = out[:, :N].reshape(FG, 32, N)
            st_last[1, :, y] = out[:, N:].reshape(FG, 32, N)

    for k in range(2):
        last_copy(k).start()
    ends = jobs + jobs - FG // FB
    lax.fori_loop(0, ends - jobs, phi_job, 0)
    for k in range(2):
        last_copy(k).wait()
    for n in range(ends - SLOTS, ends):
        for k in range(2):
            copy(hats, n, 0, k).wait()


def solution(mesh):
    consts = tables()

    def local_solve(rho_re, rho_im, g_re, g_im):
        dma, vmem, hbm = pltpu.SemaphoreType.DMA, pltpu.VMEM, pl.BlockSpec(memory_space=pl.ANY)
        tabs = [jnp.asarray(c) for c in consts]
        field = jax.ShapeDtypeStruct((FIELDS, 16, 32, N), F32)
        phi, hat = pl.pallas_call(
            kernel,
            out_shape=[pltpu.VMEM((NU, 4, 128, 128), F32), pltpu.VMEM((FIELDS, 16, 32, 128), F32)],
            in_specs=[hbm] * 10,
            out_specs=[pl.BlockSpec(memory_space=pltpu.VMEM)] * 2,
            scratch_shapes=[
                vmem((2, 2, FG, 16, 32, N), F32),
                vmem((2, 16, 32, N), F32),
                vmem((6, 3, 128, 128), BF16),
                vmem((6, 256, 256), BF16),
                vmem((6, 128, 256), BF16),
                vmem((512, 128), F32), vmem((512, 128), F32),
                vmem((RA, 4, 3, 128, 128), F32),
                vmem((NU, 4, 128, 128), F32),
                vmem((RING, 4, 64, 128), F32),
                vmem((NU, 2, 4, 64, 128), F32),
                vmem((RING, 4, 64, 128), F32),
                vmem((NU, 2, 4, 64, 128), F32),
                vmem((RING, 3, 128, 128), F32),
                dma((2, 2)), dma((4,)), dma, dma((2,)), dma((RA,)), dma((NU,)), dma((EARLY, 2)),
                dma((RING,)), dma((RECV,)), dma((RING,)), dma((RECV,)), dma((LATE, 4)), dma((RING,)), dma((NG,)),
            ],
            compiler_params=pltpu.CompilerParams(collective_id=0, has_side_effects=True,
                                                 vmem_limit_bytes=44 * 2 ** 20),
            name="spectral",
        )(jnp.transpose(rho_re, (0, 2, 3, 1)), jnp.transpose(rho_im, (0, 2, 3, 1)), g_re, g_im, *tabs)
        phi, hat = (pltpu.with_memory_space_constraint(x, pltpu.VMEM) for x in (phi, hat))
        phi_re, phi_im, hat_re, hat_im = pl.pallas_call(
            unpack,
            out_shape=[field] * 4,
            in_specs=[pl.BlockSpec(memory_space=pltpu.VMEM)] * 2 + [hbm],
            out_specs=[hbm] * 4,
            scratch_shapes=[vmem((3, 128, 128), BF16), vmem((SLOTS, 2, FB, 16, 32, N), F32),
                            vmem((2, FG, 16, 32, N), F32), dma, dma((SLOTS, 2)), dma((2,))],
            compiler_params=pltpu.CompilerParams(vmem_limit_bytes=20 * 2 ** 20),
            name="unpack",
        )(phi, hat, tabs[5])
        return jnp.transpose(phi_re, (0, 3, 1, 2)), jnp.transpose(phi_im, (0, 3, 1, 2)), hat_re, hat_im

    space_layout = P("dp", None, "py", "pz")
    wave_layout = P("dp", "py", "pz", None)
    green_layout = P("py", "pz", None)
    return jax.shard_map(local_solve, mesh=mesh,
                         in_specs=(space_layout, space_layout, green_layout, green_layout),
                         out_specs=(space_layout, space_layout, wave_layout, wave_layout),
                         check_vma=False)
```

```python
import functools

import jax
import jax.numpy as jnp
import ml_dtypes
import numpy as np
from jax import lax
from jax.experimental import pallas as pl
from jax.experimental.pallas import tpu as pltpu
from jax.sharding import PartitionSpec as P

MESH = pl.DeviceIdType.MESH
L, H, Z, Y, S, Q = 128, 64, 32, 16, 8, 4
F32, BF16 = jnp.float32, jnp.bfloat16
N = 64
FIELDS = 32
FG = 4
NG = FIELDS // FG
NU = NG * 4
NPY, NPZ = 4, 2
LAG3, LAG4 = 2, 4
LAG5 = LAG4 + 5
RING = 4
RECV = 6
RG = 4
RA = 3
AR = 16
EARLY = 2
LATE = 3
FB, SLOTS = 4, 4
HB = 8


def dft(sign):
    jk = np.outer(np.arange(N), np.arange(N)) % N
    c, s = np.cos(2 * np.pi * jk / N) / S, sign * np.sin(2 * np.pi * jk / N) / S
    return np.stack([np.stack([c, -s], 1), np.stack([s, c], 1)])


def split_np(w):
    w = np.asarray(w, np.float32)
    parts = []
    for _ in range(3):
        part = w.astype(ml_dtypes.bfloat16)
        parts.append(part)
        w = w - part.astype(np.float32)
    return np.stack(parts)


def tables():
    fwd, inv = dft(-1), dft(1)
    i16, i32 = np.arange(Y), np.arange(Z)
    w1, w2, w3, w3i, w4, w5 = [], [], [], [], [], []
    for a in range(NPY):
        to = [Y * ((a + r) % Q) + i16 for r in range(Q)]
        frm = [Y * ((a - r) % Q) + i16 for r in range(Q)]
        out = np.stack([fwd[:, k] for k in to]).reshape(Q, 2, Q, Q, 2, N)
        w1.append(out.transpose(Q, 5, 0, 2, 3, 1).reshape(L, L))
        inn = np.stack([inv[:, :, :, k] for k in frm]).reshape(Q, 2, N, 2, Q, Q)
        w5.append(inn.transpose(Q, 0, 5, 3, 1, 2).reshape(L, L))
        for b in range(NPZ):
            half = [Z * (b ^ q) + i32 for q in range(2)]
            m = np.stack([fwd[:, k] for k in half])
            m = np.stack([m[..., y] for y in frm])
            w2.append(m.transpose(1, 2, 3, 0, Q, 5).reshape(L, L))
            m = np.stack([inv[:, y] for y in to])
            m = np.stack([m[..., k] for k in half])
            w4.append(m.transpose(1, 2, 3, 0, Q, 5).reshape(L, L))
    for b in range(NPZ):
        half = [Z * (b ^ q) + i32 for q in range(2)]
        m = np.stack([fwd[..., z] for z in half])
        w3.append(m.transpose(0, 3, Q, 1, 2).reshape(L, L))
        m = np.stack([inv[:, z] for z in half])
        w3i.append(m.transpose(3, Q, 0, 1, 2).reshape(L, L))
    return [np.stack([split_np(w) for w in ws]) for ws in (w1, w2, w3, w3i, w4, w5)]


def split3(x):
    hi = x.astype(BF16)
    rest = x - hi.astype(F32)
    mid = rest.astype(BF16)
    return hi, mid, (rest - mid.astype(F32)).astype(BF16)


def dot(a, b):
    return jnp.dot(a, b, preferred_element_type=F32)


def left(w, x):
    hi, mid, lo = split3(x)
    wide = dot(w[0][...], jnp.concatenate([hi, mid], 0))
    return wide[:L] + (wide[L:] + dot(w[1][...], jnp.concatenate([hi, lo], 0)))


def right(x, w):
    hi, mid, lo = split3(x)
    wide = dot(jnp.concatenate([hi, mid], 1), w[0][...])
    return wide[:, :L] + (wide[:, L:] + dot(jnp.concatenate([hi, lo], 1), w[1][...]))


def left_table(w1, w2, w3):
    pairs = [jnp.concatenate([a, b], 1) for a, b in ((w1, w1), (w2, w2), (w3, w1))]
    return jnp.concatenate(pairs[:2], 0), pairs[2]


def right_table(w1, w2, w3):
    return jnp.concatenate([jnp.concatenate([w1, w2], 1)] * 2, 0), jnp.concatenate([w3, w1], 1)


def from_wide(w):
    return jnp.concatenate([w[:, :L], w[:, L:]], 0)


def swap_lanes(tiles):
    lane = lax.broadcasted_iota(jnp.int32, tiles[0].shape, 1)
    odd, high = (lane // Z) % 2 == 1, lane >= H
    t = list(tiles)
    for lo in (0, 2):
        a, b = t[lo], t[lo + 1]
        t[lo] = jnp.where(odd, pltpu.roll(b, Z, 1), a)
        t[lo + 1] = jnp.where(odd, b, pltpu.roll(a, 96, 1))
    for lo in (0, 1):
        a, b = t[lo], t[lo + 2]
        t[lo] = jnp.where(high, pltpu.roll(b, H, 1), a)
        t[lo + 2] = jnp.where(high, b, pltpu.roll(a, H, 1))
    return t


def kernel(rho_re, rho_im, g_re, g_im, t1, t2, t3, t3i, t4, t5, d_recv, hat_re, hat_im,
           rin, gin, wraw, wbig, wsmall, ga, gb, a_send, a_recv, b_send, b_recv, c_send, c_recv, d_send,
           in_sem, first_sem, g_sem, w_sem, as_sem, ar_sem, half_sem, bh_sem, bs_sem, br_sem, cs_sem, cr_sem, part_sem,
           ds_sem, dr_sem):
    me, mz = lax.axis_index("py"), lax.axis_index("pz")
    zero = lax.axis_index("dp")

    def py_peer(r):
        return (zero, mz, lax.rem(me + r, NPY))

    pz_peer = (zero, 1 - mz, me)

    def load_in(g):
        slot = lax.rem(g, 2)
        return [pltpu.make_async_copy(src.at[pl.ds(g * FG, FG)], rin.at[slot, i], in_sem.at[slot])
                for i, src in enumerate((rho_re, rho_im))]

    def inputs_of(g):
        ref = rin.at[lax.rem(g, 2)]
        pltpu.make_async_copy(ref, ref, in_sem.at[lax.rem(g, 2)]).wait()

    def load_first(q):
        ys = pl.ds(q * Q, Q)
        return [pltpu.make_async_copy(src.at[pl.ds(0, FG), ys], rin.at[0, i, :, ys], first_sem.at[q])
                for i, src in enumerate((rho_re, rho_im))]

    def first_loaded(q):
        ref = rin.at[0, :, :, pl.ds(q * Q, Q)]
        return pltpu.make_async_copy(ref, ref, first_sem.at[q])

    barrier = pltpu.get_barrier_semaphore()
    for peer in [py_peer(r) for r in (1, 2, 3)] + [pz_peer]:
        pl.semaphore_signal(barrier, inc=1, device_id=peer, device_id_type=MESH)
    both = me * NPZ + mz
    tabs = [pltpu.make_async_copy(t.at[i], wraw.at[k], w_sem.at[min(k, 1)])
            for k, (t, i) in enumerate(((t1, me), (t2, both), (t3, mz), (t3i, mz), (t4, both), (t5, me)))]
    greens = [pltpu.make_async_copy(src, gin.at[i], g_sem) for i, src in enumerate((g_re, g_im))]
    firsts = [cp for q in range(Q) for cp in load_first(q)]
    for cp in tabs[:1] + firsts + tabs[1:] + greens + load_in(1):
        cp.start()

    def table(k):
        wide, narrow = (left_table if k in (1, Q) else right_table)(*(wraw[k, i] for i in range(3)))
        wbig[k] = wide
        wsmall[k] = narrow

    def lmat(k):
        return wbig.at[k], wsmall.at[k]

    def rmat(k):
        return wbig[k], from_wide(wsmall[k])

    def stage1(g, y0, ny):
        slot, ring = lax.rem(g, 2), lax.rem(g, RA)
        w = rmat(0)
        for i in range(ny):
            y = y0 + i
            x = jnp.concatenate([rin[slot, 0, :, y].reshape(L, N), rin[slot, 1, :, y].reshape(L, N)], 1)
            out = right(x, w).T
            rows = pl.ds(pl.multiple_of(y * S, S), S)
            for c in range(Q):
                for r in range(Q):
                    tile = out[(r * Q + c) * S:(r * Q + c + 1) * S]
                    if r == 0:
                        a_recv[lax.rem(g * Q + c, AR), 0, rows, :] = tile
                    else:
                        a_send[ring, c, r - 1, rows, :] = tile

    def a_copy(u, r):
        g, c = u // Q, lax.rem(u, Q)
        ring = lax.rem(g, RA)
        return pltpu.make_async_remote_copy(
            src_ref=a_send.at[ring, c, r - 1], dst_ref=a_recv.at[lax.rem(u, AR), r], send_sem=as_sem.at[ring],
            recv_sem=ar_sem.at[lax.rem(u, AR)], device_id=py_peer(r), device_id_type=MESH)

    def a_half(u, r, h, y0, ny):
        part = (pl.ds(y0, ny), pl.ds(Q * h, Q))
        src, dst = (ref.reshape(Y, S, L).at[part] for ref in (a_send.at[0, u, r - 1], a_recv.at[u, r]))
        return pltpu.make_async_remote_copy(
            src_ref=src, dst_ref=dst, send_sem=as_sem.at[0], recv_sem=half_sem.at[u, h],
            device_id=py_peer(r), device_id_type=MESH)

    def half_arrived(u, h):
        ref = a_recv.at[u, pl.ds(1, 3), pl.ds(H * h, H)]
        return pltpu.make_async_copy(ref, ref, half_sem.at[u, h])

    def c_part(u, kk):
        ring = lax.rem(u, RING)
        return pltpu.make_async_remote_copy(
            src_ref=c_send.at[ring, kk], dst_ref=c_recv.at[lax.rem(u, RECV), 1, kk], send_sem=cs_sem.at[ring],
            recv_sem=part_sem.at[u - (NU - LATE), kk], device_id=pz_peer, device_id_type=MESH)

    def d_part(u, r, kk):
        part = (slice(None), pl.ds(2 * kk, 2))
        src, dst = (ref.reshape(Y, S, L).at[part] for ref in (d_send.at[u % RING, r - 1], d_recv.at[u, r]))
        return pltpu.make_async_remote_copy(
            src_ref=src, dst_ref=dst, send_sem=ds_sem.at[u % RING], recv_sem=dr_sem.at[(NG - 1) % RG],
            device_id=py_peer(r), device_id_type=MESH)

    def a_sent(g):
        ring = lax.rem(g, RA)
        return pltpu.make_async_copy(a_send.at[ring], a_send.at[ring], as_sem.at[ring])

    def a_arrived(u):
        ref = a_recv.at[lax.rem(u, AR), pl.ds(1, 3)]
        return pltpu.make_async_copy(ref, ref, ar_sem.at[lax.rem(u, AR)])

    def d_sent(u):
        ring = lax.rem(u, RING)
        return pltpu.make_async_copy(d_send.at[ring], d_send.at[ring], ds_sem.at[ring])

    def d_arrived(g):
        ref = d_recv.at[pl.ds(g * Q, Q), pl.ds(1, 3)]
        return pltpu.make_async_copy(ref, ref, dr_sem.at[lax.rem(g, RG)])

    def b_copy(u):
        ring = lax.rem(u, RING)
        return pltpu.make_async_remote_copy(
            src_ref=b_send.at[ring], dst_ref=b_recv.at[lax.rem(u, RECV), 1], send_sem=bs_sem.at[ring], recv_sem=br_sem.at[lax.rem(u, RECV)],
            device_id=pz_peer, device_id_type=MESH)

    def b_half(u, h):
        kk = pl.ds(2 * h, 2)
        return pltpu.make_async_remote_copy(
            src_ref=b_send.at[u, kk], dst_ref=b_recv.at[lax.rem(u, RECV), 1, kk], send_sem=bs_sem.at[u],
            recv_sem=bh_sem.at[h] if u == 0 else br_sem.at[u], device_id=pz_peer, device_id_type=MESH)

    def bh_arrived(h):
        ref = b_recv.at[0, 1, pl.ds(2 * h, 2)]
        return pltpu.make_async_copy(ref, ref, bh_sem.at[h])

    def c_half(h):
        kk = pl.ds(2 * h, 2)
        return pltpu.make_async_remote_copy(
            src_ref=c_send.at[0, kk], dst_ref=c_recv.at[0, 1, kk], send_sem=cs_sem.at[0], recv_sem=cr_sem.at[0],
            device_id=pz_peer, device_id_type=MESH)

    def c_copy(u):
        ring = lax.rem(u, RING)
        return pltpu.make_async_remote_copy(
            src_ref=c_send.at[ring], dst_ref=c_recv.at[lax.rem(u, RECV), 1], send_sem=cs_sem.at[ring], recv_sem=cr_sem.at[lax.rem(u, RECV)],
            device_id=pz_peer, device_id_type=MESH)

    def d_copy(u, r):
        ring = lax.rem(u, RING)
        return pltpu.make_async_remote_copy(
            src_ref=d_send.at[ring, r - 1], dst_ref=d_recv.at[u, r], send_sem=ds_sem.at[ring],
            recv_sem=dr_sem.at[lax.rem(u // Q, RG)], device_id=py_peer(r), device_id_type=MESH)

    def send_a(g):
        for c in range(Q):
            for r in (2, 1, 3):
                a_copy(g * Q + c, r).start()

    def y_lines(u, kp):
        ring = lax.rem(u, RING)
        cols = [jnp.concatenate([a_recv[lax.rem(u, AR), r, pl.ds(kk * 2 + ri, Y, stride=S), :]
                                 for r in range(Q) for ri in range(2)], 0) for kk in (2 * kp, 2 * kp + 1)]
        out = left(lmat(1), jnp.concatenate(cols, 1))
        for i in range(2):
            kk = 2 * kp + i
            b_recv[lax.rem(u, RECV), 0, kk] = out[:H, i * L:(i + 1) * L]
            b_send[ring, kk] = out[H:, i * L:(i + 1) * L]

    def stage2(u):
        a_arrived(u).wait()

        @pl.when(u >= RING)
        def _():
            b_copy(u - RING).wait_send()

        for kp in range(2):
            y_lines(u, kp)
        b_copy(u).start()

    def z_lines(u, kp):
        ring, c, f0 = lax.rem(u, RING), lax.rem(u, Q), u // Q * FG
        wf, wi = rmat(2), rmat(3)
        rows = []
        for kk in (2 * kp, 2 * kp + 1):
            rows += swap_lanes([b_recv[lax.rem(u, RECV), q, kk, ri * Z:(ri + 1) * Z, :] for q in range(2) for ri in range(2)])
        spec = right(jnp.concatenate(rows, 0), wf)
        hats = []
        for i in range(2):
            kk = 2 * kp + i
            gr = pl.ds(pl.multiple_of((c * Q + kk) * Z, Z), Z)
            gan, gbn = ga[gr, :], gb[gr, :]
            for f in range(FG):
                s = spec[(i * FG + f) * Z:(i * FG + f + 1) * Z]
                h = s * gan + pltpu.roll(s, H, 1) * gbn
                hat_re[f0 + f, c * Q + kk] = h[:, :N]
                hat_im[f0 + f, c * Q + kk] = h[:, N:]
                hats.append(h)
        back = right(jnp.concatenate(hats, 0), wi)
        for i in range(2):
            kk = 2 * kp + i
            t = swap_lanes([back[(i * FG + f) * Z:(i * FG + f + 1) * Z] for f in range(FG)])
            for ri in range(2):
                c_recv[lax.rem(u, RECV), 0, kk, ri * Z:(ri + 1) * Z, :] = t[ri]
                c_send[ring, kk, ri * Z:(ri + 1) * Z, :] = t[2 + ri]

    def stage3(u):
        b_copy(u).wait_recv()

        @pl.when(u >= RING)
        def _():
            c_copy(u - RING).wait_send()

        for kp in range(2):
            z_lines(u, kp)

        @pl.when(u < NU - LATE)
        def _():
            c_copy(u).start()

        @pl.when(u >= NU - LATE)
        def _():
            for kk in range(Q):
                c_part(u, kk).start()

    def y_lines_back(u, kks):
        ring = lax.rem(u, RING)
        cols = [jnp.concatenate([c_recv[lax.rem(u, RECV), q, kk] for q in range(2)], 0) for kk in kks]
        out = left(lmat(Q), jnp.concatenate(cols, 1))
        for i, kk in enumerate(kks):
            for r in range(Q):
                for ro in range(2):
                    rows = pl.ds(kk * 2 + ro, Y, stride=S)
                    tile = out[(r * 2 + ro) * Y:(r * 2 + ro + 1) * Y, i * L:(i + 1) * L]
                    if r == 0:
                        d_recv[u, 0, rows, :] = tile
                    else:
                        d_send[ring, r - 1, rows, :] = tile

    def stage4(u):
        c_copy(u).wait_recv()

        @pl.when(u >= RING)
        def _():
            d_sent(u - RING).wait()

        for kp in range(2):
            y_lines_back(u, (2 * kp, 2 * kp + 1))
        for r in (2, 1, 3):
            d_copy(u, r).start()

    def stage5(g, y0, ny):
        w = rmat(5)
        for i in range(ny):
            y = y0 + i
            rows = pl.ds(pl.multiple_of(y * S, S), S)
            x = jnp.concatenate([d_recv[g * Q + c, r, rows, :] for c in range(Q) for r in range(Q)], 0)
            out = right(x.T, w)
            for f in range(FG):
                for r in range(Q):
                    d_recv[g * Q + f, r, rows, :] = out[(f * Q + r) * S:(f * Q + r + 1) * S]

    tabs[0].wait()
    table(0)
    for q in range(Q):
        first_loaded(q).wait()
        stage1(0, q * Q, Q)
        if q == 0:
            pl.semaphore_wait(barrier, Q)
        for r in (2, 1, 3):
            a_half(0, r, 0, q * Q, Q).start()
    for u, h in [(0, 1)] + [(u, h) for u in range(1, EARLY) for h in range(2)]:
        for r in (2, 1, 3):
            a_half(u, r, h, 0, Y).start()
    for u in range(EARLY, Q):
        for r in (2, 1, 3):
            a_copy(u, r).start()
    for cp in load_in(2):
        cp.start()
    pltpu.make_async_copy(wraw.at[pl.ds(1, 5)], wraw.at[pl.ds(1, 5)], w_sem.at[1]).wait()
    for k in range(1, 6):
        table(k)
    pltpu.make_async_copy(gin, gin, g_sem).wait()
    gr, gi = gin[0].reshape(512, N), gin[1].reshape(512, N)
    ga[...] = jnp.concatenate([gr, gr], 1)
    gb[...] = jnp.concatenate([-gi, gi], 1)
    inputs_of(1)

    @pl.loop(0, Q)
    def _(q):
        stage1(1, q * Q, Q)

    send_a(1)
    for cp in load_in(3):
        cp.start()
    for u in range(EARLY):
        for h in range(2):
            half_arrived(u, h).wait()
            y_lines(u, h)
            b_half(u, h).start()
    for h in range(2):
        bh_arrived(h).wait()
        z_lines(0, h)
        c_half(h).start()


    inputs_of(2)
    for q in range(EARLY):
        stage1(2, q * Q, Q)

    def step(t, carry):
        c = lax.rem(t, Q)
        g1 = t // Q + 2

        @pl.when(t < NU)
        def _():
            stage2(t)

        u3 = t - LAG3

        @pl.when(u3 >= 1)
        def _():
            stage3(u3)

        u4 = t - LAG4

        @pl.when(u4 >= 0)
        def _():
            stage4(u4)

        @pl.when(g1 < NG)
        def _():
            @pl.when(c == 0)
            def _():
                inputs_of(g1)

                @pl.when(g1 >= RA)
                def _():
                    a_sent(g1 - RA).wait()

            stage1(g1, c * Q, Q)

            @pl.when(c == 3)
            def _():
                send_a(g1)

                @pl.when(g1 + 2 < NG)
                def _():
                    for cp in load_in(g1 + 2):
                        cp.start()

        u5 = t - LAG5

        @pl.when(u5 >= 0)
        def _():
            @pl.when(lax.rem(u5, Q) == 0)
            def _():
                d_arrived(u5 // Q).wait()

            stage5(u5 // Q, lax.rem(u5, Q) * Q, Q)

        return carry

    steps = NU - LATE + LAG4
    lax.fori_loop(EARLY, steps, step, 0)
    rest = [u5 for u5 in range(steps - LAG5, NU - Q)]
    u3 = [u for u in range(steps - LAG3, NU)]
    for u in range(NU - LATE, NU):
        if u3:
            stage3(u3.pop(0))
        d_sent(u - RING).wait()
        for kk in range(Q):
            c_part(u, kk).wait_recv()
            y_lines_back(u, (kk,))
            for r in (2, 1, 3):
                d_part(u, r, kk).start()
        for u5 in rest[:2]:
            if u5 % Q == 0:
                d_arrived(u5 // Q).wait()
            stage5(u5 // Q, u5 % Q * Q, Q)
        rest = rest[2:]
    d_arrived(NG - 1).wait()

    for g in range(NG - RA, NG):
        a_sent(g).wait()
    for u in range(NU - RING, NU):
        b_copy(u).wait_send()
        c_copy(u).wait_send()
        d_sent(u).wait()


def unpack(phi, re, im, t5, phi_re, phi_im, hat_re, hat_im, wraw, st, st_last, w_sem, hat_sem, sem, last_sem):
    tab = pltpu.make_async_copy(t5.at[lax.axis_index("py")], wraw, w_sem)
    tab.start()
    hats, phis = ((re, hat_re), (im, hat_im)), (phi_re, phi_im)
    for i in range(FIELDS // HB):
        part = pl.ds(i * HB, HB)
        for k, (src, dst) in enumerate(hats):
            pltpu.make_async_copy(src.at[part], dst.at[part], hat_sem.at[k]).start()

    def last_copy(k):
        return pltpu.make_async_copy(st_last.at[k], phis[k].at[pl.ds(FIELDS - FG, FG)], last_sem.at[k])

    tab.wait()
    wide, narrow = right_table(*(wraw[i] for i in range(3)))
    w = wide, from_wide(narrow)

    @pl.loop(0, Q)
    def _(q):
        for i in range(Q):
            y = q * Q + i
            rows = pl.ds(pl.multiple_of(y * S, S), S)
            x = jnp.concatenate([phi[NU - Q + c, r, rows, :] for c in range(Q) for r in range(Q)], 0)
            out = right(x.T, w)
            for k, half in enumerate((out[:, :N], out[:, N:])):
                st_last[k, :, y] = half.reshape(FG, Z, N)

    for k in range(2):
        last_copy(k).start()

    def copy(i, k):
        slot = lax.rem(i, SLOTS)
        return pltpu.make_async_copy(st.at[slot, k], phis[k].at[pl.ds(i * FB, FB)], sem.at[slot, k])

    def phi_job(i, carry):
        slot = lax.rem(i, SLOTS)

        @pl.when(i >= SLOTS)
        def _():
            for k in range(2):
                copy(i - SLOTS, k).wait()

        for f in range(FB):
            for r in range(Q):
                p = phi[i * FB + f, r]
                for k, half in enumerate((p[:, :N], p[:, N:])):
                    st[slot, k, f, :, r * S:(r + 1) * S] = half.reshape(Y, S, N)
        for k in range(2):
            copy(i, k).start()
        return carry

    jobs = (FIELDS - FG) // FB
    lax.fori_loop(0, jobs, phi_job, 0)
    for k, (src, dst) in enumerate(hats):
        pltpu.make_async_copy(src, dst, hat_sem.at[k]).wait()
        last_copy(k).wait()
    for i in range(jobs - SLOTS, jobs):
        for k in range(2):
            copy(i, k).wait()


def in_hbm(x):
    return pltpu.with_memory_space_constraint(x, pltpu.HBM)


def solution(mesh):
    consts = tables()

    def local_solve(rho_re, rho_im, g_re, g_im):
        dma, vmem, hbm = pltpu.SemaphoreType.DMA, pltpu.VMEM, pl.BlockSpec(memory_space=pl.ANY)
        tabs = [jnp.asarray(c) for c in consts]
        field = jax.ShapeDtypeStruct((FIELDS, Y, Z, N), F32)
        packed = pl.pallas_call(
            kernel,
            out_shape=[pltpu.VMEM((NU, Q, L, L), F32)] + [pltpu.VMEM(field.shape, F32)] * 2,
            in_specs=[hbm] * 10,
            out_specs=[pl.BlockSpec(memory_space=pltpu.VMEM)] * 3,
            scratch_shapes=[
                vmem((2, 2, FG, Y, Z, N), F32),
                vmem((2, Y, Z, N), F32),
                vmem((6, 3, L, L), BF16),
                vmem((6, 256, 256), BF16),
                vmem((6, L, 256), BF16),
                vmem((512, L), F32), vmem((512, L), F32),
                vmem((RA, Q, 3, L, L), F32),
                vmem((AR, Q, L, L), F32),
                vmem((RING, Q, H, L), F32),
                vmem((RECV, 2, Q, H, L), F32),
                vmem((RING, Q, H, L), F32),
                vmem((RECV, 2, Q, H, L), F32),
                vmem((RING, 3, L, L), F32),
                dma((2,)), dma((Q,)), dma, dma((2,)), dma((RA,)), dma((AR,)), dma((EARLY, 2)), dma((2,)),
                dma((RING,)), dma((RECV,)), dma((RING,)), dma((RECV,)), dma((LATE, Q)), dma((RING,)), dma((RG,)),
            ],
            compiler_params=pltpu.CompilerParams(collective_id=0, has_side_effects=True,
                                                 vmem_limit_bytes=24 << 20),
            name="spectral",
        )(*(in_hbm(x) for x in (jnp.transpose(rho_re, (0, 2, 3, 1)), jnp.transpose(rho_im, (0, 2, 3, 1)), g_re, g_im, *tabs)))
        packed = [pltpu.with_memory_space_constraint(x, pltpu.VMEM) for x in packed]
        phi_re, phi_im, hat_re, hat_im = pl.pallas_call(
            unpack,
            out_shape=[field] * Q,
            in_specs=[pl.BlockSpec(memory_space=pltpu.VMEM)] * 3 + [hbm],
            out_specs=[hbm] * Q,
            scratch_shapes=[vmem((3, L, L), BF16), vmem((SLOTS, 2, FB, Y, Z, N), F32),
                            vmem((2, FG, Y, Z, N), F32), dma, dma((2,)), dma((SLOTS, 2)), dma((2,))],
            compiler_params=pltpu.CompilerParams(vmem_limit_bytes=20 << 20),
            name="unpack",
        )(*packed, in_hbm(tabs[5]))
        return jnp.transpose(phi_re, (0, 3, 1, 2)), jnp.transpose(phi_im, (0, 3, 1, 2)), hat_re, hat_im

    space_layout = P("dp", None, "py", "pz")
    wave_layout = P("dp", "py", "pz", None)
    green_layout = P("py", "pz", None)
    return jax.shard_map(local_solve, mesh=mesh,
                         in_specs=(space_layout, space_layout, green_layout, green_layout),
                         out_specs=(space_layout, space_layout, wave_layout, wave_layout),
                         check_vma=False)
```

```python
import functools

import jax
import jax.numpy as jnp
import ml_dtypes
import numpy as np
from jax import lax
from jax.experimental import pallas as pl
from jax.experimental.pallas import tpu as pltpu
from jax.sharding import PartitionSpec as P

MESH = pl.DeviceIdType.MESH
L, H, Z, Y, S, Q = 128, 64, 32, 16, 8, 4
F32, BF16 = jnp.float32, jnp.bfloat16
N = 64
FIELDS = 32
FG = 4
NG = FIELDS // FG
NU = NG * 4
NPY, NPZ = 4, 2
LAG3, LAG4 = 2, 4
LAG5 = LAG4 + 5
RING = 4
RECV = 6
RG = 4
RA = 3
AR = 16
BLOCKS = 2
NY = 16 // BLOCKS
EARLY = 2
PIECES = [(u, k) for u in range(EARLY) for k in range(4)]
LATE = 3
FB, SLOTS = 4, 4
HB = 8


def dft(sign):
    jk = np.outer(np.arange(N), np.arange(N)) % N
    c, s = np.cos(2 * np.pi * jk / N) / S, sign * np.sin(2 * np.pi * jk / N) / S
    return np.stack([np.stack([c, -s], 1), np.stack([s, c], 1)])


def split_np(w):
    w = np.asarray(w, np.float32)
    parts = []
    for _ in range(3):
        part = w.astype(ml_dtypes.bfloat16)
        parts.append(part)
        w = w - part.astype(np.float32)
    return np.stack(parts)


def tables():
    fwd, inv = dft(-1), dft(1)
    i16, i32 = np.arange(Y), np.arange(Z)
    w1, w2, w3, w3i, w4, w5 = [], [], [], [], [], []
    for a in range(NPY):
        to = [Y * ((a + r) % Q) + i16 for r in range(Q)]
        frm = [Y * ((a - r) % Q) + i16 for r in range(Q)]
        out = np.stack([fwd[:, k] for k in to]).reshape(Q, 2, Q, Q, 2, N)
        w1.append(out.transpose(Q, 5, 0, 2, 3, 1).reshape(L, L))
        inn = np.stack([inv[:, :, :, k] for k in frm]).reshape(Q, 2, N, 2, Q, Q)
        w5.append(inn.transpose(Q, 0, 5, 3, 1, 2).reshape(L, L))
        for b in range(NPZ):
            half = [Z * (b ^ q) + i32 for q in range(2)]
            m = np.stack([fwd[:, k] for k in half])
            m = np.stack([m[..., y] for y in frm])
            w2.append(m.transpose(1, 2, 3, 0, Q, 5).reshape(L, L))
            m = np.stack([inv[:, y] for y in to])
            m = np.stack([m[..., k] for k in half])
            w4.append(m.transpose(1, 2, 3, 0, Q, 5).reshape(L, L))
    for b in range(NPZ):
        half = [Z * (b ^ q) + i32 for q in range(2)]
        m = np.stack([fwd[..., z] for z in half])
        w3.append(m.transpose(0, 3, Q, 1, 2).reshape(L, L))
        m = np.stack([inv[:, z] for z in half])
        w3i.append(m.transpose(3, Q, 0, 1, 2).reshape(L, L))
    return [np.stack([split_np(w) for w in ws]) for ws in (w1, w2, w3, w3i, w4, w5)]


def split3(x):
    hi = x.astype(BF16)
    rest = x - hi.astype(F32)
    mid = rest.astype(BF16)
    return hi, mid, (rest - mid.astype(F32)).astype(BF16)


def dot(a, b):
    return jnp.dot(a, b, preferred_element_type=F32)


def left(w, x):
    hi, mid, lo = split3(x)
    wide = dot(w[0][...], jnp.concatenate([hi, mid], 0))
    return wide[:L] + (wide[L:] + dot(w[1][...], jnp.concatenate([hi, lo], 0)))


def right(x, w):
    hi, mid, lo = split3(x)
    wide = dot(jnp.concatenate([hi, mid], 1), w[0][...])
    return wide[:, :L] + (wide[:, L:] + dot(jnp.concatenate([hi, lo], 1), w[1][...]))


def left_table(w1, w2, w3):
    pairs = [jnp.concatenate([a, b], 1) for a, b in ((w1, w1), (w2, w2), (w3, w1))]
    return jnp.concatenate(pairs[:2], 0), pairs[2]


def right_table(w1, w2, w3):
    return jnp.concatenate([jnp.concatenate([w1, w2], 1)] * 2, 0), jnp.concatenate([w3, w1], 1)


def from_wide(w):
    return jnp.concatenate([w[:, :L], w[:, L:]], 0)


def swap_lanes(tiles):
    lane = lax.broadcasted_iota(jnp.int32, tiles[0].shape, 1)
    odd, high = (lane // Z) % 2 == 1, lane >= H
    t = list(tiles)
    for lo in (0, 2):
        a, b = t[lo], t[lo + 1]
        t[lo] = jnp.where(odd, pltpu.roll(b, Z, 1), a)
        t[lo + 1] = jnp.where(odd, b, pltpu.roll(a, 96, 1))
    for lo in (0, 1):
        a, b = t[lo], t[lo + 2]
        t[lo] = jnp.where(high, pltpu.roll(b, H, 1), a)
        t[lo + 2] = jnp.where(high, b, pltpu.roll(a, H, 1))
    return t


def kernel(rho_re, rho_im, g_re, g_im, t1, t2, t3, t3i, t4, t5, d_recv, hat_re, hat_im,
           rin, gin, wraw, wbig, wsmall, ga, gb, a_send, a_recv, b_send, b_recv, c_send, c_recv, d_send,
           in_sem, first_sem, g_sem, w_sem, as_sem, ar_sem, piece_sem, bh_sem, bs_sem, br_sem, cs_sem, cr_sem, part_sem,
           ds_sem, dr_sem):
    me, mz = lax.axis_index("py"), lax.axis_index("pz")
    zero = lax.axis_index("dp")

    def py_peer(r):
        return (zero, mz, lax.rem(me + r, NPY))

    pz_peer = (zero, 1 - mz, me)

    def load_in(g):
        slot = lax.rem(g, 2)
        return [pltpu.make_async_copy(src.at[pl.ds(g * FG, FG)], rin.at[slot, i], in_sem.at[slot])
                for i, src in enumerate((rho_re, rho_im))]

    def inputs_of(g):
        ref = rin.at[lax.rem(g, 2)]
        pltpu.make_async_copy(ref, ref, in_sem.at[lax.rem(g, 2)]).wait()

    def load_first(q):
        ys = pl.ds(q * NY, NY)
        return [pltpu.make_async_copy(src.at[pl.ds(0, FG), ys], rin.at[0, i, :, ys], first_sem.at[q])
                for i, src in enumerate((rho_re, rho_im))]

    def first_loaded(q):
        ref = rin.at[0, :, :, pl.ds(q * NY, NY)]
        return pltpu.make_async_copy(ref, ref, first_sem.at[q])

    barrier = pltpu.get_barrier_semaphore()
    for peer in [py_peer(r) for r in (1, 2, 3)] + [pz_peer]:
        pl.semaphore_signal(barrier, inc=1, device_id=peer, device_id_type=MESH)
    both = me * NPZ + mz
    tabs = [pltpu.make_async_copy(t.at[i], wraw.at[k], w_sem.at[min(k, 1)])
            for k, (t, i) in enumerate(((t1, me), (t2, both), (t3, mz), (t3i, mz), (t4, both), (t5, me)))]
    greens = [pltpu.make_async_copy(src, gin.at[i], g_sem) for i, src in enumerate((g_re, g_im))]
    firsts = [cp for q in range(BLOCKS) for cp in load_first(q)]
    for cp in tabs[:1] + firsts + tabs[1:] + greens + load_in(1):
        cp.start()

    def table(k):
        wide, narrow = (left_table if k in (1, Q) else right_table)(*(wraw[k, i] for i in range(3)))
        wbig[k] = wide
        wsmall[k] = narrow

    def lmat(k):
        return wbig.at[k], wsmall.at[k]

    def rmat(k):
        return wbig[k], from_wide(wsmall[k])

    def stage1(g, y0, ny):
        slot, ring = lax.rem(g, 2), lax.rem(g, RA)
        w = rmat(0)
        for i in range(ny):
            y = y0 + i
            x = jnp.concatenate([rin[slot, 0, :, y].reshape(L, N), rin[slot, 1, :, y].reshape(L, N)], 1)
            out = right(x, w).T
            rows = pl.ds(pl.multiple_of(y * S, S), S)
            for c in range(Q):
                for r in range(Q):
                    tile = out[(r * Q + c) * S:(r * Q + c + 1) * S]
                    if r == 0:
                        a_recv[lax.rem(g * Q + c, AR), 0, rows, :] = tile
                    else:
                        a_send[ring, c, r - 1, rows, :] = tile

    def a_copy(u, r):
        g, c = u // Q, lax.rem(u, Q)
        ring = lax.rem(g, RA)
        return pltpu.make_async_remote_copy(
            src_ref=a_send.at[ring, c, r - 1], dst_ref=a_recv.at[lax.rem(u, AR), r], send_sem=as_sem.at[ring],
            recv_sem=ar_sem.at[lax.rem(u, AR)], device_id=py_peer(r), device_id_type=MESH)

    def a_piece(u, k, r, y0, ny):
        part = (pl.ds(y0, ny), pl.ds(2 * k, 2))
        src, dst = (ref.reshape(Y, S, L).at[part] for ref in (a_send.at[0, u, r - 1], a_recv.at[u, r]))
        return pltpu.make_async_remote_copy(
            src_ref=src, dst_ref=dst, send_sem=as_sem.at[0], recv_sem=piece_sem.at[u, k],
            device_id=py_peer(r), device_id_type=MESH)

    def piece_arrived(u, k):
        ref = a_recv.at[u, pl.ds(1, 3), pl.ds(Z * k, Z)]
        return pltpu.make_async_copy(ref, ref, piece_sem.at[u, k])

    def c_part(u, kk):
        ring = lax.rem(u, RING)
        return pltpu.make_async_remote_copy(
            src_ref=c_send.at[ring, kk], dst_ref=c_recv.at[lax.rem(u, RECV), 1, kk], send_sem=cs_sem.at[ring],
            recv_sem=part_sem.at[u - (NU - LATE), kk], device_id=pz_peer, device_id_type=MESH)

    def d_part(u, r, kk):
        part = (slice(None), pl.ds(2 * kk, 2))
        src, dst = (ref.reshape(Y, S, L).at[part] for ref in (d_send.at[u % RING, r - 1], d_recv.at[u, r]))
        return pltpu.make_async_remote_copy(
            src_ref=src, dst_ref=dst, send_sem=ds_sem.at[u % RING], recv_sem=dr_sem.at[(NG - 1) % RG],
            device_id=py_peer(r), device_id_type=MESH)

    def a_sent(g):
        ring = lax.rem(g, RA)
        return pltpu.make_async_copy(a_send.at[ring], a_send.at[ring], as_sem.at[ring])

    def a_arrived(u):
        ref = a_recv.at[lax.rem(u, AR), pl.ds(1, 3)]
        return pltpu.make_async_copy(ref, ref, ar_sem.at[lax.rem(u, AR)])

    def d_sent(u):
        ring = lax.rem(u, RING)
        return pltpu.make_async_copy(d_send.at[ring], d_send.at[ring], ds_sem.at[ring])

    def d_arrived(g):
        ref = d_recv.at[pl.ds(g * Q, Q), pl.ds(1, 3)]
        return pltpu.make_async_copy(ref, ref, dr_sem.at[lax.rem(g, RG)])

    def b_copy(u):
        ring = lax.rem(u, RING)
        return pltpu.make_async_remote_copy(
            src_ref=b_send.at[ring], dst_ref=b_recv.at[lax.rem(u, RECV), 1], send_sem=bs_sem.at[ring], recv_sem=br_sem.at[lax.rem(u, RECV)],
            device_id=pz_peer, device_id_type=MESH)

    def b_piece(u, k):
        return pltpu.make_async_remote_copy(
            src_ref=b_send.at[u, k], dst_ref=b_recv.at[u, 1, k], send_sem=bs_sem.at[u],
            recv_sem=br_sem.at[u] if u else bh_sem.at[k // 2], device_id=pz_peer, device_id_type=MESH)

    def bh_arrived(h):
        ref = b_recv.at[0, 1, pl.ds(2 * h, 2)]
        return pltpu.make_async_copy(ref, ref, bh_sem.at[h])

    def c_half(h):
        kk = pl.ds(2 * h, 2)
        return pltpu.make_async_remote_copy(
            src_ref=c_send.at[0, kk], dst_ref=c_recv.at[0, 1, kk], send_sem=cs_sem.at[0], recv_sem=cr_sem.at[0],
            device_id=pz_peer, device_id_type=MESH)

    def c_copy(u):
        ring = lax.rem(u, RING)
        return pltpu.make_async_remote_copy(
            src_ref=c_send.at[ring], dst_ref=c_recv.at[lax.rem(u, RECV), 1], send_sem=cs_sem.at[ring], recv_sem=cr_sem.at[lax.rem(u, RECV)],
            device_id=pz_peer, device_id_type=MESH)

    def d_copy(u, r):
        ring = lax.rem(u, RING)
        return pltpu.make_async_remote_copy(
            src_ref=d_send.at[ring, r - 1], dst_ref=d_recv.at[u, r], send_sem=ds_sem.at[ring],
            recv_sem=dr_sem.at[lax.rem(u // Q, RG)], device_id=py_peer(r), device_id_type=MESH)

    def send_a(g):
        for c in range(Q):
            for r in (2, 1, 3):
                a_copy(g * Q + c, r).start()

    def y_lines(u, kks):
        ring, slot, arrived = lax.rem(u, RING), lax.rem(u, RECV), lax.rem(u, AR)
        cols = [jnp.concatenate([a_recv[arrived, r, pl.ds(kk * 2 + ri, Y, stride=S), :]
                                 for r in range(Q) for ri in range(2)], 0) for kk in kks]
        out = left(lmat(1), jnp.concatenate(cols, 1))
        for i, kk in enumerate(kks):
            b_recv[slot, 0, kk] = out[:H, i * L:(i + 1) * L]
            b_send[ring, kk] = out[H:, i * L:(i + 1) * L]

    def stage2(u):
        a_arrived(u).wait()

        @pl.when(u >= RING)
        def _():
            b_copy(u - RING).wait_send()

        for kp in range(2):
            y_lines(u, (2 * kp, 2 * kp + 1))
        b_copy(u).start()

    def z_lines(u, kp):
        ring, c, f0 = lax.rem(u, RING), lax.rem(u, Q), u // Q * FG
        wf, wi = rmat(2), rmat(3)
        rows = []
        for kk in (2 * kp, 2 * kp + 1):
            rows += swap_lanes([b_recv[lax.rem(u, RECV), q, kk, ri * Z:(ri + 1) * Z, :] for q in range(2) for ri in range(2)])
        spec = right(jnp.concatenate(rows, 0), wf)
        hats = []
        for i in range(2):
            kk = 2 * kp + i
            gr = pl.ds(pl.multiple_of((c * Q + kk) * Z, Z), Z)
            gan, gbn = ga[gr, :], gb[gr, :]
            for f in range(FG):
                s = spec[(i * FG + f) * Z:(i * FG + f + 1) * Z]
                h = s * gan + pltpu.roll(s, H, 1) * gbn
                hat_re[f0 + f, c * Q + kk] = h[:, :N]
                hat_im[f0 + f, c * Q + kk] = h[:, N:]
                hats.append(h)
        back = right(jnp.concatenate(hats, 0), wi)
        for i in range(2):
            kk = 2 * kp + i
            t = swap_lanes([back[(i * FG + f) * Z:(i * FG + f + 1) * Z] for f in range(FG)])
            for ri in range(2):
                c_recv[lax.rem(u, RECV), 0, kk, ri * Z:(ri + 1) * Z, :] = t[ri]
                c_send[ring, kk, ri * Z:(ri + 1) * Z, :] = t[2 + ri]

    def stage3(u):
        b_copy(u).wait_recv()

        @pl.when(u >= RING)
        def _():
            c_copy(u - RING).wait_send()

        for kp in range(2):
            z_lines(u, kp)

        @pl.when(u < NU - LATE)
        def _():
            c_copy(u).start()

        @pl.when(u >= NU - LATE)
        def _():
            for kk in range(Q):
                c_part(u, kk).start()

    def y_lines_back(u, kks):
        ring = lax.rem(u, RING)
        cols = [jnp.concatenate([c_recv[lax.rem(u, RECV), q, kk] for q in range(2)], 0) for kk in kks]
        out = left(lmat(Q), jnp.concatenate(cols, 1))
        for i, kk in enumerate(kks):
            for r in range(Q):
                for ro in range(2):
                    rows = pl.ds(kk * 2 + ro, Y, stride=S)
                    tile = out[(r * 2 + ro) * Y:(r * 2 + ro + 1) * Y, i * L:(i + 1) * L]
                    if r == 0:
                        d_recv[u, 0, rows, :] = tile
                    else:
                        d_send[ring, r - 1, rows, :] = tile

    def stage4(u):
        c_copy(u).wait_recv()

        @pl.when(u >= RING)
        def _():
            d_sent(u - RING).wait()

        for kp in range(2):
            y_lines_back(u, (2 * kp, 2 * kp + 1))
        for r in (2, 1, 3):
            d_copy(u, r).start()

    def stage5(g, y0, ny):
        w = rmat(5)
        for i in range(ny):
            y = y0 + i
            rows = pl.ds(pl.multiple_of(y * S, S), S)
            x = jnp.concatenate([d_recv[g * Q + c, r, rows, :] for c in range(Q) for r in range(Q)], 0)
            out = right(x.T, w)
            for f in range(FG):
                for r in range(Q):
                    d_recv[g * Q + f, r, rows, :] = out[(f * Q + r) * S:(f * Q + r + 1) * S]

    odd = lax.rem(me, 2)
    order = (2 - odd, 3 - odd, 1 + 2 * odd)
    tabs[0].wait()
    table(0)
    for q in range(BLOCKS):
        first_loaded(q).wait()
        stage1(0, q * NY, NY)
        if q == 0:
            pl.semaphore_wait(barrier, Q)
        for r in order:
            a_piece(0, 0, r, q * NY, NY).start()
    for u, k in PIECES[1:]:
        for r in order:
            a_piece(u, k, r, 0, Y).start()
    for u in range(EARLY, Q):
        for r in (2, 1, 3):
            a_copy(u, r).start()
    for cp in load_in(2):
        cp.start()
    pltpu.make_async_copy(wraw.at[pl.ds(1, 5)], wraw.at[pl.ds(1, 5)], w_sem.at[1]).wait()
    for k in range(1, 6):
        table(k)
    pltpu.make_async_copy(gin, gin, g_sem).wait()
    gr, gi = gin[0].reshape(512, N), gin[1].reshape(512, N)
    ga[...] = jnp.concatenate([gr, gr], 1)
    gb[...] = jnp.concatenate([-gi, gi], 1)
    inputs_of(1)

    @pl.loop(0, Q)
    def _(q):
        stage1(1, q * Q, Q)

    send_a(1)
    for cp in load_in(3):
        cp.start()
    for u, k in PIECES:
        piece_arrived(u, k).wait()
        y_lines(u, (k,))
        b_piece(u, k).start()
    for h in range(2):
        bh_arrived(h).wait()
        z_lines(0, h)
        c_half(h).start()

    inputs_of(2)
    for q in range(EARLY):
        stage1(2, q * Q, Q)

    def step(t, carry):
        c = lax.rem(t, Q)
        g1 = t // Q + 2

        @pl.when(t < NU)
        def _():
            stage2(t)

        u3 = t - LAG3

        @pl.when(u3 >= 1)
        def _():
            stage3(u3)

        u4 = t - LAG4

        @pl.when(u4 >= 0)
        def _():
            stage4(u4)

        @pl.when(g1 < NG)
        def _():
            @pl.when(c == 0)
            def _():
                inputs_of(g1)

                @pl.when(g1 >= RA)
                def _():
                    a_sent(g1 - RA).wait()

            stage1(g1, c * Q, Q)

            @pl.when(c == 3)
            def _():
                send_a(g1)

                @pl.when(g1 + 2 < NG)
                def _():
                    for cp in load_in(g1 + 2):
                        cp.start()

        u5 = t - LAG5

        @pl.when(u5 >= 0)
        def _():
            @pl.when(lax.rem(u5, Q) == 0)
            def _():
                d_arrived(u5 // Q).wait()

            stage5(u5 // Q, lax.rem(u5, Q) * Q, Q)

        return carry

    steps = NU - LATE + LAG4
    lax.fori_loop(EARLY, steps, step, 0)
    rest = [u5 for u5 in range(steps - LAG5, NU - Q)]
    u3 = [u for u in range(steps - LAG3, NU)]
    for u in range(NU - LATE, NU):
        if u3:
            stage3(u3.pop(0))
        d_sent(u - RING).wait()
        for kk in range(Q):
            c_part(u, kk).wait_recv()
            y_lines_back(u, (kk,))
            for r in (2, 1, 3):
                d_part(u, r, kk).start()
        for u5 in rest[:2]:
            if u5 % Q == 0:
                d_arrived(u5 // Q).wait()
            stage5(u5 // Q, u5 % Q * Q, Q)
        rest = rest[2:]
    d_arrived(NG - 1).wait()

    for g in range(NG - RA, NG):
        a_sent(g).wait()
    for u in range(NU - RING, NU):
        b_copy(u).wait_send()
        c_copy(u).wait_send()
        d_sent(u).wait()


def unpack(phi, re, im, t5, phi_re, phi_im, hat_re, hat_im, wraw, st, st_last, w_sem, hat_sem, sem, last_sem):
    tab = pltpu.make_async_copy(t5.at[lax.axis_index("py")], wraw, w_sem)
    tab.start()
    hats, phis = ((re, hat_re), (im, hat_im)), (phi_re, phi_im)
    for i in range(FIELDS // HB):
        part = pl.ds(i * HB, HB)
        for k, (src, dst) in enumerate(hats):
            pltpu.make_async_copy(src.at[part], dst.at[part], hat_sem.at[k]).start()

    def last_copy(k):
        return pltpu.make_async_copy(st_last.at[k], phis[k].at[pl.ds(FIELDS - FG, FG)], last_sem.at[k])

    tab.wait()
    wide, narrow = right_table(*(wraw[i] for i in range(3)))
    w = wide, from_wide(narrow)

    @pl.loop(0, Q)
    def _(q):
        for i in range(Q):
            y = q * Q + i
            rows = pl.ds(pl.multiple_of(y * S, S), S)
            x = jnp.concatenate([phi[NU - Q + c, r, rows, :] for c in range(Q) for r in range(Q)], 0)
            out = right(x.T, w)
            for k, half in enumerate((out[:, :N], out[:, N:])):
                st_last[k, :, y] = half.reshape(FG, Z, N)

    for k in range(2):
        last_copy(k).start()

    def copy(i, k):
        slot = lax.rem(i, SLOTS)
        return pltpu.make_async_copy(st.at[slot, k], phis[k].at[pl.ds(i * FB, FB)], sem.at[slot, k])

    def phi_job(i, carry):
        slot = lax.rem(i, SLOTS)

        @pl.when(i >= SLOTS)
        def _():
            for k in range(2):
                copy(i - SLOTS, k).wait()

        for f in range(FB):
            for r in range(Q):
                p = phi[i * FB + f, r]
                for k, half in enumerate((p[:, :N], p[:, N:])):
                    st[slot, k, f, :, r * S:(r + 1) * S] = half.reshape(Y, S, N)
        for k in range(2):
            copy(i, k).start()
        return carry

    jobs = (FIELDS - FG) // FB
    lax.fori_loop(0, jobs, phi_job, 0)
    for k, (src, dst) in enumerate(hats):
        pltpu.make_async_copy(src, dst, hat_sem.at[k]).wait()
        last_copy(k).wait()
    for i in range(jobs - SLOTS, jobs):
        for k in range(2):
            copy(i, k).wait()


def in_hbm(x):
    return pltpu.with_memory_space_constraint(x, pltpu.HBM)


def solution(mesh):
    consts = tables()

    def local_solve(rho_re, rho_im, g_re, g_im):
        dma, vmem, hbm = pltpu.SemaphoreType.DMA, pltpu.VMEM, pl.BlockSpec(memory_space=pl.ANY)
        tabs = [jnp.asarray(c) for c in consts]
        field = jax.ShapeDtypeStruct((FIELDS, Y, Z, N), F32)
        packed = pl.pallas_call(
            kernel,
            out_shape=[pltpu.VMEM((NU, Q, L, L), F32)] + [pltpu.VMEM(field.shape, F32)] * 2,
            in_specs=[hbm] * 10,
            out_specs=[pl.BlockSpec(memory_space=pltpu.VMEM)] * 3,
            scratch_shapes=[
                vmem((2, 2, FG, Y, Z, N), F32),
                vmem((2, Y, Z, N), F32),
                vmem((6, 3, L, L), BF16),
                vmem((6, 256, 256), BF16),
                vmem((6, L, 256), BF16),
                vmem((512, L), F32), vmem((512, L), F32),
                vmem((RA, Q, 3, L, L), F32),
                vmem((AR, Q, L, L), F32),
                vmem((RING, Q, H, L), F32),
                vmem((RECV, 2, Q, H, L), F32),
                vmem((RING, Q, H, L), F32),
                vmem((RECV, 2, Q, H, L), F32),
                vmem((RING, 3, L, L), F32),
                dma((2,)), dma((BLOCKS,)), dma, dma((2,)), dma((RA,)), dma((AR,)), dma((EARLY, Q)), dma((2,)),
                dma((RING,)), dma((RECV,)), dma((RING,)), dma((RECV,)), dma((LATE, Q)), dma((RING,)), dma((RG,)),
            ],
            compiler_params=pltpu.CompilerParams(collective_id=0, has_side_effects=True,
                                                 vmem_limit_bytes=24 << 20),
            name="spectral",
        )(*(in_hbm(x) for x in (jnp.transpose(rho_re, (0, 2, 3, 1)), jnp.transpose(rho_im, (0, 2, 3, 1)), g_re, g_im, *tabs)))
        packed = [pltpu.with_memory_space_constraint(x, pltpu.VMEM) for x in packed]
        phi_re, phi_im, hat_re, hat_im = pl.pallas_call(
            unpack,
            out_shape=[field] * Q,
            in_specs=[pl.BlockSpec(memory_space=pltpu.VMEM)] * 3 + [hbm],
            out_specs=[hbm] * Q,
            scratch_shapes=[vmem((3, L, L), BF16), vmem((SLOTS, 2, FB, Y, Z, N), F32),
                            vmem((2, FG, Y, Z, N), F32), dma, dma((2,)), dma((SLOTS, 2)), dma((2,))],
            compiler_params=pltpu.CompilerParams(vmem_limit_bytes=20 << 20),
            name="unpack",
        )(*packed, in_hbm(tabs[5]))
        return jnp.transpose(phi_re, (0, 3, 1, 2)), jnp.transpose(phi_im, (0, 3, 1, 2)), hat_re, hat_im

    space_layout = P("dp", None, "py", "pz")
    wave_layout = P("dp", "py", "pz", None)
    green_layout = P("py", "pz", None)
    return jax.shard_map(local_solve, mesh=mesh,
                         in_specs=(space_layout, space_layout, green_layout, green_layout),
                         out_specs=(space_layout, space_layout, wave_layout, wave_layout),
                         check_vma=False)
```

```python
import functools

import jax
import jax.numpy as jnp
import ml_dtypes
import numpy as np
from jax import lax
from jax.experimental import pallas as pl
from jax.experimental.pallas import tpu as pltpu
from jax.sharding import PartitionSpec as P

MESH = pl.DeviceIdType.MESH
L, H, Z, Y, S, Q = 128, 64, 32, 16, 8, 4
F32, BF16 = jnp.float32, jnp.bfloat16
N = 64
FIELDS = 32
FG = 4
NG = FIELDS // FG
NU = NG * 4
NPY, NPZ = 4, 2
LAG3, LAG4 = 2, 4
LAG5 = LAG4 + 5
RING = 4
RECV = 6
RG = 4
RA = 3
AR = 16
BLOCKS = 2
NY = 16 // BLOCKS
EARLY = 2
PIECES = [(u, k) for u in range(EARLY) for k in range(4)]
LATE = 3
FB, SLOTS = 4, 4
HB = 8


def dft(sign):
    jk = np.outer(np.arange(N), np.arange(N)) % N
    c, s = np.cos(2 * np.pi * jk / N) / S, sign * np.sin(2 * np.pi * jk / N) / S
    return np.stack([np.stack([c, -s], 1), np.stack([s, c], 1)])


def split_np(w):
    w = np.asarray(w, np.float32)
    parts = []
    for _ in range(3):
        part = w.astype(ml_dtypes.bfloat16)
        parts.append(part)
        w = w - part.astype(np.float32)
    return np.stack(parts)


def tables():
    fwd, inv = dft(-1), dft(1)
    i16, i32 = np.arange(Y), np.arange(Z)
    w1, w2, w3, w3i, w4, w5 = [], [], [], [], [], []
    for a in range(NPY):
        to = [Y * ((a + r) % Q) + i16 for r in range(Q)]
        frm = [Y * ((a - r) % Q) + i16 for r in range(Q)]
        out = np.stack([fwd[:, k] for k in to]).reshape(Q, 2, Q, Q, 2, N)
        w1.append(out.transpose(Q, 5, 0, 2, 3, 1).reshape(L, L))
        inn = np.stack([inv[:, :, :, k] for k in frm]).reshape(Q, 2, N, 2, Q, Q)
        w5.append(inn.transpose(Q, 0, 5, 3, 1, 2).reshape(L, L))
        for b in range(NPZ):
            half = [Z * (b ^ q) + i32 for q in range(2)]
            m = np.stack([fwd[:, k] for k in half])
            m = np.stack([m[..., y] for y in frm])
            w2.append(m.transpose(1, 2, 3, 0, Q, 5).reshape(L, L))
            m = np.stack([inv[:, y] for y in to])
            m = np.stack([m[..., k] for k in half])
            w4.append(m.transpose(1, 2, 3, 0, Q, 5).reshape(L, L))
    for b in range(NPZ):
        half = [Z * (b ^ q) + i32 for q in range(2)]
        m = np.stack([fwd[..., z] for z in half])
        w3.append(m.transpose(0, 3, Q, 1, 2).reshape(L, L))
        m = np.stack([inv[:, z] for z in half])
        w3i.append(m.transpose(3, Q, 0, 1, 2).reshape(L, L))
    return [np.stack([split_np(w) for w in ws]) for ws in (w1, w2, w3, w3i, w4, w5)]


def split3(x):
    hi = x.astype(BF16)
    rest = x - hi.astype(F32)
    mid = rest.astype(BF16)
    return hi, mid, (rest - mid.astype(F32)).astype(BF16)


def dot(a, b):
    return jnp.dot(a, b, preferred_element_type=F32)


def left(w, x):
    hi, mid, lo = split3(x)
    wide = dot(w[0][...], jnp.concatenate([hi, mid], 0))
    return wide[:L] + (wide[L:] + dot(w[1][...], jnp.concatenate([hi, lo], 0)))


def right(x, w):
    hi, mid, lo = split3(x)
    wide = dot(jnp.concatenate([hi, mid], 1), w[0][...])
    return wide[:, :L] + (wide[:, L:] + dot(jnp.concatenate([hi, lo], 1), w[1][...]))


def left_table(w1, w2, w3):
    pairs = [jnp.concatenate([a, b], 1) for a, b in ((w1, w1), (w2, w2), (w3, w1))]
    return jnp.concatenate(pairs[:2], 0), pairs[2]


def right_table(w1, w2, w3):
    return jnp.concatenate([jnp.concatenate([w1, w2], 1)] * 2, 0), jnp.concatenate([w3, w1], 1)


def from_wide(w):
    return jnp.concatenate([w[:, :L], w[:, L:]], 0)


def swap_lanes(tiles):
    lane = lax.broadcasted_iota(jnp.int32, tiles[0].shape, 1)
    odd, high = (lane // Z) % 2 == 1, lane >= H
    t = list(tiles)
    for lo in (0, 2):
        a, b = t[lo], t[lo + 1]
        t[lo] = jnp.where(odd, pltpu.roll(b, Z, 1), a)
        t[lo + 1] = jnp.where(odd, b, pltpu.roll(a, 96, 1))
    for lo in (0, 1):
        a, b = t[lo], t[lo + 2]
        t[lo] = jnp.where(high, pltpu.roll(b, H, 1), a)
        t[lo + 2] = jnp.where(high, b, pltpu.roll(a, H, 1))
    return t


def kernel(rho_re, rho_im, g_re, g_im, t1, t2, t3, t3i, t4, t5, d_recv, hat_re, hat_im,
           rin, gin, wraw, wbig, wsmall, ga, gb, a_send, a_recv, b_send, b_recv, c_send, c_recv, d_send,
           in_sem, first_sem, g_sem, w_sem, as_sem, ar_sem, bs_sem, br_sem, cs_sem, cr_sem, part_sem,
           ds_sem, dr_sem):
    me, mz = lax.axis_index("py"), lax.axis_index("pz")
    zero = lax.axis_index("dp")

    def py_peer(r):
        return (zero, mz, lax.rem(me + r, NPY))

    pz_peer = (zero, 1 - mz, me)

    def load_in(g):
        slot = lax.rem(g, 2)
        return [pltpu.make_async_copy(src.at[pl.ds(g * FG, FG)], rin.at[slot, i], in_sem.at[slot])
                for i, src in enumerate((rho_re, rho_im))]

    def inputs_of(g):
        ref = rin.at[lax.rem(g, 2)]
        pltpu.make_async_copy(ref, ref, in_sem.at[lax.rem(g, 2)]).wait()

    def load_first(q):
        ys = pl.ds(q * NY, NY)
        return [pltpu.make_async_copy(src.at[pl.ds(0, FG), ys], rin.at[0, i, :, ys], first_sem.at[q])
                for i, src in enumerate((rho_re, rho_im))]

    def first_loaded(q):
        ref = rin.at[0, :, :, pl.ds(q * NY, NY)]
        return pltpu.make_async_copy(ref, ref, first_sem.at[q])

    barrier = pltpu.get_barrier_semaphore()
    for peer in [py_peer(r) for r in (1, 2, 3)] + [pz_peer]:
        pl.semaphore_signal(barrier, inc=1, device_id=peer, device_id_type=MESH)
    both = me * NPZ + mz
    tabs = [pltpu.make_async_copy(t.at[i], wraw.at[k], w_sem.at[min(k, 1)])
            for k, (t, i) in enumerate(((t1, me), (t2, both), (t3, mz), (t3i, mz), (t4, both), (t5, me)))]
    greens = [pltpu.make_async_copy(src, gin.at[i], g_sem) for i, src in enumerate((g_re, g_im))]
    firsts = [cp for q in range(BLOCKS) for cp in load_first(q)]
    for cp in tabs[:1] + firsts + tabs[1:] + greens + load_in(1):
        cp.start()

    def table(k):
        wide, narrow = (left_table if k in (1, Q) else right_table)(*(wraw[k, i] for i in range(3)))
        wbig[k] = wide
        wsmall[k] = narrow

    def lmat(k):
        return wbig.at[k], wsmall.at[k]

    def rmat(k):
        return wbig[k], from_wide(wsmall[k])

    def stage1(g, y0, ny):
        slot, ring = lax.rem(g, 2), lax.rem(g, RA)
        w = rmat(0)
        for i in range(ny):
            y = y0 + i
            x = jnp.concatenate([rin[slot, 0, :, y].reshape(L, N), rin[slot, 1, :, y].reshape(L, N)], 1)
            out = right(x, w).T
            rows = pl.ds(pl.multiple_of(y * S, S), S)
            for c in range(Q):
                for r in range(Q):
                    tile = out[(r * Q + c) * S:(r * Q + c + 1) * S]
                    if r == 0:
                        a_recv[lax.rem(g * Q + c, AR), 0, rows, :] = tile
                    else:
                        a_send[ring, c, r - 1, rows, :] = tile

    def a_copy(u, r):
        g, c = u // Q, lax.rem(u, Q)
        ring = lax.rem(g, RA)
        return pltpu.make_async_remote_copy(
            src_ref=a_send.at[ring, c, r - 1], dst_ref=a_recv.at[lax.rem(u, AR), r], send_sem=as_sem.at[ring],
            recv_sem=ar_sem.at[lax.rem(u, AR)], device_id=py_peer(r), device_id_type=MESH)

    def a_piece(u, k, r, y0, ny):
        part = (pl.ds(y0, ny), pl.ds(2 * k, 2))
        src, dst = (ref.reshape(Y, S, L).at[part] for ref in (a_send.at[0, u, r - 1], a_recv.at[u, r]))
        return pltpu.make_async_remote_copy(
            src_ref=src, dst_ref=dst, send_sem=as_sem.at[0], recv_sem=part_sem.at[u, k],
            device_id=py_peer(r), device_id_type=MESH)

    def piece_arrived(u, k):
        ref = a_recv.at[u, pl.ds(1, 3), pl.ds(Z * k, Z)]
        return pltpu.make_async_copy(ref, ref, part_sem.at[u, k])

    def c_part(u, kk):
        ring = lax.rem(u, RING)
        return pltpu.make_async_remote_copy(
            src_ref=c_send.at[ring, kk], dst_ref=c_recv.at[lax.rem(u, RECV), 1, kk], send_sem=cs_sem.at[ring],
            recv_sem=part_sem.at[u - (NU - LATE), kk], device_id=pz_peer, device_id_type=MESH)

    def d_part(u, r, kk):
        part = (slice(None), pl.ds(2 * kk, 2))
        src, dst = (ref.reshape(Y, S, L).at[part] for ref in (d_send.at[u % RING, r - 1], d_recv.at[u, r]))
        return pltpu.make_async_remote_copy(
            src_ref=src, dst_ref=dst, send_sem=ds_sem.at[u % RING], recv_sem=dr_sem.at[(NG - 1) % RG],
            device_id=py_peer(r), device_id_type=MESH)

    def a_sent(g):
        ring = lax.rem(g, RA)
        return pltpu.make_async_copy(a_send.at[ring], a_send.at[ring], as_sem.at[ring])

    def a_arrived(u):
        ref = a_recv.at[lax.rem(u, AR), pl.ds(1, 3)]
        return pltpu.make_async_copy(ref, ref, ar_sem.at[lax.rem(u, AR)])

    def d_sent(u):
        ring = lax.rem(u, RING)
        return pltpu.make_async_copy(d_send.at[ring], d_send.at[ring], ds_sem.at[ring])

    def d_arrived(g):
        ref = d_recv.at[pl.ds(g * Q, Q), pl.ds(1, 3)]
        return pltpu.make_async_copy(ref, ref, dr_sem.at[lax.rem(g, RG)])

    def b_copy(u):
        ring = lax.rem(u, RING)
        return pltpu.make_async_remote_copy(
            src_ref=b_send.at[ring], dst_ref=b_recv.at[lax.rem(u, RECV), 1], send_sem=bs_sem.at[ring], recv_sem=br_sem.at[lax.rem(u, RECV)],
            device_id=pz_peer, device_id_type=MESH)

    def b_piece(u, k):
        return pltpu.make_async_remote_copy(
            src_ref=b_send.at[u, k], dst_ref=b_recv.at[u, 1, k], send_sem=bs_sem.at[u],
            recv_sem=br_sem.at[u] if u else part_sem.at[EARLY, k // 2], device_id=pz_peer, device_id_type=MESH)

    def bh_arrived(h):
        ref = b_recv.at[0, 1, pl.ds(2 * h, 2)]
        return pltpu.make_async_copy(ref, ref, part_sem.at[EARLY, h])

    def c_half(h):
        kk = pl.ds(2 * h, 2)
        return pltpu.make_async_remote_copy(
            src_ref=c_send.at[0, kk], dst_ref=c_recv.at[0, 1, kk], send_sem=cs_sem.at[0], recv_sem=cr_sem.at[0],
            device_id=pz_peer, device_id_type=MESH)

    def c_copy(u):
        ring = lax.rem(u, RING)
        return pltpu.make_async_remote_copy(
            src_ref=c_send.at[ring], dst_ref=c_recv.at[lax.rem(u, RECV), 1], send_sem=cs_sem.at[ring], recv_sem=cr_sem.at[lax.rem(u, RECV)],
            device_id=pz_peer, device_id_type=MESH)

    def d_copy(u, r):
        ring = lax.rem(u, RING)
        return pltpu.make_async_remote_copy(
            src_ref=d_send.at[ring, r - 1], dst_ref=d_recv.at[u, r], send_sem=ds_sem.at[ring],
            recv_sem=dr_sem.at[lax.rem(u // Q, RG)], device_id=py_peer(r), device_id_type=MESH)

    def send_a(g):
        for c in range(Q):
            for r in (2, 1, 3):
                a_copy(g * Q + c, r).start()

    def y_lines(u, kks):
        ring, slot, arrived = lax.rem(u, RING), lax.rem(u, RECV), lax.rem(u, AR)
        cols = [jnp.concatenate([a_recv[arrived, r, pl.ds(kk * 2 + ri, Y, stride=S), :]
                                 for r in range(Q) for ri in range(2)], 0) for kk in kks]
        out = left(lmat(1), jnp.concatenate(cols, 1))
        for i, kk in enumerate(kks):
            b_recv[slot, 0, kk] = out[:H, i * L:(i + 1) * L]
            b_send[ring, kk] = out[H:, i * L:(i + 1) * L]

    def stage2(u):
        a_arrived(u).wait()

        @pl.when(u >= RING)
        def _():
            b_copy(u - RING).wait_send()

        for kp in range(2):
            y_lines(u, (2 * kp, 2 * kp + 1))
        b_copy(u).start()

    def z_lines(u, kp):
        ring, c, f0 = lax.rem(u, RING), lax.rem(u, Q), u // Q * FG
        wf, wi = rmat(2), rmat(3)
        rows = []
        for kk in (2 * kp, 2 * kp + 1):
            rows += swap_lanes([b_recv[lax.rem(u, RECV), q, kk, ri * Z:(ri + 1) * Z, :] for q in range(2) for ri in range(2)])
        spec = right(jnp.concatenate(rows, 0), wf)
        hats = []
        for i in range(2):
            kk = 2 * kp + i
            gr = pl.ds(pl.multiple_of((c * Q + kk) * Z, Z), Z)
            gan, gbn = ga[gr, :], gb[gr, :]
            for f in range(FG):
                s = spec[(i * FG + f) * Z:(i * FG + f + 1) * Z]
                h = s * gan + pltpu.roll(s, H, 1) * gbn
                hat_re[f0 + f, c * Q + kk] = h[:, :N]
                hat_im[f0 + f, c * Q + kk] = h[:, N:]
                hats.append(h)
        back = right(jnp.concatenate(hats, 0), wi)
        for i in range(2):
            kk = 2 * kp + i
            t = swap_lanes([back[(i * FG + f) * Z:(i * FG + f + 1) * Z] for f in range(FG)])
            for ri in range(2):
                c_recv[lax.rem(u, RECV), 0, kk, ri * Z:(ri + 1) * Z, :] = t[ri]
                c_send[ring, kk, ri * Z:(ri + 1) * Z, :] = t[2 + ri]

    def stage3(u):
        b_copy(u).wait_recv()

        @pl.when(u >= RING)
        def _():
            c_copy(u - RING).wait_send()

        for kp in range(2):
            z_lines(u, kp)

        @pl.when(u < NU - LATE)
        def _():
            c_copy(u).start()

        @pl.when(u >= NU - LATE)
        def _():
            for kk in range(Q):
                c_part(u, kk).start()

    def y_lines_back(u, kks):
        ring = lax.rem(u, RING)
        cols = [jnp.concatenate([c_recv[lax.rem(u, RECV), q, kk] for q in range(2)], 0) for kk in kks]
        out = left(lmat(Q), jnp.concatenate(cols, 1))
        for i, kk in enumerate(kks):
            for r in range(Q):
                for ro in range(2):
                    rows = pl.ds(kk * 2 + ro, Y, stride=S)
                    tile = out[(r * 2 + ro) * Y:(r * 2 + ro + 1) * Y, i * L:(i + 1) * L]
                    if r == 0:
                        d_recv[u, 0, rows, :] = tile
                    else:
                        d_send[ring, r - 1, rows, :] = tile

    def stage4(u):
        c_copy(u).wait_recv()

        @pl.when(u >= RING)
        def _():
            d_sent(u - RING).wait()

        for kp in range(2):
            y_lines_back(u, (2 * kp, 2 * kp + 1))
        for r in (2, 1, 3):
            d_copy(u, r).start()

    def stage5(g, y0, ny):
        w = rmat(5)
        for i in range(ny):
            y = y0 + i
            rows = pl.ds(pl.multiple_of(y * S, S), S)
            x = jnp.concatenate([d_recv[g * Q + c, r, rows, :] for c in range(Q) for r in range(Q)], 0)
            out = right(x.T, w)
            for f in range(FG):
                for r in range(Q):
                    d_recv[g * Q + f, r, rows, :] = out[(f * Q + r) * S:(f * Q + r + 1) * S]

    odd = lax.rem(me, 2)
    order = (2 - odd, 3 - odd, 1 + 2 * odd)
    tabs[0].wait()
    table(0)
    for q in range(BLOCKS):
        first_loaded(q).wait()
        stage1(0, q * NY, NY)
        if q == 0:
            pl.semaphore_wait(barrier, Q)
        for r in order:
            a_piece(0, 0, r, q * NY, NY).start()
    for u, k in PIECES[1:]:
        for r in order:
            a_piece(u, k, r, 0, Y).start()
    for u in range(EARLY, Q):
        for r in (2, 1, 3):
            a_copy(u, r).start()
    for cp in load_in(2):
        cp.start()
    pltpu.make_async_copy(wraw.at[pl.ds(1, 5)], wraw.at[pl.ds(1, 5)], w_sem.at[1]).wait()
    for k in range(1, 6):
        table(k)
    pltpu.make_async_copy(gin, gin, g_sem).wait()
    gr, gi = gin[0].reshape(512, N), gin[1].reshape(512, N)
    ga[...] = jnp.concatenate([gr, gr], 1)
    gb[...] = jnp.concatenate([-gi, gi], 1)
    inputs_of(1)

    @pl.loop(0, Q)
    def _(q):
        stage1(1, q * Q, Q)

    send_a(1)
    for cp in load_in(3):
        cp.start()
    for u, k in PIECES:
        piece_arrived(u, k).wait()
        y_lines(u, (k,))
        b_piece(u, k).start()
    for h in range(2):
        bh_arrived(h).wait()
        z_lines(0, h)
        c_half(h).start()

    inputs_of(2)
    for q in range(EARLY):
        stage1(2, q * Q, Q)

    def step(t, carry):
        c = lax.rem(t, Q)
        g1 = t // Q + 2

        @pl.when(t < NU)
        def _():
            stage2(t)

        u3 = t - LAG3

        @pl.when(u3 >= 1)
        def _():
            stage3(u3)

        u4 = t - LAG4

        @pl.when(u4 >= 0)
        def _():
            stage4(u4)

        @pl.when(g1 < NG)
        def _():
            @pl.when(c == 0)
            def _():
                inputs_of(g1)

                @pl.when(g1 >= RA)
                def _():
                    a_sent(g1 - RA).wait()

            stage1(g1, c * Q, Q)

            @pl.when(c == 3)
            def _():
                send_a(g1)

                @pl.when(g1 + 2 < NG)
                def _():
                    for cp in load_in(g1 + 2):
                        cp.start()

        u5 = t - LAG5

        @pl.when(u5 >= 0)
        def _():
            @pl.when(lax.rem(u5, Q) == 0)
            def _():
                d_arrived(u5 // Q).wait()

            stage5(u5 // Q, lax.rem(u5, Q) * Q, Q)

        return carry

    steps = NU - LATE + LAG4
    lax.fori_loop(EARLY, steps, step, 0)
    rest = [u5 for u5 in range(steps - LAG5, NU - Q)]
    u3 = [u for u in range(steps - LAG3, NU)]
    for u in range(NU - LATE, NU):
        if u3:
            stage3(u3.pop(0))
        d_sent(u - RING).wait()
        for kk in range(Q):
            c_part(u, kk).wait_recv()
            y_lines_back(u, (kk,))
            for r in (2, 1, 3):
                d_part(u, r, kk).start()
        for u5 in rest[:2]:
            if u5 % Q == 0:
                d_arrived(u5 // Q).wait()
            stage5(u5 // Q, u5 % Q * Q, Q)
        rest = rest[2:]
    d_arrived(NG - 1).wait()

    for g in range(NG - RA, NG):
        a_sent(g).wait()
    for u in range(NU - RING, NU):
        b_copy(u).wait_send()
        c_copy(u).wait_send()
        d_sent(u).wait()


def unpack(phi, re, im, t5, phi_re, phi_im, hat_re, hat_im, wraw, st, st_last, w_sem, hat_sem, sem, last_sem):
    tab = pltpu.make_async_copy(t5.at[lax.axis_index("py")], wraw, w_sem)
    tab.start()
    hats, phis = ((re, hat_re), (im, hat_im)), (phi_re, phi_im)
    for i in range(FIELDS // HB):
        part = pl.ds(i * HB, HB)
        for k, (src, dst) in enumerate(hats):
            pltpu.make_async_copy(src.at[part], dst.at[part], hat_sem.at[k]).start()

    def last_copy(k):
        return pltpu.make_async_copy(st_last.at[k], phis[k].at[pl.ds(FIELDS - FG, FG)], last_sem.at[k])

    tab.wait()
    wide, narrow = right_table(*(wraw[i] for i in range(3)))
    w = wide, from_wide(narrow)

    @pl.loop(0, Q)
    def _(q):
        for i in range(Q):
            y = q * Q + i
            rows = pl.ds(pl.multiple_of(y * S, S), S)
            x = jnp.concatenate([phi[NU - Q + c, r, rows, :] for c in range(Q) for r in range(Q)], 0)
            out = right(x.T, w)
            for k, half in enumerate((out[:, :N], out[:, N:])):
                st_last[k, :, y] = half.reshape(FG, Z, N)

    for k in range(2):
        last_copy(k).start()

    def copy(i, k):
        slot = lax.rem(i, SLOTS)
        return pltpu.make_async_copy(st.at[slot, k], phis[k].at[pl.ds(i * FB, FB)], sem.at[slot, k])

    def phi_job(i, carry):
        slot = lax.rem(i, SLOTS)

        @pl.when(i >= SLOTS)
        def _():
            for k in range(2):
                copy(i - SLOTS, k).wait()

        for f in range(FB):
            for r in range(Q):
                p = phi[i * FB + f, r]
                for k, half in enumerate((p[:, :N], p[:, N:])):
                    st[slot, k, f, :, r * S:(r + 1) * S] = half.reshape(Y, S, N)
        for k in range(2):
            copy(i, k).start()
        return carry

    jobs = (FIELDS - FG) // FB
    lax.fori_loop(0, jobs, phi_job, 0)
    for k, (src, dst) in enumerate(hats):
        pltpu.make_async_copy(src, dst, hat_sem.at[k]).wait()
        last_copy(k).wait()
    for i in range(jobs - SLOTS, jobs):
        for k in range(2):
            copy(i, k).wait()


def in_hbm(x):
    return pltpu.with_memory_space_constraint(x, pltpu.HBM)


def solution(mesh):
    consts = tables()

    def local_solve(rho_re, rho_im, g_re, g_im):
        dma, vmem, hbm = pltpu.SemaphoreType.DMA, pltpu.VMEM, pl.BlockSpec(memory_space=pl.ANY)
        tabs = [jnp.asarray(c) for c in consts]
        field = jax.ShapeDtypeStruct((FIELDS, Y, Z, N), F32)
        packed = pl.pallas_call(
            kernel,
            out_shape=[pltpu.VMEM((NU, Q, L, L), F32)] + [pltpu.VMEM(field.shape, F32)] * 2,
            in_specs=[hbm] * 10,
            out_specs=[pl.BlockSpec(memory_space=pltpu.VMEM)] * 3,
            scratch_shapes=[
                vmem((2, 2, FG, Y, Z, N), F32),
                vmem((2, Y, Z, N), F32),
                vmem((6, 3, L, L), BF16),
                vmem((6, 256, 256), BF16),
                vmem((6, L, 256), BF16),
                vmem((512, L), F32), vmem((512, L), F32),
                vmem((RA, Q, 3, L, L), F32),
                vmem((AR, Q, L, L), F32),
                vmem((RING, Q, H, L), F32),
                vmem((RECV, 2, Q, H, L), F32),
                vmem((RING, Q, H, L), F32),
                vmem((RECV, 2, Q, H, L), F32),
                vmem((RING, 3, L, L), F32),
                dma((2,)), dma((BLOCKS,)), dma, dma((2,)), dma((RA,)), dma((AR,)),
                dma((RING,)), dma((RECV,)), dma((RING,)), dma((RECV,)), dma((LATE, Q)), dma((RING,)), dma((RG,)),
            ],
            compiler_params=pltpu.CompilerParams(collective_id=0, has_side_effects=True,
                                                 vmem_limit_bytes=24 << 20),
            name="spectral",
        )(*(in_hbm(x) for x in (jnp.transpose(rho_re, (0, 2, 3, 1)), jnp.transpose(rho_im, (0, 2, 3, 1)), g_re, g_im, *tabs)))
        packed = [pltpu.with_memory_space_constraint(x, pltpu.VMEM) for x in packed]
        phi_re, phi_im, hat_re, hat_im = pl.pallas_call(
            unpack,
            out_shape=[field] * Q,
            in_specs=[pl.BlockSpec(memory_space=pltpu.VMEM)] * 3 + [hbm],
            out_specs=[hbm] * Q,
            scratch_shapes=[vmem((3, L, L), BF16), vmem((SLOTS, 2, FB, Y, Z, N), F32),
                            vmem((2, FG, Y, Z, N), F32), dma, dma((2,)), dma((SLOTS, 2)), dma((2,))],
            compiler_params=pltpu.CompilerParams(vmem_limit_bytes=20 << 20),
            name="unpack",
        )(*packed, in_hbm(tabs[5]))
        return jnp.transpose(phi_re, (0, 3, 1, 2)), jnp.transpose(phi_im, (0, 3, 1, 2)), hat_re, hat_im

    space_layout = P("dp", None, "py", "pz")
    wave_layout = P("dp", "py", "pz", None)
    green_layout = P("py", "pz", None)
    return jax.shard_map(local_solve, mesh=mesh,
                         in_specs=(space_layout, space_layout, green_layout, green_layout),
                         out_specs=(space_layout, space_layout, wave_layout, wave_layout),
                         check_vma=False)
```

```python
import functools

import jax
import jax.numpy as jnp
import ml_dtypes
import numpy as np
from jax import lax
from jax.experimental import pallas as pl
from jax.experimental.pallas import tpu as pltpu
from jax.sharding import PartitionSpec as P

MESH = pl.DeviceIdType.MESH
L, H, Z, Y, S, Q = 128, 64, 32, 16, 8, 4
F32, BF16 = jnp.float32, jnp.bfloat16
N = 64
FIELDS = 32
FG = 4
NG = FIELDS // FG
NU = NG * 4
NPY, NPZ = 4, 2
LAG3, LAG4 = 2, 4
LAG5 = LAG4 + 5
RING = 4
RECV = 6
RG = 4
RA = 3
AR = 16
BLOCKS = 2
NY = 16 // BLOCKS
EARLY = 2
PIECES = [(u, k) for u in range(EARLY) for k in range(4)]
LATE = 3
FB, SLOTS = 4, 4
HB = 8


def dft(sign):
    jk = np.outer(np.arange(N), np.arange(N)) % N
    c, s = np.cos(2 * np.pi * jk / N) / S, sign * np.sin(2 * np.pi * jk / N) / S
    return np.stack([np.stack([c, -s], 1), np.stack([s, c], 1)])


def split_np(w):
    w = np.asarray(w, np.float32)
    parts = []
    for _ in range(3):
        part = w.astype(ml_dtypes.bfloat16)
        parts.append(part)
        w = w - part.astype(np.float32)
    return np.stack(parts)


def tables():
    fwd, inv = dft(-1), dft(1)
    i16, i32 = np.arange(Y), np.arange(Z)
    w1, w2, w3, w3i, w4, w5 = [], [], [], [], [], []
    for a in range(NPY):
        to = [Y * ((a + r) % Q) + i16 for r in range(Q)]
        frm = [Y * ((a - r) % Q) + i16 for r in range(Q)]
        out = np.stack([fwd[:, k] for k in to]).reshape(Q, 2, Q, Q, 2, N)
        w1.append(out.transpose(Q, 5, 0, 2, 3, 1).reshape(L, L))
        inn = np.stack([inv[:, :, :, k] for k in frm]).reshape(Q, 2, N, 2, Q, Q)
        w5.append(inn.transpose(Q, 0, 5, 3, 1, 2).reshape(L, L))
        for b in range(NPZ):
            half = [Z * (b ^ q) + i32 for q in range(2)]
            m = np.stack([fwd[:, k] for k in half])
            m = np.stack([m[..., y] for y in frm])
            w2.append(m.transpose(1, 2, 3, 0, Q, 5).reshape(L, L))
            m = np.stack([inv[:, y] for y in to])
            m = np.stack([m[..., k] for k in half])
            w4.append(m.transpose(1, 2, 3, 0, Q, 5).reshape(L, L))
    for b in range(NPZ):
        half = [Z * (b ^ q) + i32 for q in range(2)]
        m = np.stack([fwd[..., z] for z in half])
        w3.append(m.transpose(0, 3, Q, 1, 2).reshape(L, L))
        m = np.stack([inv[:, z] for z in half])
        w3i.append(m.transpose(3, Q, 0, 1, 2).reshape(L, L))
    return [np.stack([split_np(w) for w in ws]) for ws in (w1, w2, w3, w3i, w4, w5)]


def split3(x):
    hi = x.astype(BF16)
    rest = x - hi.astype(F32)
    mid = rest.astype(BF16)
    return hi, mid, (rest - mid.astype(F32)).astype(BF16)


def dot(a, b):
    return jnp.dot(a, b, preferred_element_type=F32)


def left(w, x):
    hi, mid, lo = split3(x)
    wide = dot(w[0][...], jnp.concatenate([hi, mid], 0))
    return wide[:L] + (wide[L:] + dot(w[1][...], jnp.concatenate([hi, lo], 0)))


def right(x, w):
    hi, mid, lo = split3(x)
    wide = dot(jnp.concatenate([hi, mid], 1), w[0][...])
    return wide[:, :L] + (wide[:, L:] + dot(jnp.concatenate([hi, lo], 1), w[1][...]))


def left_table(w1, w2, w3):
    pairs = [jnp.concatenate([a, b], 1) for a, b in ((w1, w1), (w2, w2), (w3, w1))]
    return jnp.concatenate(pairs[:2], 0), pairs[2]


def right_table(w1, w2, w3):
    return jnp.concatenate([jnp.concatenate([w1, w2], 1)] * 2, 0), jnp.concatenate([w3, w1], 1)


def from_wide(w):
    return jnp.concatenate([w[:, :L], w[:, L:]], 0)


def swap_lanes(tiles):
    lane = lax.broadcasted_iota(jnp.int32, tiles[0].shape, 1)
    odd, high = (lane // Z) % 2 == 1, lane >= H
    t = list(tiles)
    for lo in (0, 2):
        a, b = t[lo], t[lo + 1]
        t[lo] = jnp.where(odd, pltpu.roll(b, Z, 1), a)
        t[lo + 1] = jnp.where(odd, b, pltpu.roll(a, 96, 1))
    for lo in (0, 1):
        a, b = t[lo], t[lo + 2]
        t[lo] = jnp.where(high, pltpu.roll(b, H, 1), a)
        t[lo + 2] = jnp.where(high, b, pltpu.roll(a, H, 1))
    return t


def kernel(rho_re, rho_im, g_re, g_im, t1, t2, t3, t3i, t4, t5, d_recv, hat_re, hat_im,
           rin, gin, wraw, wbig, wsmall, ga, gb, a_send, a_recv, b_send, b_recv, c_send, c_recv, d_send,
           in_sem, first_sem, g_sem, w_sem, as_sem, ar_sem, bs_sem, br_sem, cs_sem, cr_sem, part_sem,
           ds_sem, dr_sem):
    me, mz = lax.axis_index("py"), lax.axis_index("pz")
    zero = lax.axis_index("dp")

    def py_peer(r):
        return (zero, mz, lax.rem(me + r, NPY))

    pz_peer = (zero, 1 - mz, me)

    def load_in(g):
        slot = lax.rem(g, 2)
        return [pltpu.make_async_copy(src.at[pl.ds(g * FG, FG)], rin.at[slot, i], in_sem.at[slot])
                for i, src in enumerate((rho_re, rho_im))]

    def inputs_of(g):
        ref = rin.at[lax.rem(g, 2)]
        pltpu.make_async_copy(ref, ref, in_sem.at[lax.rem(g, 2)]).wait()

    def load_first(q):
        ys = pl.ds(q * NY, NY)
        return [pltpu.make_async_copy(src.at[pl.ds(0, FG), ys], rin.at[0, i, :, ys], first_sem.at[q])
                for i, src in enumerate((rho_re, rho_im))]

    def first_loaded(q):
        ref = rin.at[0, :, :, pl.ds(q * NY, NY)]
        return pltpu.make_async_copy(ref, ref, first_sem.at[q])

    barrier = pltpu.get_barrier_semaphore()
    for peer in [py_peer(r) for r in (1, 2, 3)] + [pz_peer]:
        pl.semaphore_signal(barrier, inc=1, device_id=peer, device_id_type=MESH)
    both = me * NPZ + mz
    tabs = [pltpu.make_async_copy(t.at[i], wraw.at[k], w_sem.at[min(k, 1)])
            for k, (t, i) in enumerate(((t1, me), (t2, both), (t3, mz), (t3i, mz), (t4, both), (t5, me)))]
    greens = [pltpu.make_async_copy(src, gin.at[i], g_sem) for i, src in enumerate((g_re, g_im))]
    firsts = [cp for q in range(BLOCKS) for cp in load_first(q)]
    for cp in tabs[:1] + firsts + tabs[1:] + greens + load_in(1):
        cp.start()

    def table(k):
        wide, narrow = (left_table if k in (1, Q) else right_table)(*(wraw[k, i] for i in range(3)))
        wbig[k] = wide
        wsmall[k] = narrow

    def lmat(k):
        return wbig.at[k], wsmall.at[k]

    def rmat(k):
        return wbig[k], from_wide(wsmall[k])

    def stage1(g, y0, ny):
        slot, ring = lax.rem(g, 2), lax.rem(g, RA)
        w = rmat(0)
        for i in range(ny):
            y = y0 + i
            x = jnp.concatenate([rin[slot, 0, :, y].reshape(L, N), rin[slot, 1, :, y].reshape(L, N)], 1)
            out = right(x, w).T
            rows = pl.ds(pl.multiple_of(y * S, S), S)
            for c in range(Q):
                for r in range(Q):
                    tile = out[(r * Q + c) * S:(r * Q + c + 1) * S]
                    if r == 0:
                        a_recv[lax.rem(g * Q + c, AR), 0, rows, :] = tile
                    else:
                        a_send[ring, c, r - 1, rows, :] = tile

    def a_copy(u, r):
        g, c = u // Q, lax.rem(u, Q)
        ring = lax.rem(g, RA)
        return pltpu.make_async_remote_copy(
            src_ref=a_send.at[ring, c, r - 1], dst_ref=a_recv.at[lax.rem(u, AR), r], send_sem=as_sem.at[ring],
            recv_sem=ar_sem.at[lax.rem(u, AR)], device_id=py_peer(r), device_id_type=MESH)

    def a_piece(u, k, r, y0, ny):
        part = (pl.ds(y0, ny), pl.ds(2 * k, 2))
        src, dst = (ref.reshape(Y, S, L).at[part] for ref in (a_send.at[0, u, r - 1], a_recv.at[u, r]))
        return pltpu.make_async_remote_copy(
            src_ref=src, dst_ref=dst, send_sem=as_sem.at[0], recv_sem=part_sem.at[u, k],
            device_id=py_peer(r), device_id_type=MESH)

    def piece_arrived(u, k):
        ref = a_recv.at[u, pl.ds(1, 3), pl.ds(Z * k, Z)]
        return pltpu.make_async_copy(ref, ref, part_sem.at[u, k])

    def c_part(u, kk):
        ring = lax.rem(u, RING)
        return pltpu.make_async_remote_copy(
            src_ref=c_send.at[ring, kk], dst_ref=c_recv.at[lax.rem(u, RECV), 1, kk], send_sem=cs_sem.at[ring],
            recv_sem=part_sem.at[u - (NU - LATE), kk], device_id=pz_peer, device_id_type=MESH)

    def d_part(u, r, kk):
        part = (slice(None), pl.ds(2 * kk, 2))
        src, dst = (ref.reshape(Y, S, L).at[part] for ref in (d_send.at[u % RING, r - 1], d_recv.at[u, r]))
        return pltpu.make_async_remote_copy(
            src_ref=src, dst_ref=dst, send_sem=ds_sem.at[u % RING], recv_sem=dr_sem.at[(NG - 1) % RG],
            device_id=py_peer(r), device_id_type=MESH)

    def a_sent(g):
        ring = lax.rem(g, RA)
        return pltpu.make_async_copy(a_send.at[ring], a_send.at[ring], as_sem.at[ring])

    def a_arrived(u):
        ref = a_recv.at[lax.rem(u, AR), pl.ds(1, 3)]
        return pltpu.make_async_copy(ref, ref, ar_sem.at[lax.rem(u, AR)])

    def d_sent(u):
        ring = lax.rem(u, RING)
        return pltpu.make_async_copy(d_send.at[ring], d_send.at[ring], ds_sem.at[ring])

    def d_arrived(g):
        ref = d_recv.at[pl.ds(g * Q, Q), pl.ds(1, 3)]
        return pltpu.make_async_copy(ref, ref, dr_sem.at[lax.rem(g, RG)])

    def b_copy(u):
        ring = lax.rem(u, RING)
        return pltpu.make_async_remote_copy(
            src_ref=b_send.at[ring], dst_ref=b_recv.at[lax.rem(u, RECV), 1], send_sem=bs_sem.at[ring], recv_sem=br_sem.at[lax.rem(u, RECV)],
            device_id=pz_peer, device_id_type=MESH)

    def b_piece(u, k):
        return pltpu.make_async_remote_copy(
            src_ref=b_send.at[u, k], dst_ref=b_recv.at[u, 1, k], send_sem=bs_sem.at[u],
            recv_sem=br_sem.at[u] if u else part_sem.at[EARLY, k // 2], device_id=pz_peer, device_id_type=MESH)

    def bh_arrived(h):
        ref = b_recv.at[0, 1, pl.ds(2 * h, 2)]
        return pltpu.make_async_copy(ref, ref, part_sem.at[EARLY, h])

    def c_half(h):
        kk = pl.ds(2 * h, 2)
        return pltpu.make_async_remote_copy(
            src_ref=c_send.at[0, kk], dst_ref=c_recv.at[0, 1, kk], send_sem=cs_sem.at[0], recv_sem=cr_sem.at[0],
            device_id=pz_peer, device_id_type=MESH)

    def c_copy(u):
        ring = lax.rem(u, RING)
        return pltpu.make_async_remote_copy(
            src_ref=c_send.at[ring], dst_ref=c_recv.at[lax.rem(u, RECV), 1], send_sem=cs_sem.at[ring], recv_sem=cr_sem.at[lax.rem(u, RECV)],
            device_id=pz_peer, device_id_type=MESH)

    def d_copy(u, r):
        ring = lax.rem(u, RING)
        return pltpu.make_async_remote_copy(
            src_ref=d_send.at[ring, r - 1], dst_ref=d_recv.at[u, r], send_sem=ds_sem.at[ring],
            recv_sem=dr_sem.at[lax.rem(u // Q, RG)], device_id=py_peer(r), device_id_type=MESH)

    def send_a(g):
        for c in range(Q):
            for r in (2, 1, 3):
                a_copy(g * Q + c, r).start()

    def y_lines(u, kks):
        ring, slot, arrived = lax.rem(u, RING), lax.rem(u, RECV), lax.rem(u, AR)
        cols = [jnp.concatenate([a_recv[arrived, r, pl.ds(kk * 2 + ri, Y, stride=S), :]
                                 for r in range(Q) for ri in range(2)], 0) for kk in kks]
        out = left(lmat(1), jnp.concatenate(cols, 1))
        for i, kk in enumerate(kks):
            b_recv[slot, 0, kk] = out[:H, i * L:(i + 1) * L]
            b_send[ring, kk] = out[H:, i * L:(i + 1) * L]

    def stage2(u):
        a_arrived(u).wait()

        @pl.when(u >= RING)
        def _():
            b_copy(u - RING).wait_send()

        for kp in range(2):
            y_lines(u, (2 * kp, 2 * kp + 1))
        b_copy(u).start()

    def z_lines(u, kp):
        ring, c, f0 = lax.rem(u, RING), lax.rem(u, Q), u // Q * FG
        wf, wi = rmat(2), rmat(3)
        rows = []
        for kk in (2 * kp, 2 * kp + 1):
            rows += swap_lanes([b_recv[lax.rem(u, RECV), q, kk, ri * Z:(ri + 1) * Z, :] for q in range(2) for ri in range(2)])
        spec = right(jnp.concatenate(rows, 0), wf)
        hats = []
        for i in range(2):
            kk = 2 * kp + i
            gr = pl.ds(pl.multiple_of((c * Q + kk) * Z, Z), Z)
            gan, gbn = ga[gr, :], gb[gr, :]
            for f in range(FG):
                s = spec[(i * FG + f) * Z:(i * FG + f + 1) * Z]
                h = s * gan + pltpu.roll(s, H, 1) * gbn
                hat_re[f0 + f, c * Q + kk] = h[:, :N]
                hat_im[f0 + f, c * Q + kk] = h[:, N:]
                hats.append(h)
        back = right(jnp.concatenate(hats, 0), wi)
        for i in range(2):
            kk = 2 * kp + i
            t = swap_lanes([back[(i * FG + f) * Z:(i * FG + f + 1) * Z] for f in range(FG)])
            for ri in range(2):
                c_recv[lax.rem(u, RECV), 0, kk, ri * Z:(ri + 1) * Z, :] = t[ri]
                c_send[ring, kk, ri * Z:(ri + 1) * Z, :] = t[2 + ri]

    def stage3(u):
        b_copy(u).wait_recv()

        @pl.when(u >= RING)
        def _():
            c_copy(u - RING).wait_send()

        for kp in range(2):
            z_lines(u, kp)

        @pl.when(u < NU - LATE)
        def _():
            c_copy(u).start()

        @pl.when(u >= NU - LATE)
        def _():
            for kk in range(Q):
                c_part(u, kk).start()

    def y_lines_back(u, kks):
        ring = lax.rem(u, RING)
        cols = [jnp.concatenate([c_recv[lax.rem(u, RECV), q, kk] for q in range(2)], 0) for kk in kks]
        out = left(lmat(Q), jnp.concatenate(cols, 1))
        for i, kk in enumerate(kks):
            for r in range(Q):
                for ro in range(2):
                    rows = pl.ds(kk * 2 + ro, Y, stride=S)
                    tile = out[(r * 2 + ro) * Y:(r * 2 + ro + 1) * Y, i * L:(i + 1) * L]
                    if r == 0:
                        d_recv[u, 0, rows, :] = tile
                    else:
                        d_send[ring, r - 1, rows, :] = tile

    def stage4(u):
        c_copy(u).wait_recv()

        @pl.when(u >= RING)
        def _():
            d_sent(u - RING).wait()

        for kp in range(2):
            y_lines_back(u, (2 * kp, 2 * kp + 1))
        for r in (2, 1, 3):
            d_copy(u, r).start()

    def stage5(g, y0, ny):
        w = rmat(5)
        for i in range(ny):
            y = y0 + i
            rows = pl.ds(pl.multiple_of(y * S, S), S)
            x = jnp.concatenate([d_recv[g * Q + c, r, rows, :] for c in range(Q) for r in range(Q)], 0)
            out = right(x.T, w)
            for f in range(FG):
                for r in range(Q):
                    d_recv[g * Q + f, r, rows, :] = out[(f * Q + r) * S:(f * Q + r + 1) * S]

    odd = lax.rem(me, 2)
    order = (2 - odd, 3 - odd, 1 + 2 * odd)
    tabs[0].wait()
    table(0)
    for q in range(BLOCKS):
        first_loaded(q).wait()
        stage1(0, q * NY, NY)
        if q == 0:
            pl.semaphore_wait(barrier, Q)
        for r in order:
            a_piece(0, 0, r, q * NY, NY).start()
    for u, k in PIECES[1:]:
        for r in order:
            a_piece(u, k, r, 0, Y).start()
    for u in range(EARLY, Q):
        for r in (2, 1, 3):
            a_copy(u, r).start()
    for cp in load_in(2):
        cp.start()
    pltpu.make_async_copy(wraw.at[pl.ds(1, 5)], wraw.at[pl.ds(1, 5)], w_sem.at[1]).wait()
    for k in range(1, 6):
        table(k)
    pltpu.make_async_copy(gin, gin, g_sem).wait()
    gr, gi = gin[0].reshape(512, N), gin[1].reshape(512, N)
    ga[...] = jnp.concatenate([gr, gr], 1)
    gb[...] = jnp.concatenate([-gi, gi], 1)
    inputs_of(1)

    @pl.loop(0, Q)
    def _(q):
        stage1(1, q * Q, Q)

    send_a(1)
    for cp in load_in(3):
        cp.start()
    for u, k in PIECES:
        piece_arrived(u, k).wait()
        y_lines(u, (k,))
        b_piece(u, k).start()
    for h in range(2):
        bh_arrived(h).wait()
        z_lines(0, h)
        c_half(h).start()

    inputs_of(2)
    for q in range(EARLY):
        stage1(2, q * Q, Q)

    def step(t, carry):
        c = lax.rem(t, Q)
        g1 = t // Q + 2

        @pl.when(t < NU)
        def _():
            stage2(t)

        u3 = t - LAG3

        @pl.when(u3 >= 1)
        def _():
            stage3(u3)

        u4 = t - LAG4

        @pl.when(u4 >= 0)
        def _():
            stage4(u4)

        @pl.when(g1 < NG)
        def _():
            @pl.when(c == 0)
            def _():
                inputs_of(g1)

                @pl.when(g1 >= RA)
                def _():
                    a_sent(g1 - RA).wait()

            stage1(g1, c * Q, Q)

            @pl.when(c == 3)
            def _():
                send_a(g1)

                @pl.when(g1 + 2 < NG)
                def _():
                    for cp in load_in(g1 + 2):
                        cp.start()

        u5 = t - LAG5

        @pl.when(u5 >= 0)
        def _():
            @pl.when(lax.rem(u5, Q) == 0)
            def _():
                d_arrived(u5 // Q).wait()

            stage5(u5 // Q, lax.rem(u5, Q) * Q, Q)

        return carry

    steps = NU - LATE + LAG4
    lax.fori_loop(EARLY, steps, step, 0)
    rest = [u5 for u5 in range(steps - LAG5, NU - Q)]
    u3 = [u for u in range(steps - LAG3, NU)]
    for u in range(NU - LATE, NU):
        if u3:
            stage3(u3.pop(0))
        d_sent(u - RING).wait()
        for kk in range(Q):
            c_part(u, kk).wait_recv()
            y_lines_back(u, (kk,))
            for r in (2, 1, 3):
                d_part(u, r, kk).start()
        for u5 in rest[:2]:
            if u5 % Q == 0:
                d_arrived(u5 // Q).wait()
            stage5(u5 // Q, u5 % Q * Q, Q)
        rest = rest[2:]
    d_arrived(NG - 1).wait()

    for g in range(NG - RA, NG):
        a_sent(g).wait()
    for u in range(NU - RING, NU):
        b_copy(u).wait_send()
        c_copy(u).wait_send()
        d_sent(u).wait()


def unpack(phi, re, im, t5, phi_re, phi_im, hat_re, hat_im, wraw, st, st_last, w_sem, hat_sem, sem, last_sem):
    tab = pltpu.make_async_copy(t5.at[lax.axis_index("py")], wraw, w_sem)
    tab.start()
    hats, phis = ((re, hat_re), (im, hat_im)), (phi_re, phi_im)
    for i in range(FIELDS // HB):
        part = pl.ds(i * HB, HB)
        for k, (src, dst) in enumerate(hats):
            pltpu.make_async_copy(src.at[part], dst.at[part], hat_sem.at[k]).start()

    def last_copy(k):
        return pltpu.make_async_copy(st_last.at[k], phis[k].at[pl.ds(FIELDS - FG, FG)], last_sem)

    tab.wait()
    wide, narrow = right_table(*(wraw[i] for i in range(3)))
    w = wide, from_wide(narrow)

    @pl.loop(0, Q)
    def _(q):
        for i in range(Q):
            y = q * Q + i
            rows = pl.ds(pl.multiple_of(y * S, S), S)
            x = jnp.concatenate([phi[NU - Q + c, r, rows, :] for c in range(Q) for r in range(Q)], 0)
            out = right(x.T, w)
            for k, half in enumerate((out[:, :N], out[:, N:])):
                st_last[k, :, y] = half.reshape(FG, Z, N)

    for k in range(2):
        last_copy(k).start()

    def copy(i, k):
        slot = lax.rem(i, SLOTS)
        return pltpu.make_async_copy(st.at[slot, k], phis[k].at[pl.ds(i * FB, FB)], sem.at[slot])

    def written(i):
        slot = lax.rem(i, SLOTS)
        pltpu.make_async_copy(st.at[slot], st.at[slot], sem.at[slot]).wait()

    def phi_job(i, carry):
        slot = lax.rem(i, SLOTS)

        @pl.when(i >= SLOTS)
        def _():
            written(i - SLOTS)

        for f in range(FB):
            for r in range(Q):
                p = phi[i * FB + f, r]
                for k, half in enumerate((p[:, :N], p[:, N:])):
                    st[slot, k, f, :, r * S:(r + 1) * S] = half.reshape(Y, S, N)
        for k in range(2):
            copy(i, k).start()
        return carry

    jobs = (FIELDS - FG) // FB
    lax.fori_loop(0, jobs, phi_job, 0)
    for k, (src, dst) in enumerate(hats):
        pltpu.make_async_copy(src, dst, hat_sem.at[k]).wait()
    pltpu.make_async_copy(st_last, st_last, last_sem).wait()
    for i in range(jobs - SLOTS, jobs):
        written(i)


def in_hbm(x):
    return pltpu.with_memory_space_constraint(x, pltpu.HBM)


def solution(mesh):
    consts = tables()

    def local_solve(rho_re, rho_im, g_re, g_im):
        dma, vmem, hbm = pltpu.SemaphoreType.DMA, pltpu.VMEM, pl.BlockSpec(memory_space=pl.ANY)
        tabs = [jnp.asarray(c) for c in consts]
        field = jax.ShapeDtypeStruct((FIELDS, Y, Z, N), F32)
        packed = pl.pallas_call(
            kernel,
            out_shape=[pltpu.VMEM((NU, Q, L, L), F32)] + [pltpu.VMEM(field.shape, F32)] * 2,
            in_specs=[hbm] * 10,
            out_specs=[pl.BlockSpec(memory_space=pltpu.VMEM)] * 3,
            scratch_shapes=[
                vmem((2, 2, FG, Y, Z, N), F32),
                vmem((2, Y, Z, N), F32),
                vmem((6, 3, L, L), BF16),
                vmem((6, 256, 256), BF16),
                vmem((6, L, 256), BF16),
                vmem((512, L), F32), vmem((512, L), F32),
                vmem((RA, Q, 3, L, L), F32),
                vmem((AR, Q, L, L), F32),
                vmem((RING, Q, H, L), F32),
                vmem((RECV, 2, Q, H, L), F32),
                vmem((RING, Q, H, L), F32),
                vmem((RECV, 2, Q, H, L), F32),
                vmem((RING, 3, L, L), F32),
                dma((2,)), dma((BLOCKS,)), dma, dma((2,)), dma((RA,)), dma((AR,)),
                dma((RING,)), dma((RECV,)), dma((RING,)), dma((RECV,)), dma((LATE, Q)), dma((RING,)), dma((RG,)),
            ],
            compiler_params=pltpu.CompilerParams(collective_id=0, has_side_effects=True,
                                                 vmem_limit_bytes=24 << 20),
            name="spectral",
        )(*(in_hbm(x) for x in (jnp.transpose(rho_re, (0, 2, 3, 1)), jnp.transpose(rho_im, (0, 2, 3, 1)), g_re, g_im, *tabs)))
        packed = [pltpu.with_memory_space_constraint(x, pltpu.VMEM) for x in packed]
        phi_re, phi_im, hat_re, hat_im = pl.pallas_call(
            unpack,
            out_shape=[field] * Q,
            in_specs=[pl.BlockSpec(memory_space=pltpu.VMEM)] * 3 + [hbm],
            out_specs=[hbm] * Q,
            scratch_shapes=[vmem((3, L, L), BF16), vmem((SLOTS, 2, FB, Y, Z, N), F32),
                            vmem((2, FG, Y, Z, N), F32), dma, dma((2,)), dma((SLOTS,)), dma],
            compiler_params=pltpu.CompilerParams(vmem_limit_bytes=20 << 20),
            name="unpack",
        )(*packed, in_hbm(tabs[5]))
        return jnp.transpose(phi_re, (0, 3, 1, 2)), jnp.transpose(phi_im, (0, 3, 1, 2)), hat_re, hat_im

    space_layout = P("dp", None, "py", "pz")
    wave_layout = P("dp", "py", "pz", None)
    green_layout = P("py", "pz", None)
    return jax.shard_map(local_solve, mesh=mesh,
                         in_specs=(space_layout, space_layout, green_layout, green_layout),
                         out_specs=(space_layout, space_layout, wave_layout, wave_layout),
                         check_vma=False)
```

```python
import functools

import jax
import jax.numpy as jnp
import ml_dtypes
import numpy as np
from jax import lax
from jax.experimental import pallas as pl
from jax.experimental.pallas import tpu as pltpu
from jax.sharding import PartitionSpec as P

MESH = pl.DeviceIdType.MESH
L, H, Z, Y, S, Q = 128, 64, 32, 16, 8, 4
F32, BF16 = jnp.float32, jnp.bfloat16
N = 64
FIELDS = 32
FG = 4
NG = FIELDS // FG
NU = NG * 4
NPY, NPZ = 4, 2
LAG3, LAG4 = 2, 4
LAG5 = LAG4 + 5
RING = 3
RECV = 6
RG = 4
RA = 3
AR = 16
BLOCKS = 2
NY = 16 // BLOCKS
EARLY = 2
PIECES = [(u, k) for u in range(EARLY) for k in range(4)]
LATE = 3
FB, SLOTS = 4, 4
HB = 8


def dft(sign):
    jk = np.outer(np.arange(N), np.arange(N)) % N
    c, s = np.cos(2 * np.pi * jk / N) / S, sign * np.sin(2 * np.pi * jk / N) / S
    return np.stack([np.stack([c, -s], 1), np.stack([s, c], 1)])


def split_np(w):
    w = np.asarray(w, np.float32)
    parts = []
    for _ in range(3):
        part = w.astype(ml_dtypes.bfloat16)
        parts.append(part)
        w = w - part.astype(np.float32)
    return np.stack(parts)


def tables():
    fwd, inv = dft(-1), dft(1)
    i16, i32 = np.arange(Y), np.arange(Z)
    w1, w2, w3, w3i, w4, w5 = [], [], [], [], [], []
    for a in range(NPY):
        to = [Y * ((a + r) % Q) + i16 for r in range(Q)]
        frm = [Y * ((a - r) % Q) + i16 for r in range(Q)]
        out = np.stack([fwd[:, k] for k in to]).reshape(Q, 2, Q, Q, 2, N)
        w1.append(out.transpose(Q, 5, 0, 2, 3, 1).reshape(L, L))
        inn = np.stack([inv[:, :, :, k] for k in frm]).reshape(Q, 2, N, 2, Q, Q)
        w5.append(inn.transpose(Q, 0, 5, 3, 1, 2).reshape(L, L))
        for b in range(NPZ):
            half = [Z * (b ^ q) + i32 for q in range(2)]
            m = np.stack([fwd[:, k] for k in half])
            m = np.stack([m[..., y] for y in frm])
            w2.append(m.transpose(1, 2, 3, 0, Q, 5).reshape(L, L))
            m = np.stack([inv[:, y] for y in to])
            m = np.stack([m[..., k] for k in half])
            w4.append(m.transpose(1, 2, 3, 0, Q, 5).reshape(L, L))
    for b in range(NPZ):
        half = [Z * (b ^ q) + i32 for q in range(2)]
        m = np.stack([fwd[..., z] for z in half])
        w3.append(m.transpose(0, 3, Q, 1, 2).reshape(L, L))
        m = np.stack([inv[:, z] for z in half])
        w3i.append(m.transpose(3, Q, 0, 1, 2).reshape(L, L))
    return [np.stack([split_np(w) for w in ws]) for ws in (w1, w2, w3, w3i, w4, w5)]


def split3(x):
    hi = x.astype(BF16)
    rest = x - hi.astype(F32)
    mid = rest.astype(BF16)
    return hi, mid, (rest - mid.astype(F32)).astype(BF16)


def dot(a, b):
    return jnp.dot(a, b, preferred_element_type=F32)


def left(w, x):
    hi, mid, lo = split3(x)
    wide = dot(w[0][...], jnp.concatenate([hi, mid], 0))
    return wide[:L] + (wide[L:] + dot(w[1][...], jnp.concatenate([hi, lo], 0)))


def right(x, w):
    hi, mid, lo = split3(x)
    wide = dot(jnp.concatenate([hi, mid], 1), w[0][...])
    return wide[:, :L] + (wide[:, L:] + dot(jnp.concatenate([hi, lo], 1), w[1][...]))


def left_table(w1, w2, w3):
    pairs = [jnp.concatenate([a, b], 1) for a, b in ((w1, w1), (w2, w2), (w3, w1))]
    return jnp.concatenate(pairs[:2], 0), pairs[2]


def right_table(w1, w2, w3):
    return jnp.concatenate([jnp.concatenate([w1, w2], 1)] * 2, 0), jnp.concatenate([w3, w1], 1)


def from_wide(w):
    return jnp.concatenate([w[:, :L], w[:, L:]], 0)


def swap_lanes(tiles):
    lane = lax.broadcasted_iota(jnp.int32, tiles[0].shape, 1)
    odd, high = (lane // Z) % 2 == 1, lane >= H
    t = list(tiles)
    for lo in (0, 2):
        a, b = t[lo], t[lo + 1]
        t[lo] = jnp.where(odd, pltpu.roll(b, Z, 1), a)
        t[lo + 1] = jnp.where(odd, b, pltpu.roll(a, 96, 1))
    for lo in (0, 1):
        a, b = t[lo], t[lo + 2]
        t[lo] = jnp.where(high, pltpu.roll(b, H, 1), a)
        t[lo + 2] = jnp.where(high, b, pltpu.roll(a, H, 1))
    return t


def kernel(rho_re, rho_im, g_re, g_im, t1, t2, t3, t3i, t4, t5, d_recv, hat_re, hat_im,
           rin, gin, wraw, wbig, wsmall, ga, gb, a_send, a_recv, b_send, b_recv, c_send, c_recv, d_send,
           in_sem, first_sem, g_sem, w_sem, as_sem, ar_sem, bs_sem, br_sem, cs_sem, cr_sem, part_sem,
           ds_sem, dr_sem):
    me, mz = lax.axis_index("py"), lax.axis_index("pz")
    zero = lax.axis_index("dp")

    def py_peer(r):
        return (zero, mz, lax.rem(me + r, NPY))

    pz_peer = (zero, 1 - mz, me)

    def load_in(g):
        slot = lax.rem(g, 2)
        return [pltpu.make_async_copy(src.at[pl.ds(g * FG, FG)], rin.at[slot, i], in_sem.at[slot])
                for i, src in enumerate((rho_re, rho_im))]

    def inputs_of(g):
        ref = rin.at[lax.rem(g, 2)]
        pltpu.make_async_copy(ref, ref, in_sem.at[lax.rem(g, 2)]).wait()

    def load_first(q):
        ys = pl.ds(q * NY, NY)
        return [pltpu.make_async_copy(src.at[pl.ds(0, FG), ys], rin.at[0, i, :, ys], first_sem.at[q])
                for i, src in enumerate((rho_re, rho_im))]

    def first_loaded(q):
        ref = rin.at[0, :, :, pl.ds(q * NY, NY)]
        return pltpu.make_async_copy(ref, ref, first_sem.at[q])

    barrier = pltpu.get_barrier_semaphore()
    for peer in [py_peer(r) for r in (1, 2, 3)] + [pz_peer]:
        pl.semaphore_signal(barrier, inc=1, device_id=peer, device_id_type=MESH)
    both = me * NPZ + mz
    tabs = [pltpu.make_async_copy(t.at[i], wraw.at[k], w_sem.at[min(k, 1)])
            for k, (t, i) in enumerate(((t1, me), (t2, both), (t3, mz), (t3i, mz), (t4, both), (t5, me)))]
    greens = [pltpu.make_async_copy(src, gin.at[i], g_sem) for i, src in enumerate((g_re, g_im))]
    firsts = [cp for q in range(BLOCKS) for cp in load_first(q)]
    for cp in tabs[:1] + firsts + tabs[1:] + greens + load_in(1):
        cp.start()

    def table(k):
        wide, narrow = (left_table if k in (1, Q) else right_table)(*(wraw[k, i] for i in range(3)))
        wbig[k] = wide
        wsmall[k] = narrow

    def lmat(k):
        return wbig.at[k], wsmall.at[k]

    def rmat(k):
        return wbig[k], from_wide(wsmall[k])

    def stage1(g, y0, ny):
        slot, ring = lax.rem(g, 2), lax.rem(g, RA)
        w = rmat(0)
        for i in range(ny):
            y = y0 + i
            x = jnp.concatenate([rin[slot, 0, :, y].reshape(L, N), rin[slot, 1, :, y].reshape(L, N)], 1)
            out = right(x, w).T
            rows = pl.ds(pl.multiple_of(y * S, S), S)
            for c in range(Q):
                for r in range(Q):
                    tile = out[(r * Q + c) * S:(r * Q + c + 1) * S]
                    if r == 0:
                        a_recv[lax.rem(g * Q + c, AR), 0, rows, :] = tile
                    else:
                        a_send[ring, c, r - 1, rows, :] = tile

    def a_copy(u, r):
        g, c = u // Q, lax.rem(u, Q)
        ring = lax.rem(g, RA)
        return pltpu.make_async_remote_copy(
            src_ref=a_send.at[ring, c, r - 1], dst_ref=a_recv.at[lax.rem(u, AR), r], send_sem=as_sem.at[ring],
            recv_sem=ar_sem.at[lax.rem(u, AR)], device_id=py_peer(r), device_id_type=MESH)

    def a_piece(u, k, r, y0, ny):
        part = (pl.ds(y0, ny), pl.ds(2 * k, 2))
        src, dst = (ref.reshape(Y, S, L).at[part] for ref in (a_send.at[0, u, r - 1], a_recv.at[u, r]))
        return pltpu.make_async_remote_copy(
            src_ref=src, dst_ref=dst, send_sem=as_sem.at[0], recv_sem=part_sem.at[u, k],
            device_id=py_peer(r), device_id_type=MESH)

    def piece_arrived(u, k):
        ref = a_recv.at[u, pl.ds(1, 3), pl.ds(Z * k, Z)]
        return pltpu.make_async_copy(ref, ref, part_sem.at[u, k])

    def c_part(u, kk):
        ring = lax.rem(u, RING)
        return pltpu.make_async_remote_copy(
            src_ref=c_send.at[ring, kk], dst_ref=c_recv.at[lax.rem(u, RECV), 1, kk], send_sem=cs_sem.at[ring],
            recv_sem=part_sem.at[u - (NU - LATE), kk], device_id=pz_peer, device_id_type=MESH)

    def d_part(u, r, kk):
        part = (slice(None), pl.ds(2 * kk, 2))
        src, dst = (ref.reshape(Y, S, L).at[part] for ref in (d_send.at[u % RING, r - 1], d_recv.at[u, r]))
        return pltpu.make_async_remote_copy(
            src_ref=src, dst_ref=dst, send_sem=ds_sem.at[u % RING], recv_sem=dr_sem.at[(NG - 1) % RG],
            device_id=py_peer(r), device_id_type=MESH)

    def a_sent(g):
        ring = lax.rem(g, RA)
        return pltpu.make_async_copy(a_send.at[ring], a_send.at[ring], as_sem.at[ring])

    def a_arrived(u):
        ref = a_recv.at[lax.rem(u, AR), pl.ds(1, 3)]
        return pltpu.make_async_copy(ref, ref, ar_sem.at[lax.rem(u, AR)])

    def d_sent(u):
        ring = lax.rem(u, RING)
        return pltpu.make_async_copy(d_send.at[ring], d_send.at[ring], ds_sem.at[ring])

    def d_arrived(g):
        ref = d_recv.at[pl.ds(g * Q, Q), pl.ds(1, 3)]
        return pltpu.make_async_copy(ref, ref, dr_sem.at[lax.rem(g, RG)])

    def b_copy(u):
        ring = lax.rem(u, RING)
        return pltpu.make_async_remote_copy(
            src_ref=b_send.at[ring], dst_ref=b_recv.at[lax.rem(u, RECV), 1], send_sem=bs_sem.at[ring], recv_sem=br_sem.at[lax.rem(u, RECV)],
            device_id=pz_peer, device_id_type=MESH)

    def b_piece(u, k):
        return pltpu.make_async_remote_copy(
            src_ref=b_send.at[u, k], dst_ref=b_recv.at[u, 1, k], send_sem=bs_sem.at[u],
            recv_sem=br_sem.at[u] if u else part_sem.at[EARLY, k // 2], device_id=pz_peer, device_id_type=MESH)

    def bh_arrived(h):
        ref = b_recv.at[0, 1, pl.ds(2 * h, 2)]
        return pltpu.make_async_copy(ref, ref, part_sem.at[EARLY, h])

    def c_half(h):
        kk = pl.ds(2 * h, 2)
        return pltpu.make_async_remote_copy(
            src_ref=c_send.at[0, kk], dst_ref=c_recv.at[0, 1, kk], send_sem=cs_sem.at[0], recv_sem=cr_sem.at[0],
            device_id=pz_peer, device_id_type=MESH)

    def c_copy(u):
        ring = lax.rem(u, RING)
        return pltpu.make_async_remote_copy(
            src_ref=c_send.at[ring], dst_ref=c_recv.at[lax.rem(u, RECV), 1], send_sem=cs_sem.at[ring], recv_sem=cr_sem.at[lax.rem(u, RECV)],
            device_id=pz_peer, device_id_type=MESH)

    def d_copy(u, r):
        ring = lax.rem(u, RING)
        return pltpu.make_async_remote_copy(
            src_ref=d_send.at[ring, r - 1], dst_ref=d_recv.at[u, r], send_sem=ds_sem.at[ring],
            recv_sem=dr_sem.at[lax.rem(u // Q, RG)], device_id=py_peer(r), device_id_type=MESH)

    def send_a(g):
        for c in range(Q):
            for r in (2, 1, 3):
                a_copy(g * Q + c, r).start()

    def y_lines(u, kks):
        ring, slot, arrived = lax.rem(u, RING), lax.rem(u, RECV), lax.rem(u, AR)
        cols = [jnp.concatenate([a_recv[arrived, r, pl.ds(kk * 2 + ri, Y, stride=S), :]
                                 for r in range(Q) for ri in range(2)], 0) for kk in kks]
        out = left(lmat(1), jnp.concatenate(cols, 1))
        for i, kk in enumerate(kks):
            b_recv[slot, 0, kk] = out[:H, i * L:(i + 1) * L]
            b_send[ring, kk] = out[H:, i * L:(i + 1) * L]

    def stage2(u):
        a_arrived(u).wait()

        @pl.when(u >= RING)
        def _():
            b_copy(u - RING).wait_send()

        for kp in range(2):
            y_lines(u, (2 * kp, 2 * kp + 1))
        b_copy(u).start()

    def z_lines(u, kp):
        ring, c, f0 = lax.rem(u, RING), lax.rem(u, Q), u // Q * FG
        wf, wi = rmat(2), rmat(3)
        rows = []
        for kk in (2 * kp, 2 * kp + 1):
            rows += swap_lanes([b_recv[lax.rem(u, RECV), q, kk, ri * Z:(ri + 1) * Z, :] for q in range(2) for ri in range(2)])
        spec = right(jnp.concatenate(rows, 0), wf)
        hats = []
        for i in range(2):
            kk = 2 * kp + i
            gr = pl.ds(pl.multiple_of((c * Q + kk) * Z, Z), Z)
            gan, gbn = ga[gr, :], gb[gr, :]
            for f in range(FG):
                s = spec[(i * FG + f) * Z:(i * FG + f + 1) * Z]
                h = s * gan + pltpu.roll(s, H, 1) * gbn
                hat_re[f0 + f, c * Q + kk] = h[:, :N]
                hat_im[f0 + f, c * Q + kk] = h[:, N:]
                hats.append(h)
        back = right(jnp.concatenate(hats, 0), wi)
        for i in range(2):
            kk = 2 * kp + i
            t = swap_lanes([back[(i * FG + f) * Z:(i * FG + f + 1) * Z] for f in range(FG)])
            for ri in range(2):
                c_recv[lax.rem(u, RECV), 0, kk, ri * Z:(ri + 1) * Z, :] = t[ri]
                c_send[ring, kk, ri * Z:(ri + 1) * Z, :] = t[2 + ri]

    def stage3(u):
        b_copy(u).wait_recv()

        @pl.when(u >= RING)
        def _():
            c_copy(u - RING).wait_send()

        for kp in range(2):
            z_lines(u, kp)

        @pl.when(u < NU - LATE)
        def _():
            c_copy(u).start()

        @pl.when(u >= NU - LATE)
        def _():
            for kk in range(Q):
                c_part(u, kk).start()

    def y_lines_back(u, kks):
        ring = lax.rem(u, RING)
        cols = [jnp.concatenate([c_recv[lax.rem(u, RECV), q, kk] for q in range(2)], 0) for kk in kks]
        out = left(lmat(Q), jnp.concatenate(cols, 1))
        for i, kk in enumerate(kks):
            for r in range(Q):
                for ro in range(2):
                    rows = pl.ds(kk * 2 + ro, Y, stride=S)
                    tile = out[(r * 2 + ro) * Y:(r * 2 + ro + 1) * Y, i * L:(i + 1) * L]
                    if r == 0:
                        d_recv[u, 0, rows, :] = tile
                    else:
                        d_send[ring, r - 1, rows, :] = tile

    def stage4(u):
        c_copy(u).wait_recv()

        @pl.when(u >= RING)
        def _():
            d_sent(u - RING).wait()

        for kp in range(2):
            y_lines_back(u, (2 * kp, 2 * kp + 1))
        for r in (2, 1, 3):
            d_copy(u, r).start()

    def stage5(g, y0, ny):
        w = rmat(5)
        for i in range(ny):
            y = y0 + i
            rows = pl.ds(pl.multiple_of(y * S, S), S)
            x = jnp.concatenate([d_recv[g * Q + c, r, rows, :] for c in range(Q) for r in range(Q)], 0)
            out = right(x.T, w)
            for f in range(FG):
                for r in range(Q):
                    d_recv[g * Q + f, r, rows, :] = out[(f * Q + r) * S:(f * Q + r + 1) * S]

    odd = lax.rem(me, 2)
    order = (2 - odd, 3 - odd, 1 + 2 * odd)
    tabs[0].wait()
    table(0)
    for q in range(BLOCKS):
        first_loaded(q).wait()
        stage1(0, q * NY, NY)
        if q == 0:
            pl.semaphore_wait(barrier, Q)
        for r in order:
            a_piece(0, 0, r, q * NY, NY).start()
    for u, k in PIECES[1:]:
        for r in order:
            a_piece(u, k, r, 0, Y).start()
    for u in range(EARLY, Q):
        for r in (2, 1, 3):
            a_copy(u, r).start()
    for cp in load_in(2):
        cp.start()
    pltpu.make_async_copy(wraw.at[pl.ds(1, 5)], wraw.at[pl.ds(1, 5)], w_sem.at[1]).wait()
    for k in range(1, 6):
        table(k)
    pltpu.make_async_copy(gin, gin, g_sem).wait()
    gr, gi = gin[0].reshape(512, N), gin[1].reshape(512, N)
    ga[...] = jnp.concatenate([gr, gr], 1)
    gb[...] = jnp.concatenate([-gi, gi], 1)
    inputs_of(1)

    @pl.loop(0, Q)
    def _(q):
        stage1(1, q * Q, Q)

    send_a(1)
    for cp in load_in(3):
        cp.start()
    for u, k in PIECES:
        piece_arrived(u, k).wait()
        y_lines(u, (k,))
        b_piece(u, k).start()
    for h in range(2):
        bh_arrived(h).wait()
        z_lines(0, h)
        c_half(h).start()

    inputs_of(2)
    for q in range(EARLY):
        stage1(2, q * Q, Q)

    def step(t, carry):
        c = lax.rem(t, Q)
        g1 = t // Q + 2

        @pl.when(t < NU)
        def _():
            stage2(t)

        u3 = t - LAG3

        @pl.when(u3 >= 1)
        def _():
            stage3(u3)

        u4 = t - LAG4

        @pl.when(u4 >= 0)
        def _():
            stage4(u4)

        @pl.when(g1 < NG)
        def _():
            @pl.when(c == 0)
            def _():
                inputs_of(g1)

                @pl.when(g1 >= RA)
                def _():
                    a_sent(g1 - RA).wait()

            stage1(g1, c * Q, Q)

            @pl.when(c == 3)
            def _():
                send_a(g1)

                @pl.when(g1 + 2 < NG)
                def _():
                    for cp in load_in(g1 + 2):
                        cp.start()

        u5 = t - LAG5

        @pl.when(u5 >= 0)
        def _():
            @pl.when(lax.rem(u5, Q) == 0)
            def _():
                d_arrived(u5 // Q).wait()

            stage5(u5 // Q, lax.rem(u5, Q) * Q, Q)

        return carry

    steps = NU - LATE + LAG4
    lax.fori_loop(EARLY, steps, step, 0)
    rest = [u5 for u5 in range(steps - LAG5, NU - Q)]
    u3 = [u for u in range(steps - LAG3, NU)]
    for u in range(NU - LATE, NU):
        if u3:
            stage3(u3.pop(0))
        d_sent(u - RING).wait()
        for kk in range(Q):
            c_part(u, kk).wait_recv()
            y_lines_back(u, (kk,))
            for r in (2, 1, 3):
                d_part(u, r, kk).start()
        for u5 in rest[:2]:
            if u5 % Q == 0:
                d_arrived(u5 // Q).wait()
            stage5(u5 // Q, u5 % Q * Q, Q)
        rest = rest[2:]
    d_arrived(NG - 1).wait()

    for g in range(NG - RA, NG):
        a_sent(g).wait()
    for u in range(NU - RING, NU):
        b_copy(u).wait_send()
        c_copy(u).wait_send()
        d_sent(u).wait()


def unpack(phi, re, im, t5, phi_re, phi_im, hat_re, hat_im, wraw, st, st_last, w_sem, hat_sem, sem, last_sem):
    tab = pltpu.make_async_copy(t5.at[lax.axis_index("py")], wraw, w_sem)
    tab.start()
    hats, phis = ((re, hat_re), (im, hat_im)), (phi_re, phi_im)
    for i in range(FIELDS // HB):
        part = pl.ds(i * HB, HB)
        for k, (src, dst) in enumerate(hats):
            pltpu.make_async_copy(src.at[part], dst.at[part], hat_sem.at[k]).start()

    def last_copy(k):
        return pltpu.make_async_copy(st_last.at[k], phis[k].at[pl.ds(FIELDS - FG, FG)], last_sem)

    tab.wait()
    wide, narrow = right_table(*(wraw[i] for i in range(3)))
    w = wide, from_wide(narrow)

    @pl.loop(0, Q)
    def _(q):
        for i in range(Q):
            y = q * Q + i
            rows = pl.ds(pl.multiple_of(y * S, S), S)
            x = jnp.concatenate([phi[NU - Q + c, r, rows, :] for c in range(Q) for r in range(Q)], 0)
            out = right(x.T, w)
            for k, half in enumerate((out[:, :N], out[:, N:])):
                st_last[k, :, y] = half.reshape(FG, Z, N)

    for k in range(2):
        last_copy(k).start()

    def copy(i, k):
        slot = lax.rem(i, SLOTS)
        return pltpu.make_async_copy(st.at[slot, k], phis[k].at[pl.ds(i * FB, FB)], sem.at[slot])

    def written(i):
        slot = lax.rem(i, SLOTS)
        pltpu.make_async_copy(st.at[slot], st.at[slot], sem.at[slot]).wait()

    def phi_job(i, carry):
        slot = lax.rem(i, SLOTS)

        @pl.when(i >= SLOTS)
        def _():
            written(i - SLOTS)

        for f in range(FB):
            for r in range(Q):
                p = phi[i * FB + f, r]
                for k, half in enumerate((p[:, :N], p[:, N:])):
                    st[slot, k, f, :, r * S:(r + 1) * S] = half.reshape(Y, S, N)
        for k in range(2):
            copy(i, k).start()
        return carry

    jobs = (FIELDS - FG) // FB
    lax.fori_loop(0, jobs, phi_job, 0)
    for k, (src, dst) in enumerate(hats):
        pltpu.make_async_copy(src, dst, hat_sem.at[k]).wait()
    pltpu.make_async_copy(st_last, st_last, last_sem).wait()
    for i in range(jobs - SLOTS, jobs):
        written(i)


def in_hbm(x):
    return pltpu.with_memory_space_constraint(x, pltpu.HBM)


def solution(mesh):
    consts = tables()

    def local_solve(rho_re, rho_im, g_re, g_im):
        dma, vmem, hbm = pltpu.SemaphoreType.DMA, pltpu.VMEM, pl.BlockSpec(memory_space=pl.ANY)
        tabs = [jnp.asarray(c) for c in consts]
        field = jax.ShapeDtypeStruct((FIELDS, Y, Z, N), F32)
        packed = pl.pallas_call(
            kernel,
            out_shape=[pltpu.VMEM((NU, Q, L, L), F32)] + [pltpu.VMEM(field.shape, F32)] * 2,
            in_specs=[hbm] * 10,
            out_specs=[pl.BlockSpec(memory_space=pltpu.VMEM)] * 3,
            scratch_shapes=[
                vmem((2, 2, FG, Y, Z, N), F32),
                vmem((2, Y, Z, N), F32),
                vmem((6, 3, L, L), BF16),
                vmem((6, 256, 256), BF16),
                vmem((6, L, 256), BF16),
                vmem((512, L), F32), vmem((512, L), F32),
                vmem((RA, Q, 3, L, L), F32),
                vmem((AR, Q, L, L), F32),
                vmem((RING, Q, H, L), F32),
                vmem((RECV, 2, Q, H, L), F32),
                vmem((RING, Q, H, L), F32),
                vmem((RECV, 2, Q, H, L), F32),
                vmem((RING, 3, L, L), F32),
                dma((2,)), dma((BLOCKS,)), dma, dma((2,)), dma((RA,)), dma((AR,)),
                dma((RING,)), dma((RECV,)), dma((RING,)), dma((RECV,)), dma((LATE, Q)), dma((RING,)), dma((RG,)),
            ],
            compiler_params=pltpu.CompilerParams(collective_id=0, has_side_effects=True,
                                                 vmem_limit_bytes=24 << 20),
            name="spectral",
        )(*(in_hbm(x) for x in (jnp.transpose(rho_re, (0, 2, 3, 1)), jnp.transpose(rho_im, (0, 2, 3, 1)), g_re, g_im, *tabs)))
        packed = [pltpu.with_memory_space_constraint(x, pltpu.VMEM) for x in packed]
        phi_re, phi_im, hat_re, hat_im = pl.pallas_call(
            unpack,
            out_shape=[field] * Q,
            in_specs=[pl.BlockSpec(memory_space=pltpu.VMEM)] * 3 + [hbm],
            out_specs=[hbm] * Q,
            scratch_shapes=[vmem((3, L, L), BF16), vmem((SLOTS, 2, FB, Y, Z, N), F32),
                            vmem((2, FG, Y, Z, N), F32), dma, dma((2,)), dma((SLOTS,)), dma],
            compiler_params=pltpu.CompilerParams(vmem_limit_bytes=20 << 20),
            name="unpack",
        )(*packed, in_hbm(tabs[5]))
        return jnp.transpose(phi_re, (0, 3, 1, 2)), jnp.transpose(phi_im, (0, 3, 1, 2)), hat_re, hat_im

    space_layout = P("dp", None, "py", "pz")
    wave_layout = P("dp", "py", "pz", None)
    green_layout = P("py", "pz", None)
    return jax.shard_map(local_solve, mesh=mesh,
                         in_specs=(space_layout, space_layout, green_layout, green_layout),
                         out_specs=(space_layout, space_layout, wave_layout, wave_layout),
                         check_vma=False)
```

```python
import functools

import jax
import jax.numpy as jnp
import ml_dtypes
import numpy as np
from jax import lax
from jax.experimental import pallas as pl
from jax.experimental.pallas import tpu as pltpu
from jax.sharding import PartitionSpec as P

MESH = pl.DeviceIdType.MESH
L, H, Z, Y, S, Q = 128, 64, 32, 16, 8, 4
F32, BF16 = jnp.float32, jnp.bfloat16
N = 64
FIELDS = 32
FG = 4
NG = FIELDS // FG
NU = NG * 4
NPY, NPZ = 4, 2
LAG3, LAG4 = 2, 4
LAG5 = LAG4 + 5
RING = 3
RECV = 6
RG = 4
RA = 3
AR = 16
BLOCKS = 2
NY = 16 // BLOCKS
EARLY = 2
PIECES = [(u, k) for u in range(EARLY) for k in range(4)]
LATE = 3
FB, SLOTS = 4, 4
HB = 8


def dft(sign):
    jk = np.outer(np.arange(N), np.arange(N)) % N
    c, s = np.cos(2 * np.pi * jk / N) / S, sign * np.sin(2 * np.pi * jk / N) / S
    return np.stack([np.stack([c, -s], 1), np.stack([s, c], 1)])


def split_np(w):
    w = np.asarray(w, np.float32)
    parts = []
    for _ in range(3):
        part = w.astype(ml_dtypes.bfloat16)
        parts.append(part)
        w = w - part.astype(np.float32)
    return np.stack(parts)


def tables():
    fwd, inv = dft(-1), dft(1)
    i16, i32 = np.arange(Y), np.arange(Z)
    w1, w2, w3, w3i, w4, w5 = [], [], [], [], [], []
    for a in range(NPY):
        to = [Y * ((a + r) % Q) + i16 for r in range(Q)]
        frm = [Y * ((a - r) % Q) + i16 for r in range(Q)]
        out = np.stack([fwd[:, k] for k in to]).reshape(Q, 2, Q, Q, 2, N)
        w1.append(out.transpose(Q, 5, 0, 2, 3, 1).reshape(L, L))
        inn = np.stack([inv[:, :, :, k] for k in frm]).reshape(Q, 2, N, 2, Q, Q)
        w5.append(inn.transpose(Q, 0, 5, 3, 1, 2).reshape(L, L))
        for b in range(NPZ):
            half = [Z * (b ^ q) + i32 for q in range(2)]
            m = np.stack([fwd[:, k] for k in half])
            m = np.stack([m[..., y] for y in frm])
            w2.append(m.transpose(1, 2, 3, 0, Q, 5).reshape(L, L))
            m = np.stack([inv[:, y] for y in to])
            m = np.stack([m[..., k] for k in half])
            w4.append(m.transpose(1, 2, 3, 0, Q, 5).reshape(L, L))
    for b in range(NPZ):
        half = [Z * (b ^ q) + i32 for q in range(2)]
        m = np.stack([fwd[..., z] for z in half])
        w3.append(m.transpose(0, 3, Q, 1, 2).reshape(L, L))
        m = np.stack([inv[:, z] for z in half])
        w3i.append(m.transpose(3, Q, 0, 1, 2).reshape(L, L))
    return [np.stack([split_np(w) for w in ws]) for ws in (w1, w2, w3, w3i, w4, w5)]


def split3(x):
    hi = x.astype(BF16)
    rest = x - hi.astype(F32)
    mid = rest.astype(BF16)
    return hi, mid, (rest - mid.astype(F32)).astype(BF16)


def dot(a, b):
    return jnp.dot(a, b, preferred_element_type=F32)


def left(w, x):
    hi, mid, lo = split3(x)
    wide = dot(w[0][...], jnp.concatenate([hi, mid], 0))
    return wide[:L] + (wide[L:] + dot(w[1][...], jnp.concatenate([hi, lo], 0)))


def right(x, w):
    hi, mid, lo = split3(x)
    wide = dot(jnp.concatenate([hi, mid], 1), w[0][...])
    return wide[:, :L] + (wide[:, L:] + dot(jnp.concatenate([hi, lo], 1), w[1][...]))


def left_table(w1, w2, w3):
    pairs = [jnp.concatenate([a, b], 1) for a, b in ((w1, w1), (w2, w2), (w3, w1))]
    return jnp.concatenate(pairs[:2], 0), pairs[2]


def right_table(w1, w2, w3):
    return jnp.concatenate([jnp.concatenate([w1, w2], 1)] * 2, 0), jnp.concatenate([w3, w1], 1)


def from_wide(w):
    return jnp.concatenate([w[:, :L], w[:, L:]], 0)


def swap_lanes(tiles):
    lane = lax.broadcasted_iota(jnp.int32, tiles[0].shape, 1)
    odd, high = (lane // Z) % 2 == 1, lane >= H
    t = list(tiles)
    for lo in (0, 2):
        a, b = t[lo], t[lo + 1]
        t[lo] = jnp.where(odd, pltpu.roll(b, Z, 1), a)
        t[lo + 1] = jnp.where(odd, b, pltpu.roll(a, 96, 1))
    for lo in (0, 1):
        a, b = t[lo], t[lo + 2]
        t[lo] = jnp.where(high, pltpu.roll(b, H, 1), a)
        t[lo + 2] = jnp.where(high, b, pltpu.roll(a, H, 1))
    return t


def kernel(rho_re, rho_im, g_re, g_im, t1, t2, t3, t3i, t4, t5, d_recv, hat_re, hat_im,
           rin, gin, wraw, wbig, wsmall, ga, gb, a_send, a_recv, b_send, b_recv, c_send, c_recv, d_send,
           in_sem, first_sem, g_sem, w_sem, as_sem, ar_sem, bs_sem, br_sem, cs_sem, cr_sem, part_sem,
           ds_sem, dr_sem):
    me, mz = lax.axis_index("py"), lax.axis_index("pz")
    zero = lax.axis_index("dp")

    def py_peer(r):
        return (zero, mz, lax.rem(me + r, NPY))

    pz_peer = (zero, 1 - mz, me)

    def load_in(g):
        slot = lax.rem(g, 2)
        return [pltpu.make_async_copy(src.at[pl.ds(g * FG, FG)], rin.at[slot, i], in_sem.at[slot])
                for i, src in enumerate((rho_re, rho_im))]

    def inputs_of(g):
        ref = rin.at[lax.rem(g, 2)]
        pltpu.make_async_copy(ref, ref, in_sem.at[lax.rem(g, 2)]).wait()

    def load_first(q):
        ys = pl.ds(q * NY, NY)
        return [pltpu.make_async_copy(src.at[pl.ds(0, FG), ys], rin.at[0, i, :, ys], first_sem.at[q])
                for i, src in enumerate((rho_re, rho_im))]

    def first_loaded(q):
        ref = rin.at[0, :, :, pl.ds(q * NY, NY)]
        return pltpu.make_async_copy(ref, ref, first_sem.at[q])

    barrier = pltpu.get_barrier_semaphore()
    for peer in [py_peer(r) for r in (1, 2, 3)] + [pz_peer]:
        pl.semaphore_signal(barrier, inc=1, device_id=peer, device_id_type=MESH)
    both = me * NPZ + mz
    tabs = [pltpu.make_async_copy(t.at[i], wraw.at[k], w_sem.at[min(k, 1)])
            for k, (t, i) in enumerate(((t1, me), (t2, both), (t3, mz), (t3i, mz), (t4, both), (t5, me)))]
    greens = [pltpu.make_async_copy(src, gin.at[i], g_sem) for i, src in enumerate((g_re, g_im))]
    firsts = [cp for q in range(BLOCKS) for cp in load_first(q)]
    for cp in tabs[:1] + firsts + tabs[1:] + greens + load_in(1):
        cp.start()

    def table(k):
        wide, narrow = (left_table if k in (1, Q) else right_table)(*(wraw[k, i] for i in range(3)))
        wbig[k] = wide
        wsmall[k] = narrow

    def lmat(k):
        return wbig.at[k], wsmall.at[k]

    def rmat(k):
        return wbig[k], from_wide(wsmall[k])

    def stage1(g, y0, ny):
        slot, ring = lax.rem(g, 2), lax.rem(g, RA)
        w = rmat(0)
        for i in range(ny):
            y = y0 + i
            x = jnp.concatenate([rin[slot, 0, :, y].reshape(L, N), rin[slot, 1, :, y].reshape(L, N)], 1)
            out = right(x, w).T
            rows = pl.ds(pl.multiple_of(y * S, S), S)
            for c in range(Q):
                for r in range(Q):
                    tile = out[(r * Q + c) * S:(r * Q + c + 1) * S]
                    if r == 0:
                        a_recv[lax.rem(g * Q + c, AR), 0, rows, :] = tile
                    else:
                        a_send[ring, c, r - 1, rows, :] = tile

    def a_copy(u, r):
        g, c = u // Q, lax.rem(u, Q)
        ring = lax.rem(g, RA)
        return pltpu.make_async_remote_copy(
            src_ref=a_send.at[ring, c, r - 1], dst_ref=a_recv.at[lax.rem(u, AR), r], send_sem=as_sem.at[ring],
            recv_sem=ar_sem.at[lax.rem(u, AR)], device_id=py_peer(r), device_id_type=MESH)

    def a_piece(u, k, r, y0, ny):
        part = (pl.ds(y0, ny), pl.ds(2 * k, 2))
        src, dst = (ref.reshape(Y, S, L).at[part] for ref in (a_send.at[0, u, r - 1], a_recv.at[u, r]))
        return pltpu.make_async_remote_copy(
            src_ref=src, dst_ref=dst, send_sem=as_sem.at[0], recv_sem=part_sem.at[u, k],
            device_id=py_peer(r), device_id_type=MESH)

    def piece_arrived(u, k):
        ref = a_recv.at[u, pl.ds(1, 3), pl.ds(Z * k, Z)]
        return pltpu.make_async_copy(ref, ref, part_sem.at[u, k])

    def c_part(u, kk):
        ring = lax.rem(u, RING)
        return pltpu.make_async_remote_copy(
            src_ref=c_send.at[ring, kk], dst_ref=c_recv.at[lax.rem(u, RECV), 1, kk], send_sem=cs_sem.at[ring],
            recv_sem=part_sem.at[u - (NU - LATE), kk], device_id=pz_peer, device_id_type=MESH)

    def d_part(u, r, kk):
        part = (slice(None), pl.ds(2 * kk, 2))
        src, dst = (ref.reshape(Y, S, L).at[part] for ref in (d_send.at[u % RING, r - 1], d_recv.at[u, r]))
        return pltpu.make_async_remote_copy(
            src_ref=src, dst_ref=dst, send_sem=ds_sem.at[u % RING], recv_sem=dr_sem.at[(NG - 1) % RG],
            device_id=py_peer(r), device_id_type=MESH)

    def a_sent(g):
        ring = lax.rem(g, RA)
        return pltpu.make_async_copy(a_send.at[ring], a_send.at[ring], as_sem.at[ring])

    def a_arrived(u):
        ref = a_recv.at[lax.rem(u, AR), pl.ds(1, 3)]
        return pltpu.make_async_copy(ref, ref, ar_sem.at[lax.rem(u, AR)])

    def d_sent(u):
        ring = lax.rem(u, RING)
        return pltpu.make_async_copy(d_send.at[ring], d_send.at[ring], ds_sem.at[ring])

    def d_arrived(g):
        ref = d_recv.at[pl.ds(g * Q, Q), pl.ds(1, 3)]
        return pltpu.make_async_copy(ref, ref, dr_sem.at[lax.rem(g, RG)])

    def b_copy(u):
        ring = lax.rem(u, RING)
        return pltpu.make_async_remote_copy(
            src_ref=b_send.at[ring], dst_ref=b_recv.at[lax.rem(u, RECV), 1], send_sem=bs_sem.at[ring], recv_sem=br_sem.at[lax.rem(u, RECV)],
            device_id=pz_peer, device_id_type=MESH)

    def b_piece(u, k):
        return pltpu.make_async_remote_copy(
            src_ref=b_send.at[u, k], dst_ref=b_recv.at[u, 1, k], send_sem=bs_sem.at[u],
            recv_sem=br_sem.at[u] if u else part_sem.at[EARLY, k // 2], device_id=pz_peer, device_id_type=MESH)

    def bh_arrived(h):
        ref = b_recv.at[0, 1, pl.ds(2 * h, 2)]
        return pltpu.make_async_copy(ref, ref, part_sem.at[EARLY, h])

    def c_half(h):
        kk = pl.ds(2 * h, 2)
        return pltpu.make_async_remote_copy(
            src_ref=c_send.at[0, kk], dst_ref=c_recv.at[0, 1, kk], send_sem=cs_sem.at[0], recv_sem=cr_sem.at[0],
            device_id=pz_peer, device_id_type=MESH)

    def c_copy(u):
        ring = lax.rem(u, RING)
        return pltpu.make_async_remote_copy(
            src_ref=c_send.at[ring], dst_ref=c_recv.at[lax.rem(u, RECV), 1], send_sem=cs_sem.at[ring], recv_sem=cr_sem.at[lax.rem(u, RECV)],
            device_id=pz_peer, device_id_type=MESH)

    def d_copy(u, r):
        ring = lax.rem(u, RING)
        return pltpu.make_async_remote_copy(
            src_ref=d_send.at[ring, r - 1], dst_ref=d_recv.at[u, r], send_sem=ds_sem.at[ring],
            recv_sem=dr_sem.at[lax.rem(u // Q, RG)], device_id=py_peer(r), device_id_type=MESH)

    def send_a(g):
        for c in range(Q):
            for r in (2, 1, 3):
                a_copy(g * Q + c, r).start()

    def y_lines(u, kks):
        ring, slot, arrived = lax.rem(u, RING), lax.rem(u, RECV), lax.rem(u, AR)
        cols = [jnp.concatenate([a_recv[arrived, r, pl.ds(kk * 2 + ri, Y, stride=S), :]
                                 for r in range(Q) for ri in range(2)], 0) for kk in kks]
        out = left(lmat(1), jnp.concatenate(cols, 1))
        for i, kk in enumerate(kks):
            b_recv[slot, 0, kk] = out[:H, i * L:(i + 1) * L]
            b_send[ring, kk] = out[H:, i * L:(i + 1) * L]

    def stage2(u):
        a_arrived(u).wait()

        @pl.when(u >= RING)
        def _():
            b_copy(u - RING).wait_send()

        for kp in range(2):
            y_lines(u, (2 * kp, 2 * kp + 1))
        b_copy(u).start()

    def z_lines(u, kp):
        ring, c, f0 = lax.rem(u, RING), lax.rem(u, Q), u // Q * FG
        wf, wi = rmat(2), rmat(3)
        rows = []
        for kk in (2 * kp, 2 * kp + 1):
            rows += swap_lanes([b_recv[lax.rem(u, RECV), q, kk, ri * Z:(ri + 1) * Z, :] for q in range(2) for ri in range(2)])
        spec = right(jnp.concatenate(rows, 0), wf)
        hats = []
        for i in range(2):
            kk = 2 * kp + i
            gr = pl.ds(pl.multiple_of((c * Q + kk) * Z, Z), Z)
            gan, gbn = ga[gr, :], gb[gr, :]
            for f in range(FG):
                s = spec[(i * FG + f) * Z:(i * FG + f + 1) * Z]
                h = s * gan + pltpu.roll(s, H, 1) * gbn
                hat_re[f0 + f, c * Q + kk] = h[:, :N]
                hat_im[f0 + f, c * Q + kk] = h[:, N:]
                hats.append(h)
        back = right(jnp.concatenate(hats, 0), wi)
        for i in range(2):
            kk = 2 * kp + i
            t = swap_lanes([back[(i * FG + f) * Z:(i * FG + f + 1) * Z] for f in range(FG)])
            for ri in range(2):
                c_recv[lax.rem(u, RECV), 0, kk, ri * Z:(ri + 1) * Z, :] = t[ri]
                c_send[ring, kk, ri * Z:(ri + 1) * Z, :] = t[2 + ri]

    def stage3(u):
        b_copy(u).wait_recv()

        @pl.when(u >= RING)
        def _():
            c_copy(u - RING).wait_send()

        for kp in range(2):
            z_lines(u, kp)

        @pl.when(u < NU - LATE)
        def _():
            c_copy(u).start()

        @pl.when(u >= NU - LATE)
        def _():
            for kk in range(Q):
                c_part(u, kk).start()

    def y_lines_back(u, kks):
        ring = lax.rem(u, RING)
        cols = [jnp.concatenate([c_recv[lax.rem(u, RECV), q, kk] for q in range(2)], 0) for kk in kks]
        out = left(lmat(Q), jnp.concatenate(cols, 1))
        for i, kk in enumerate(kks):
            for r in range(Q):
                for ro in range(2):
                    rows = pl.ds(kk * 2 + ro, Y, stride=S)
                    tile = out[(r * 2 + ro) * Y:(r * 2 + ro + 1) * Y, i * L:(i + 1) * L]
                    if r == 0:
                        d_recv[u, 0, rows, :] = tile
                    else:
                        d_send[ring, r - 1, rows, :] = tile

    def stage4(u):
        c_copy(u).wait_recv()

        @pl.when(u >= RING)
        def _():
            d_sent(u - RING).wait()

        for kp in range(2):
            y_lines_back(u, (2 * kp, 2 * kp + 1))
        for r in (2, 1, 3):
            d_copy(u, r).start()

    def stage5(g, y0, ny):
        w = rmat(5)
        for i in range(ny):
            y = y0 + i
            rows = pl.ds(pl.multiple_of(y * S, S), S)
            x = jnp.concatenate([d_recv[g * Q + c, r, rows, :] for c in range(Q) for r in range(Q)], 0)
            out = right(x.T, w)
            for f in range(FG):
                for r in range(Q):
                    d_recv[g * Q + f, r, rows, :] = out[(f * Q + r) * S:(f * Q + r + 1) * S]

    odd = lax.rem(me, 2)
    order = (2 - odd, 3 - odd, 1 + 2 * odd)
    tabs[0].wait()
    table(0)
    for q in range(BLOCKS):
        first_loaded(q).wait()
        stage1(0, q * NY, NY)
        if q == 0:
            pl.semaphore_wait(barrier, Q)
        for r in order:
            a_piece(0, 0, r, q * NY, NY).start()
    for u, k in PIECES[1:]:
        for r in order:
            a_piece(u, k, r, 0, Y).start()
    for u in range(EARLY, Q):
        for r in (2, 1, 3):
            a_copy(u, r).start()
    for cp in load_in(2):
        cp.start()
    pltpu.make_async_copy(wraw.at[pl.ds(1, 5)], wraw.at[pl.ds(1, 5)], w_sem.at[1]).wait()
    for k in range(1, 6):
        table(k)
    pltpu.make_async_copy(gin, gin, g_sem).wait()
    gr, gi = gin[0].reshape(512, N), gin[1].reshape(512, N)
    ga[...] = jnp.concatenate([gr, gr], 1)
    gb[...] = jnp.concatenate([-gi, gi], 1)
    inputs_of(1)

    @pl.loop(0, Q)
    def _(q):
        stage1(1, q * Q, Q)

    send_a(1)
    for cp in load_in(3):
        cp.start()
    for u, k in PIECES:
        piece_arrived(u, k).wait()
        y_lines(u, (k,))
        b_piece(u, k).start()
    for h in range(2):
        bh_arrived(h).wait()
        z_lines(0, h)
        c_half(h).start()

    inputs_of(2)
    for q in range(EARLY):
        stage1(2, q * Q, Q)

    def step(t, carry):
        c = lax.rem(t, Q)
        g1 = t // Q + 2

        @pl.when(t < NU)
        def _():
            stage2(t)

        u3 = t - LAG3

        @pl.when(u3 >= 1)
        def _():
            stage3(u3)

        u4 = t - LAG4

        @pl.when(u4 >= 0)
        def _():
            stage4(u4)

        @pl.when(g1 < NG)
        def _():
            @pl.when(c == 0)
            def _():
                inputs_of(g1)

                @pl.when(g1 >= RA)
                def _():
                    a_sent(g1 - RA).wait()

            stage1(g1, c * Q, Q)

            @pl.when(c == 3)
            def _():
                send_a(g1)

                @pl.when(g1 + 2 < NG)
                def _():
                    for cp in load_in(g1 + 2):
                        cp.start()

        u5 = t - LAG5

        @pl.when(u5 >= 0)
        def _():
            @pl.when(lax.rem(u5, Q) == 0)
            def _():
                d_arrived(u5 // Q).wait()

            stage5(u5 // Q, lax.rem(u5, Q) * Q, Q)

        return carry

    steps = NU - LATE + LAG4
    lax.fori_loop(EARLY, steps, step, 0)
    rest = [u5 for u5 in range(steps - LAG5, NU - Q)]
    u3 = [u for u in range(steps - LAG3, NU)]
    for u in range(NU - LATE, NU):
        if u3:
            stage3(u3.pop(0))
        d_sent(u - RING).wait()
        for kk in range(Q):
            c_part(u, kk).wait_recv()
            y_lines_back(u, (kk,))
            for r in (2, 1, 3):
                d_part(u, r, kk).start()
        for u5 in rest[:2]:
            if u5 % Q == 0:
                d_arrived(u5 // Q).wait()
            stage5(u5 // Q, u5 % Q * Q, Q)
        rest = rest[2:]
    d_arrived(NG - 1).wait()

    for g in range(NG - RA, NG):
        a_sent(g).wait()
    for u in range(NU - RING, NU):
        b_copy(u).wait_send()
        c_copy(u).wait_send()
        d_sent(u).wait()


def unpack(phi, re, im, t5, phi_re, phi_im, hat_re, hat_im, wraw, st, st_last, w_sem, hat_sem, sem):
    tab = pltpu.make_async_copy(t5.at[lax.axis_index("py")], wraw, w_sem)
    tab.start()
    hats, phis = ((re, hat_re), (im, hat_im)), (phi_re, phi_im)
    for i in range(FIELDS // HB):
        part = pl.ds(i * HB, HB)
        for k, (src, dst) in enumerate(hats):
            pltpu.make_async_copy(src.at[part], dst.at[part], hat_sem.at[k]).start()

    def last_copy(k):
        return pltpu.make_async_copy(st_last.at[k], phis[k].at[pl.ds(FIELDS - FG, FG)], w_sem)

    tab.wait()
    wide, narrow = right_table(*(wraw[i] for i in range(3)))
    w = wide, from_wide(narrow)

    @pl.loop(0, Q)
    def _(q):
        for i in range(Q):
            y = q * Q + i
            rows = pl.ds(pl.multiple_of(y * S, S), S)
            x = jnp.concatenate([phi[NU - Q + c, r, rows, :] for c in range(Q) for r in range(Q)], 0)
            out = right(x.T, w)
            for k, half in enumerate((out[:, :N], out[:, N:])):
                st_last[k, :, y] = half.reshape(FG, Z, N)

    for k in range(2):
        last_copy(k).start()

    def copy(i, k):
        slot = lax.rem(i, SLOTS)
        return pltpu.make_async_copy(st.at[slot, k], phis[k].at[pl.ds(i * FB, FB)], sem.at[slot])

    def written(i):
        slot = lax.rem(i, SLOTS)
        pltpu.make_async_copy(st.at[slot], st.at[slot], sem.at[slot]).wait()

    def phi_job(i, carry):
        slot = lax.rem(i, SLOTS)

        @pl.when(i >= SLOTS)
        def _():
            written(i - SLOTS)

        for f in range(FB):
            for r in range(Q):
                p = phi[i * FB + f, r]
                for k, half in enumerate((p[:, :N], p[:, N:])):
                    st[slot, k, f, :, r * S:(r + 1) * S] = half.reshape(Y, S, N)
        for k in range(2):
            copy(i, k).start()
        return carry

    jobs = (FIELDS - FG) // FB
    lax.fori_loop(0, jobs, phi_job, 0)
    for k, (src, dst) in enumerate(hats):
        pltpu.make_async_copy(src, dst, hat_sem.at[k]).wait()
    pltpu.make_async_copy(st_last, st_last, w_sem).wait()
    for i in range(jobs - SLOTS, jobs):
        written(i)


def in_hbm(x):
    return pltpu.with_memory_space_constraint(x, pltpu.HBM)


def solution(mesh):
    consts = tables()

    def local_solve(rho_re, rho_im, g_re, g_im):
        dma, vmem, hbm = pltpu.SemaphoreType.DMA, pltpu.VMEM, pl.BlockSpec(memory_space=pl.ANY)
        tabs = [jnp.asarray(c) for c in consts]
        field = jax.ShapeDtypeStruct((FIELDS, Y, Z, N), F32)
        packed = pl.pallas_call(
            kernel,
            out_shape=[pltpu.VMEM((NU, Q, L, L), F32)] + [pltpu.VMEM(field.shape, F32)] * 2,
            in_specs=[hbm] * 10,
            out_specs=[pl.BlockSpec(memory_space=pltpu.VMEM)] * 3,
            scratch_shapes=[
                vmem((2, 2, FG, Y, Z, N), F32),
                vmem((2, Y, Z, N), F32),
                vmem((6, 3, L, L), BF16),
                vmem((6, 256, 256), BF16),
                vmem((6, L, 256), BF16),
                vmem((512, L), F32), vmem((512, L), F32),
                vmem((RA, Q, 3, L, L), F32),
                vmem((AR, Q, L, L), F32),
                vmem((RING, Q, H, L), F32),
                vmem((RECV, 2, Q, H, L), F32),
                vmem((RING, Q, H, L), F32),
                vmem((RECV, 2, Q, H, L), F32),
                vmem((RING, 3, L, L), F32),
                dma((2,)), dma((BLOCKS,)), dma, dma((2,)), dma((RA,)), dma((AR,)),
                dma((RING,)), dma((RECV,)), dma((RING,)), dma((RECV,)), dma((LATE, Q)), dma((RING,)), dma((RG,)),
            ],
            compiler_params=pltpu.CompilerParams(collective_id=0, has_side_effects=True,
                                                 vmem_limit_bytes=24 << 20),
            name="spectral",
        )(*(in_hbm(x) for x in (jnp.transpose(rho_re, (0, 2, 3, 1)), jnp.transpose(rho_im, (0, 2, 3, 1)), g_re, g_im, *tabs)))
        packed = [pltpu.with_memory_space_constraint(x, pltpu.VMEM) for x in packed]
        phi_re, phi_im, hat_re, hat_im = pl.pallas_call(
            unpack,
            out_shape=[field] * Q,
            in_specs=[pl.BlockSpec(memory_space=pltpu.VMEM)] * 3 + [hbm],
            out_specs=[hbm] * Q,
            scratch_shapes=[vmem((3, L, L), BF16), vmem((SLOTS, 2, FB, Y, Z, N), F32),
                            vmem((2, FG, Y, Z, N), F32), dma, dma((2,)), dma((SLOTS,))],
            compiler_params=pltpu.CompilerParams(vmem_limit_bytes=20 << 20),
            name="unpack",
        )(*packed, in_hbm(tabs[5]))
        return jnp.transpose(phi_re, (0, 3, 1, 2)), jnp.transpose(phi_im, (0, 3, 1, 2)), hat_re, hat_im

    space_layout = P("dp", None, "py", "pz")
    wave_layout = P("dp", "py", "pz", None)
    green_layout = P("py", "pz", None)
    return jax.shard_map(local_solve, mesh=mesh,
                         in_specs=(space_layout, space_layout, green_layout, green_layout),
                         out_specs=(space_layout, space_layout, wave_layout, wave_layout),
                         check_vma=False)
```
